32 devices in a mesh: dp: 8 (over y, x, core), expert: 4 (over z).
Axes of the slice: x: 2, y: 2, z: 4, core: 2. Of those that a mesh axis runs over, the one named last changes fastest.
Arguments:
- layer_input: bfloat16 [10240, 2048], P(('dp', 'expert')), may hold values from -6 to 6
- cotangent: bfloat16 [10240, 2048], P(('dp', 'expert')), may hold values from -6 to 6
- cont_ids: int32 [10240], P('dp'), may hold values from 0 to 2, as said below
- attn_routes: int32 [10240, 2], P('dp'), may hold values from 0 to 3, all different within a row; in each aligned block of 320 rows (0 to 319, 320 to 639, ...) at most 180 rows name the same one
- attn_gates: float32 [10240, 2], P(('dp', 'expert')), may hold values from 0.25 to 1
- mlp_routes: int32 [10240, 2], P(('dp', 'expert')), may hold values from 0 to 3, all different within a row; in each aligned block of 320 rows (0 to 319, 320 to 639, ...) at most 180 rows name the same one
- mlp_gates: float32 [10240, 2], P(('dp', 'expert')), may hold values from 0.25 to 1
- gain_attn: bfloat16 [2048], P(('dp', 'expert')), may hold values from 0.5 to 1.5
- gain_mlp: bfloat16 [2048], P(('dp', 'expert')), may hold values from 0.5 to 1.5
- kv_weight: bfloat16 [2048, 4096], P(('dp', 'expert')), may hold values from -0.125 to 0.125
- query_weight: bfloat16 [2048, 4, 2048], P('dp', 'expert'), may hold values from -0.125 to 0.125
- output_weight: bfloat16 [2048, 4, 2048], P('dp', 'expert'), may hold values from -0.5 to 0.5
- mlp_weight: bfloat16 [5632, 4, 3, 2048], P('dp', 'expert'), may hold values from -0.125 to 0.125
Outputs:
- output: bfloat16 [10240, 2048], P(('dp', 'expert'))
- grad_input: float32 [10240, 2048], P(('dp', 'expert'))
- grad_gain_attn: float32 [2048], P(('dp', 'expert'))
- grad_gain_mlp: float32 [2048], P(('dp', 'expert'))
- grad_kv_weight: float32 [2048, 4096], P(('dp', 'expert'))
- grad_query_weight: float32 [2048, 4, 2048], P('dp', 'expert')
- grad_output_weight: float32 [2048, 4, 2048], P('dp', 'expert')
- grad_mlp_weight: float32 [5632, 4, 3, 2048], P('dp', 'expert')
The draws below stay inside these ranges and needn't reach their ends.
Inputs may be any that keep to these rules, and one draw needn't show every extreme that they name: `cont_ids`: in each group of 1280 consecutive rows the first 1024 have id 0 and ids 1 to 2 follow in order; continuation 1 starts at place 1024, and continuation c > 1 at place 1024 + (c - 1) * 128 plus a shift drawn evenly from -64 to 63. `attn_routes`: each row names 2 different experts; in the rows of one device no expert is named by more than 180 rows, a bound that some block reaches. `mlp_routes`: each row names 2 different experts; in the rows of one device no expert is named by more than 180 rows, a bound that some block reaches.
All inputs are finite; a program needn't handle non-finite values.
Results may differ from the reference program's by a relative error of at most 0.02.
Values may be sent and summed in bfloat16 or wider, within the bound.
A program may use at most 640 MiB of HBM per device.

```python
import math
import jax
import jax.numpy as jnp
import numpy as np
from jax import lax

D = 2048
FF = 5632
HEADS_KV = 16
HEAD = 128
TOP = 2
PROMPT = 1024
CONT_LEN = 128
CONTS = 2
EXPERTS = 4
F = 2048
GROUP_TOK = 1280
TOK_DEV = 320
TOKENS = 10240
CAP = 180


def draw_cont_ids(key, part):
    groups = TOKENS // GROUP_TOK
    shifts = jax.random.randint(key, (groups, CONTS), -(CONT_LEN // 2), CONT_LEN // 2)
    shifts = shifts * (jnp.arange(CONTS, dtype=jnp.int32)[None, :] > 0).astype(jnp.int32)
    starts = PROMPT + jnp.arange(CONTS, dtype=jnp.int32)[None, :] * CONT_LEN + shifts
    places = jnp.arange(GROUP_TOK, dtype=jnp.int32)
    labels = jnp.sum((places[None, :, None] >= starts[:, None, :]).astype(jnp.int32), axis=2)
    return labels.reshape(-1).astype(jnp.int32)


def level_of(stream_key, dims, shards, smallest, high):
    def one(axis_at, shards_of):
        heights = jax.random.uniform(jax.random.fold_in(jax.random.fold_in(stream_key, 6), axis_at), (shards_of,), jnp.float32, smallest / len(shards), high / len(shards))
        return jnp.repeat(jnp.exp(heights), dims[axis_at] // shards_of).reshape((-1,) + (1,) * (len(dims) - axis_at - 1))

    factor_of = one(*shards[0])
    for cut in shards[1:]:
        factor_of = factor_of * one(*cut)
    return factor_of


def assign_block(rng, own, number, rows, number_of, top, limit, skew):
    sequence = jax.random.permutation(rng, number_of)
    packed, common = shares(number_of, rows * top, limit, skew, True), shares(number_of, rows * top, limit, skew, False)
    places = jnp.arange(number_of)

    def named(sizes, rotation):
        used = int((sizes > 0).sum())
        fixed = max(1, used // 4)
        moved = fixed + (places - fixed + rotation * (used - fixed)) % max(1, number_of - fixed)
        return jnp.zeros((number_of,), jnp.int32).at[sequence[jnp.where(places < fixed, places, moved)]].set(jnp.asarray(sizes, jnp.int32))

    sizes = jnp.where(number % 4 == 0, named(packed, number // 4), named(common, number - number // 4 - 1))
    mixed = jax.random.permutation(jax.random.fold_in(own, 3), number_of)
    giver, sink = mixed[0:number_of // 2 * 2:2], mixed[1:number_of // 2 * 2:2]
    margin = jnp.minimum(sizes[giver] - 1, limit - sizes[sink]) // 2
    margin = jnp.where((giver == sequence[0]) | (sink == sequence[0]) | (sizes[sink] == 0), 0, jnp.maximum(margin, 0))
    moved = jax.random.randint(jax.random.fold_in(own, 4), (number_of // 2,), 0, 1 << 20) % (margin + 1)
    sizes = sizes.at[giver].add(-moved).at[sink].add(moved)
    items = jnp.searchsorted(jnp.cumsum(sizes), jnp.arange(rows * top), side="right").astype(jnp.int32)
    grid = items.reshape(top, rows).T
    grid = grid[jax.random.permutation(jax.random.fold_in(own, 1), rows)]
    rotation = jax.random.randint(jax.random.fold_in(own, 2), (rows, 1), 0, top)
    return jnp.take_along_axis(grid, (jnp.arange(top)[None, :] + rotation) % top, axis=1)


def shares(number_of, total, most, lean, full):
    weights = [(1 << 20) // math.isqrt(standing ** lean) + 1 for standing in range(1, number_of + 1)]
    largest = most if full else min(most, max(-(-total // number_of), total * weights[0] // sum(weights)))
    least = 1 if total - largest >= number_of - 1 else 0
    given, surplus = [largest] + [least] * (number_of - 1), total - largest - least * (number_of - 1)
    while surplus > 0:
        free = [i for i in range(1, number_of) if given[i] < largest] or [i for i in range(1, number_of) if given[i] < most]
        mass, budget = sum([weights[i] for i in free]), surplus
        for i in free:
            extra = min(most - given[i], max(1, budget * weights[i] // mass), surplus)
            given[i] = given[i] + extra
            surplus = surplus - extra
    return np.array(given)


def bell_draw(stream_key, dims, scale, most, shards=(), held_as=jnp.bfloat16):
    factor_of = level_of(stream_key, dims, shards, -0.22, 0.18) if shards else 1.0
    drawn = jax.random.normal(stream_key, dims, jnp.float32) * scale * factor_of
    return jnp.minimum(jnp.maximum(drawn, -most), most).astype(held_as)


def setup_inputs(seed: int = 0) -> dict:
    keys = jax.random.split(jax.random.key(seed), 14)
    layer_input = bell_draw(keys[0], (TOKENS, D), 1.0, 6.0, ((0, 32),))
    cotangent = bell_draw(keys[1], (TOKENS, D), 1.0, 6.0, ((0, 32),))
    cont_ids = draw_cont_ids(jax.random.fold_in(keys[13], 71), 0)
    attn_routes_keys = jax.random.split(jax.random.fold_in(keys[3], 1), TOKENS // TOK_DEV)
    attn_routes_turns = jax.random.permutation(jax.random.fold_in(keys[3], 3), TOKENS // TOK_DEV)
    attn_routes = jax.vmap(lambda own, number: assign_block(jax.random.fold_in(keys[3], 2), own, number, TOK_DEV, EXPERTS, TOP, CAP, 1))(attn_routes_keys, attn_routes_turns).reshape((TOKENS, TOP))
    attn_gates = jnp.clip(0.25 + 0.75 * jax.random.uniform(keys[4], (TOKENS, TOP), jnp.float32) ** level_of(keys[4], (TOKENS, TOP), ((0, 32),), -0.2, 0.2), 0.25, 1.0)
    mlp_routes_keys = jax.random.split(jax.random.fold_in(keys[5], 1), TOKENS // TOK_DEV)
    mlp_routes_turns = jax.random.permutation(jax.random.fold_in(keys[5], 3), TOKENS // TOK_DEV)
    mlp_routes = jax.vmap(lambda own, number: assign_block(jax.random.fold_in(keys[5], 2), own, number, TOK_DEV, EXPERTS, TOP, CAP, 1))(mlp_routes_keys, mlp_routes_turns).reshape((TOKENS, TOP))
    mlp_gates = jnp.clip(0.25 + 0.75 * jax.random.uniform(keys[6], (TOKENS, TOP), jnp.float32) ** level_of(keys[6], (TOKENS, TOP), ((0, 32),), -0.2, 0.2), 0.25, 1.0)
    gain_attn = jnp.clip(1.0 + 0.1 * jax.random.normal(keys[7], (D,), jnp.float32), 0.5, 1.5).astype(jnp.bfloat16)
    gain_mlp = jnp.clip(1.0 + 0.1 * jax.random.normal(keys[8], (D,), jnp.float32), 0.5, 1.5).astype(jnp.bfloat16)
    kv_weight = bell_draw(keys[9], (D, 2 * F), D ** -0.5, 0.125, ((0, 32),))
    query_weight = bell_draw(keys[10], (D, EXPERTS, F), D ** -0.5, 0.125, ((0, 8), (1, 4)))
    output_weight = bell_draw(keys[11], (F, EXPERTS, D), (F // 16) ** -0.5, 0.5, ((0, 8), (1, 4)))
    mlp_weight = bell_draw(keys[12], (FF, EXPERTS, 3, D), D ** -0.5, 0.125, ((0, 8), (1, 4)))
    return dict(layer_input=layer_input, cotangent=cotangent, cont_ids=cont_ids, attn_routes=attn_routes, attn_gates=attn_gates, mlp_routes=mlp_routes, mlp_gates=mlp_gates, gain_attn=gain_attn, gain_mlp=gain_mlp, kv_weight=kv_weight, query_weight=query_weight, output_weight=output_weight, mlp_weight=mlp_weight)


norm_eps = 1e-06
rope_base = 10000.0
neg_fill = -1e+30

@jax.custom_vjp
def low(v):
    return lax.optimization_barrier(v.astype(jnp.bfloat16)).astype(jnp.float32)

@jax.custom_vjp
def low_back(v):
    return v

def low_keep(v):
    return (low(v), None)

def low_pass(kept, grad):
    return (grad,)

def back_keep(v):
    return (v, None)

def back_low(kept, grad):
    return (low(grad),)
low.defvjp(low_keep, low_pass)
low_back.defvjp(back_keep, back_low)

def highest(left, right):
    return jnp.dot(left, right, precision=lax.Precision.HIGHEST)

def rope_angles(positions, head_size):
    half_size = head_size // 2
    freq_steps = jnp.arange(half_size, dtype=jnp.float32)
    inverse_freq = jnp.exp(-math.log(rope_base) * 2.0 * freq_steps / head_size)
    angle_table = positions.astype(jnp.float32)[:, None] * inverse_freq[None, :]
    return (jnp.cos(angle_table), jnp.sin(angle_table))

def rotate(values, cosine, sine):
    half_size = cosine.shape[1]
    head_count = values.shape[1] // (2 * half_size)
    shaped = values.reshape(values.shape[0], head_count, 2 * half_size)
    first_half = shaped[:, :, :half_size]
    second_half = shaped[:, :, half_size:]
    cos_part = cosine[:, None, :]
    sin_part = sine[:, None, :]
    turned = jnp.concatenate([first_half * cos_part - second_half * sin_part, second_half * cos_part + first_half * sin_part], axis=2)
    return turned.reshape(values.shape)

def token_positions(cont_ids):
    row_count = cont_ids.shape[0]
    group_count = row_count // GROUP_TOK
    places = jnp.arange(row_count, dtype=jnp.int32) % GROUP_TOK
    labels = jnp.arange(CONTS + 1, dtype=jnp.int32)
    one_hot = (cont_ids[:, None] == labels[None, :]).astype(jnp.int32)
    counts = lax.optimization_barrier(jnp.sum(one_hot.reshape(group_count, GROUP_TOK, CONTS + 1), axis=1))
    starts = jnp.cumsum(counts, axis=1) - counts
    starts_tok = jnp.broadcast_to(starts[:, None, :], (group_count, GROUP_TOK, CONTS + 1)).reshape(row_count, CONTS + 1)
    start_of = lax.optimization_barrier(jnp.sum(starts_tok * one_hot, axis=1))
    return places - start_of + PROMPT * (cont_ids > 0).astype(jnp.int32)

def rms_apply(values, gain_vec):
    row_scale = lax.rsqrt(lax.optimization_barrier(jnp.mean(values * values, axis=-1, keepdims=True)) + norm_eps)
    return values * row_scale * gain_vec

def group_attend(operands):
    query_group, key_group, value_group, ids_group = operands
    scores = jnp.einsum('qhd,khd->hqk', query_group, key_group, precision=lax.Precision.HIGHEST) * (1.0 / math.sqrt(HEAD))
    scores = low_back(scores)
    places = jnp.arange(GROUP_TOK, dtype=jnp.int32)
    allowed = (places[None, :] <= places[:, None]) & ((ids_group[None, :] == 0) | (ids_group[None, :] == ids_group[:, None]))
    scores = jnp.where(allowed[None, :, :], scores, neg_fill)
    probs_full = jax.nn.softmax(scores, axis=-1)
    return jnp.einsum('hqk,khd->qhd', low(probs_full), value_group, precision=lax.Precision.HIGHEST)

def forward(layer_input, gain_attn, gain_mlp, kv_weight, query_weight, output_weight, mlp_weight, cont_ids, position, attn_comb, mlp_comb):
    groups = layer_input.shape[0] // GROUP_TOK
    features = HEADS_KV * HEAD
    cosine, sine = rope_angles(position, HEAD)
    hidden_low = low(rms_apply(layer_input, gain_attn))
    kv_proj = low_back(highest(hidden_low, kv_weight))
    keys_low = low(rotate(kv_proj[:, :features], cosine, sine))
    values_low = low(kv_proj[:, features:])
    keys_grouped = keys_low.reshape(groups, GROUP_TOK, HEADS_KV, HEAD)
    values_grouped = values_low.reshape(groups, GROUP_TOK, HEADS_KV, HEAD)
    ids_grouped = cont_ids.reshape(groups, GROUP_TOK)
    attend = jax.checkpoint(group_attend)

    def attn_expert(total, operands):
        query_w, output_w, comb_row = operands
        rows_in = low_back(hidden_low)
        query_low = low(rotate(low_back(highest(rows_in, query_w)), cosine, sine))
        mixed = lax.map(attend, (query_low.reshape(groups, GROUP_TOK, HEADS_KV, HEAD), keys_grouped, values_grouped, ids_grouped))
        mixed_low = low(low_back(mixed.reshape(-1, features)))
        result_low = low(low_back(highest(mixed_low, output_w)))
        return (total + comb_row[:, None] * result_low, None)
    attn_total, unused_one = lax.scan(jax.checkpoint(attn_expert), jnp.zeros_like(layer_input), (jnp.transpose(query_weight, (1, 0, 2)), jnp.transpose(output_weight, (1, 0, 2)), attn_comb))
    residual = layer_input + attn_total
    second_low = low(rms_apply(residual, gain_mlp))

    def mlp_expert(total, operands):
        expert_w, comb_row = operands
        rows_in = low_back(second_low)
        gate_val = low_back(highest(rows_in, expert_w[:, 0, :].T))
        up_val = low_back(highest(rows_in, expert_w[:, 1, :].T))
        hidden = low(jax.nn.silu(gate_val) * up_val)
        result_low = low(low_back(highest(hidden, expert_w[:, 2, :])))
        return (total + comb_row[:, None] * result_low, None)
    mlp_total, unused_two = lax.scan(jax.checkpoint(mlp_expert), jnp.zeros_like(layer_input), (jnp.transpose(mlp_weight, (1, 0, 2, 3)), mlp_comb))
    return residual + mlp_total

def reference(layer_input, cotangent, cont_ids, attn_routes, attn_gates, mlp_routes, mlp_gates, gain_attn, gain_mlp, kv_weight, query_weight, output_weight, mlp_weight):
    position = token_positions(cont_ids)
    labels = jnp.arange(EXPERTS, dtype=jnp.int32)
    attn_comb = lax.optimization_barrier(jnp.sum(attn_gates[:, :, None] * (attn_routes[:, :, None] == labels[None, None, :]).astype(attn_gates.dtype), axis=1)).T
    mlp_comb = lax.optimization_barrier(jnp.sum(mlp_gates[:, :, None] * (mlp_routes[:, :, None] == labels[None, None, :]).astype(mlp_gates.dtype), axis=1)).T

    def wrapped(input_f, gain_one, gain_two, kv_f, query_f, output_f, mlp_f):
        return forward(input_f, gain_one, gain_two, kv_f, query_f, output_f, mlp_f, cont_ids, position, attn_comb, mlp_comb)
    params = (layer_input.astype(jnp.float32), gain_attn.astype(jnp.float32), gain_mlp.astype(jnp.float32), kv_weight.astype(jnp.float32), query_weight.astype(jnp.float32), output_weight.astype(jnp.float32), mlp_weight.astype(jnp.float32))
    result, pull = jax.vjp(wrapped, *params)
    grads = pull(cotangent.astype(jnp.float32))
    return (result.astype(jnp.bfloat16), grads[0], grads[1], grads[2], grads[3], grads[4], grads[5], grads[6])
```

```python
import functools
import math

import jax
import jax.numpy as jnp
from jax import lax
from jax.experimental import pallas as pl
from jax.experimental.pallas import tpu as pltpu
from jax.sharding import PartitionSpec as P


HEAD = 128
PROMPT = 1024
CONTS = 2
GROUP_TOK = 1280
MLP_FIRST = 0.4

norm_eps = 1e-06
rope_base = 10000.0
neg_fill = -1e30
log2e = 1.4426950408889634
MESH = pl.DeviceIdType.MESH
contract_last = (((1,), (1,)), ((), ()))
contract_first = (((0,), (0,)), ((), ()))
f32 = jnp.float32
bf16 = jnp.bfloat16


def rope_tables(positions):
    half_size = HEAD // 2
    freq_steps = jnp.arange(half_size, dtype=f32)
    inverse_freq = jnp.exp(-math.log(rope_base) * 2.0 * freq_steps / HEAD)
    angles = positions.astype(f32)[:, None] * inverse_freq[None, :]
    cosine, sine = jnp.cos(angles), jnp.sin(angles)
    return (
        jnp.concatenate([cosine, cosine], axis=1),
        jnp.concatenate([-sine, sine], axis=1),
    )


def token_positions(cont_ids):
    row_count = cont_ids.shape[0]
    group_count = row_count // GROUP_TOK
    places = jnp.arange(row_count, dtype=jnp.int32) % GROUP_TOK
    labels = jnp.arange(CONTS + 1, dtype=jnp.int32)
    one_hot = (cont_ids[:, None] == labels[None, :]).astype(jnp.int32)
    counts = jnp.sum(one_hot.reshape(group_count, GROUP_TOK, CONTS + 1), axis=1)
    starts = jnp.cumsum(counts, axis=1) - counts
    starts_tok = jnp.broadcast_to(starts[:, None, :], (group_count, GROUP_TOK, CONTS + 1)).reshape(
        row_count, CONTS + 1
    )
    start_of = jnp.sum(starts_tok * one_hot, axis=1)
    return (places, places - start_of + PROMPT * (cont_ids > 0).astype(jnp.int32))


def rms_parts(values):
    row_scale = lax.rsqrt(jnp.mean(values * values, axis=-1, keepdims=True) + norm_eps)
    return (values * row_scale, row_scale)


def rms_back(grad_out, normed, row_scale, gain_vec):
    through = grad_out * gain_vec
    grad_in = row_scale * (through - normed * jnp.mean(through * normed, axis=-1, keepdims=True))
    return grad_in


def dot_nt(left, right):
    return lax.dot_general(left, right, contract_last, preferred_element_type=f32)


def dot_tn(left, right):
    return lax.dot_general(left, right, contract_first, preferred_element_type=f32)


def dot_nn(left, right):
    return jnp.dot(left, right, preferred_element_type=f32)


def before_counts(flags):
    count = flags.shape[-1]
    steps = jnp.arange(count, dtype=jnp.int32)
    earlier = (steps[:, None] < steps[None, :]).astype(bf16)
    return jnp.dot(flags.astype(bf16), earlier, preferred_element_type=f32).astype(jnp.int32)


def project_kernel(rope_blocks, tile, x_ref, w_ref, cos_ref, sin_ref, out_ref):
    rows = x_ref.shape[0]
    turn = pl.program_id(0) < rope_blocks
    for start in range(0, rows, tile):
        span = pl.ds(start, tile)
        product = jnp.dot(x_ref[span, :], w_ref[...], preferred_element_type=f32)

        @pl.when(turn)
        def _():
            cosine, sine = cos_ref[span, :], sin_ref[span, :]
            for col in range(0, product.shape[1], HEAD):
                piece = product[:, col : col + HEAD]
                turned = piece * cosine + pltpu.roll(piece, HEAD // 2, 1) * sine
                out_ref[span, col : col + HEAD] = turned.astype(bf16)

        @pl.when(jnp.logical_not(turn))
        def _():
            out_ref[span, :] = product.astype(bf16)


def project(rows, weight, cosine, sine, rope_cols, tile):
    count, width = rows.shape
    cols = weight.shape[1]
    block = 512
    return pl.pallas_call(
        functools.partial(project_kernel, rope_cols // block, tile),
        grid=(cols // block,),
        in_specs=[
            pl.BlockSpec((count, width), lambda i: (0, 0)),
            pl.BlockSpec((width, block), lambda i: (0, i)),
            pl.BlockSpec((count, HEAD), lambda i: (0, 0)),
            pl.BlockSpec((count, HEAD), lambda i: (0, 0)),
        ],
        out_specs=pl.BlockSpec((count, block), lambda i: (0, i)),
        out_shape=jax.ShapeDtypeStruct((count, cols), bf16),
        cost_estimate=pl.CostEstimate(
            flops=2 * count * width * cols,
            bytes_accessed=2 * (count * width + width * cols + count * cols),
            transcendentals=0,
        ),
    )(rows, weight, cosine, sine)


def key_spans(blocks, tokens, keys):
    return [min(-(-(tokens * (s + 1)) // 128) * 128, keys) for s in range(blocks)]


def fill_bias(bias, place_ref, cont_ref, kcont_ref):
    blocks, slots, keys = bias.shape
    kplace = lax.broadcasted_iota(jnp.int32, (slots, keys), 1)
    kcont = kcont_ref[...]
    for s in range(blocks):
        allowed = (kplace <= place_ref[s]) & ((kcont == 0) | (kcont == cont_ref[s]))
        bias[s] = jnp.where(allowed, 0.0, neg_fill)


def attend_kernel(spans, q_ref, k_ref, v_ref, place_ref, cont_ref, kcont_ref, out_ref, lse_ref, bias):
    @pl.when(pl.program_id(0) == 0)
    def _():
        fill_bias(bias, place_ref, cont_ref, kcont_ref)

    scale2 = log2e / math.sqrt(HEAD)
    for s, span in enumerate(spans):
        scores = dot_nt(q_ref[s], k_ref[:span, :]) * scale2 + bias[s, :, :span]
        peak = jnp.max(scores, axis=1, keepdims=True)
        weights = jnp.exp2(scores - peak)
        total = jnp.sum(weights, axis=1, keepdims=True)
        mixed = dot_nn(weights.astype(bf16), v_ref[:span, :])
        out_ref[s] = (mixed / total).astype(bf16)
        lse_ref[s] = jnp.broadcast_to(peak + jnp.log2(total), lse_ref.shape[1:])


def attend(query, kv_low, place, cont, kcont, tokens):
    blocks, slots, features = query.shape
    keys = kv_low.shape[0]
    heads = features // HEAD
    spans = key_spans(blocks, tokens, keys)
    work = 2 * 2 * slots * sum(spans) * HEAD * heads
    qspec = pl.BlockSpec((blocks, slots, HEAD), lambda h: (0, 0, h))
    whole = pl.BlockSpec((blocks, slots, 1), lambda h: (0, 0, 0))
    return pl.pallas_call(
        functools.partial(attend_kernel, spans),
        grid=(heads,),
        in_specs=[
            qspec,
            pl.BlockSpec((keys, HEAD), lambda h: (0, h)),
            pl.BlockSpec((keys, HEAD), lambda h: (0, heads + h)),
            whole,
            whole,
            pl.BlockSpec((1, keys), lambda h: (0, 0)),
        ],
        out_specs=[qspec, qspec],
        out_shape=[
            jax.ShapeDtypeStruct(query.shape, bf16),
            jax.ShapeDtypeStruct(query.shape, f32),
        ],
        scratch_shapes=[pltpu.VMEM((blocks, slots, keys), f32)],
        cost_estimate=pl.CostEstimate(
            flops=work,
            bytes_accessed=4 * query.size + 2 * kv_low.size + 4 * query.size,
            transcendentals=slots * sum(spans) * heads,
        ),
        name="attend",
    )(query, kv_low, kv_low, place, cont, kcont)


def attend_back_kernel(
    spans,
    q_ref,
    k_ref,
    v_ref,
    g_ref,
    lse_ref,
    place_ref,
    cont_ref,
    kcont_ref,
    qcos_ref,
    qsin_ref,
    kcos_ref,
    ksin_ref,
    dq_ref,
    dk_ref,
    dv_ref,
    bias,
    dk_sum,
    dv_sum,
):
    @pl.when(pl.program_id(0) == 0)
    def _():
        fill_bias(bias, place_ref, cont_ref, kcont_ref)

    scale = 1.0 / math.sqrt(HEAD)
    scale2 = log2e * scale
    last = len(spans) - 1
    for s in range(last, -1, -1):
        span = spans[s]
        query, grad = q_ref[s], g_ref[s]
        keys = k_ref[:span, :]
        scores = dot_nt(query, keys) * scale2 + bias[s, :, :span]
        prob = jnp.exp2(scores - lse_ref[s][:, :1])
        grad_prob = dot_nt(grad, v_ref[:span, :])
        inner = jnp.sum(prob * grad_prob, axis=1, keepdims=True)
        grad_scores = (prob * (grad_prob - inner)).astype(bf16)
        dq = dot_nn(grad_scores, keys) * scale
        dq = dq * qcos_ref[s] - pltpu.roll(dq, HEAD // 2, 1) * qsin_ref[s]
        dq_ref[s] = dq.astype(bf16)
        dk = dot_tn(grad_scores, query)
        dv = dot_tn(prob.astype(bf16), grad)
        if s == last:
            dk_sum[...] = dk
            dv_sum[...] = dv
        else:
            dk_sum[:span, :] += dk
            dv_sum[:span, :] += dv
    dk = dk_sum[...] * scale
    dk_ref[...] = (dk * kcos_ref[...] - pltpu.roll(dk, HEAD // 2, 1) * ksin_ref[...]).astype(bf16)
    dv_ref[...] = dv_sum[...].astype(bf16)


def attend_back(query, kv_low, grad, lse, place, cont, kcont, qcos, qsin, kcos, ksin, tokens):
    blocks, slots, features = query.shape
    keys = kv_low.shape[0]
    heads = features // HEAD
    spans = key_spans(blocks, tokens, keys)
    work = 5 * 2 * slots * sum(spans) * HEAD * heads
    qspec = pl.BlockSpec((blocks, slots, HEAD), lambda h: (0, 0, h))
    kspec = pl.BlockSpec((keys, HEAD), lambda h: (0, h))
    whole = pl.BlockSpec((blocks, slots, 1), lambda h: (0, 0, 0))
    qtab = pl.BlockSpec((blocks, slots, HEAD), lambda h: (0, 0, 0))
    ktab = pl.BlockSpec((keys, HEAD), lambda h: (0, 0))
    return pl.pallas_call(
        functools.partial(attend_back_kernel, spans),
        grid=(heads,),
        in_specs=[
            qspec,
            kspec,
            pl.BlockSpec((keys, HEAD), lambda h: (0, heads + h)),
            qspec,
            qspec,
            whole,
            whole,
            pl.BlockSpec((1, keys), lambda h: (0, 0)),
            qtab,
            qtab,
            ktab,
            ktab,
        ],
        out_specs=[qspec, kspec, kspec],
        out_shape=[
            jax.ShapeDtypeStruct(query.shape, bf16),
            jax.ShapeDtypeStruct((keys, features), bf16),
            jax.ShapeDtypeStruct((keys, features), bf16),
        ],
        scratch_shapes=[
            pltpu.VMEM((blocks, slots, keys), f32),
            pltpu.VMEM((keys, HEAD), f32),
            pltpu.VMEM((keys, HEAD), f32),
        ],
        cost_estimate=pl.CostEstimate(
            flops=work,
            bytes_accessed=10 * query.size + 4 * kv_low.size,
            transcendentals=slots * sum(spans) * heads,
        ),
        name="attend_back",
    )(query, kv_low, kv_low, grad, lse, place, cont, kcont, qcos, qsin, kcos, ksin)


def unit_kernel(
    x_hbm,
    g_hbm,
    gate_ref,
    up_ref,
    down_ref,
    in_ref,
    out_hbm,
    gg_hbm,
    gu_hbm,
    hid_hbm,
    xbuf,
    gbuf,
    obuf,
    kbuf,
    psend,
    precv,
    ssend,
    frecv,
    load_sem,
    store_sem,
    psend_sem,
    precv_sem,
    ssend_sem,
    frecv_sem,
):
    rows = xbuf.shape[1]
    chips = ssend.shape[0]
    me = lax.axis_index("dp")
    chip = me // 2
    core = me % 2
    partner = me + 1 - 2 * core

    def peer(hop):
        return {"dp": (chip + hop) % chips * 2 + core}

    barrier = pltpu.get_barrier_semaphore()
    pl.semaphore_signal(barrier, inc=1, device_id={"dp": partner}, device_id_type=MESH)
    for hop in range(1, chips):
        pl.semaphore_signal(barrier, inc=1, device_id=peer(hop), device_id_type=MESH)
    pl.semaphore_wait(barrier, chips)

    def block_rows(j, own):
        dest = (chip + chips - 1 - j) % chips
        block = dest * 2 + (core if own else 1 - core)
        return pl.ds(pl.multiple_of(block * rows, 8), rows)

    def loads(j, own):
        span, slot = block_rows(j, own), int(own)
        return [
            pltpu.make_async_copy(x_hbm.at[span], xbuf.at[slot], load_sem.at[0, slot]),
            pltpu.make_async_copy(g_hbm.at[span], gbuf.at[slot], load_sem.at[1, slot]),
        ]

    def stores(j, own):
        span, slot = block_rows(j, own), int(own)
        return [pltpu.make_async_copy(obuf.at[slot], out_hbm.at[span], store_sem.at[0, slot])] + [
            pltpu.make_async_copy(kbuf.at[slot, i], dst.at[span], store_sem.at[1 + i, slot])
            for i, dst in enumerate((gg_hbm, gu_hbm, hid_hbm))
        ]

    def to_partner(j):
        return pltpu.make_async_remote_copy(
            src_ref=psend.at[j % 2],
            dst_ref=precv.at[j],
            send_sem=psend_sem.at[j % 2],
            recv_sem=precv_sem.at[j],
            device_id={"dp": partner},
            device_id_type=MESH,
        )

    def to_owner(j):
        return pltpu.make_async_remote_copy(
            src_ref=ssend.at[j],
            dst_ref=frecv.at[j],
            send_sem=ssend_sem.at[j],
            recv_sem=frecv_sem.at[j],
            device_id=peer(chips - 1 - j),
            device_id_type=MESH,
        )

    def compute(j, own):
        slot = int(own)
        for copy in loads(j, own):
            copy.wait()
        rows_in, rows_grad = xbuf[slot], gbuf[slot]
        gate_val = dot_nt(rows_in, gate_ref[...])
        up_val = dot_nt(rows_in, up_ref[...])
        grad_hidden = dot_nt(rows_grad, down_ref[...])
        sigma = jax.nn.sigmoid(gate_val)
        active = gate_val * sigma
        hidden = (active * up_val).astype(bf16)
        grad_gate = (grad_hidden * up_val * sigma * (1.0 + gate_val * (1.0 - sigma))).astype(bf16)
        grad_up = (grad_hidden * active).astype(bf16)

        @pl.when(j > 0)
        def _():
            for copy in stores(j - 1, own):
                copy.wait()

        kbuf[slot, 0] = grad_gate
        kbuf[slot, 1] = grad_up
        kbuf[slot, 2] = hidden
        obuf[slot] = dot_nn(hidden, down_ref[...]).astype(bf16)
        for copy in stores(j, own):
            copy.start()
        return dot_nn(grad_gate, gate_ref[...]) + dot_nn(grad_up, up_ref[...])

    for copy in loads(0, False):
        copy.start()

    def step(j, carry):
        for copy in loads(j, True):
            copy.start()
        term = compute(j, False)

        @pl.when(j > 1)
        def _():
            to_partner(j - 2).wait_send()

        psend[j % 2] = term.astype(bf16)
        to_partner(j).start()

        @pl.when(j < chips - 1)
        def _():
            for copy in loads(j + 1, False):
                copy.start()

        term = compute(j, True)
        to_partner(j).wait_recv()
        ssend[j] = (term + precv[j].astype(f32)).astype(bf16)

        @pl.when(j < chips - 1)
        def _():
            to_owner(j).start()

        return carry

    lax.fori_loop(0, chips, step, 0)
    total = ssend[chips - 1].astype(f32)
    for j in range(chips - 1):
        to_owner(j).wait_recv()
        total = total + frecv[j].astype(f32)
    in_ref[...] = total.astype(bf16)
    for j in range(chips - 1):
        to_owner(j).wait_send()
    for j in range(max(chips - 2, 0), chips):
        to_partner(j).wait_send()
    for own in (False, True):
        for copy in stores(chips - 1, own):
            copy.wait()


def unit_block(rows_in, rows_grad, gate_rows, up_rows, down_rows, owners, number):
    total, width = rows_in.shape
    units = gate_rows.shape[0]
    rows = total // owners
    chips = owners // 2
    hbm = pl.BlockSpec(memory_space=pl.ANY)
    vmem = pl.BlockSpec(memory_space=pltpu.VMEM)
    kept = jax.ShapeDtypeStruct((total, units), bf16)
    return pl.pallas_call(
        unit_kernel,
        in_specs=[hbm, hbm, vmem, vmem, vmem],
        out_specs=[vmem, hbm, hbm, hbm, hbm],
        out_shape=[
            jax.ShapeDtypeStruct((rows, width), bf16),
            jax.ShapeDtypeStruct((total, width), bf16),
            kept,
            kept,
            kept,
        ],
        scratch_shapes=[
            pltpu.VMEM((2, rows, width), bf16),
            pltpu.VMEM((2, rows, width), bf16),
            pltpu.VMEM((2, rows, width), bf16),
            pltpu.VMEM((2, 3, rows, units), bf16),
            pltpu.VMEM((2, rows, width), bf16),
            pltpu.VMEM((chips, rows, width), bf16),
            pltpu.VMEM((chips, rows, width), bf16),
            pltpu.VMEM((chips - 1, rows, width), bf16),
            pltpu.SemaphoreType.DMA((2, 2)),
            pltpu.SemaphoreType.DMA((4, 2)),
            pltpu.SemaphoreType.DMA((2,)),
            pltpu.SemaphoreType.DMA((chips,)),
            pltpu.SemaphoreType.DMA((chips,)),
            pltpu.SemaphoreType.DMA((chips,)),
        ],
        compiler_params=pltpu.CompilerParams(
            collective_id=number, has_side_effects=True, vmem_limit_bytes=67043328
        ),
        cost_estimate=pl.CostEstimate(
            flops=6 * 2 * total * units * width,
            bytes_accessed=2 * (3 * total * width + 3 * total * units + 3 * units * width),
            transcendentals=total * units,
        ),
        name="unit_block",
    )(rows_in, rows_grad, gate_rows, up_rows, down_rows)


def line_kernel(own_ref, *refs):
    all_ref, bounce, up_send, up_recv, down_send, down_recv, local_sem = refs[-7:]
    me = lax.axis_index("expert")
    count = all_ref.shape[0]
    below = jnp.maximum(me - 1, 0)
    above = jnp.minimum(me + 1, count - 1)
    barrier = pltpu.get_barrier_semaphore()

    @pl.when(me > 0)
    def _():
        pl.semaphore_signal(barrier, inc=1, device_id={"expert": below}, device_id_type=MESH)

    @pl.when(me < count - 1)
    def _():
        pl.semaphore_signal(barrier, inc=1, device_id={"expert": above}, device_id_type=MESH)

    inner = (me > 0) & (me < count - 1)

    @pl.when(inner)
    def _():
        pl.semaphore_wait(barrier, 2)

    @pl.when(jnp.logical_not(inner))
    def _():
        pl.semaphore_wait(barrier, 1)

    def upward(step, block):
        return pltpu.make_async_remote_copy(
            src_ref=own_ref if step == 0 else all_ref.at[block],
            dst_ref=all_ref.at[block],
            send_sem=up_send.at[step],
            recv_sem=up_recv.at[step],
            device_id={"expert": above},
            device_id_type=MESH,
        )

    def downward(step, block):
        return pltpu.make_async_remote_copy(
            src_ref=own_ref if step == 0 else all_ref.at[block],
            dst_ref=all_ref.at[block],
            send_sem=down_send.at[step],
            recv_sem=down_recv.at[step],
            device_id={"expert": below},
            device_id_type=MESH,
        )

    steps = range(count - 1)
    for step in steps:
        if step > 0:

            @pl.when(me - step >= 0)
            def _():
                upward(step - 1, jnp.maximum(me - step, 0)).wait_recv()

            @pl.when(me + step < count)
            def _():
                downward(step - 1, jnp.minimum(me + step, count - 1)).wait_recv()

        @pl.when((me - step >= 0) & (me < count - 1))
        def _():
            upward(step, jnp.maximum(me - step, 0)).start()

        @pl.when((me + step < count) & (me > 0))
        def _():
            downward(step, jnp.minimum(me + step, count - 1)).start()

        if step == 0:
            copy = pltpu.make_async_copy(own_ref, bounce, local_sem.at[0])
            copy.start()
            copy.wait()
            copy = pltpu.make_async_copy(bounce, all_ref.at[me], local_sem.at[1])
            copy.start()
            copy.wait()

    @pl.when(me == count - 1)
    def _():
        upward(count - 2, 0).wait_recv()

    @pl.when(me == 0)
    def _():
        downward(count - 2, count - 1).wait_recv()

    for step in steps:

        @pl.when((me - step >= 0) & (me < count - 1))
        def _():
            upward(step, jnp.maximum(me - step, 0)).wait_send()

        @pl.when((me + step < count) & (me > 0))
        def _():
            downward(step, jnp.minimum(me + step, count - 1)).wait_send()


def line_gather(own, experts, number, *waits):
    hbm = pl.BlockSpec(memory_space=pl.ANY)
    steps = (max(experts - 1, 1),)
    return pl.pallas_call(
        line_kernel,
        in_specs=[hbm] * (1 + len(waits)),
        out_specs=hbm,
        out_shape=jax.ShapeDtypeStruct((experts,) + own.shape, own.dtype),
        scratch_shapes=[pltpu.VMEM(own.shape, own.dtype)]
        + [pltpu.SemaphoreType.DMA(steps)] * 4
        + [pltpu.SemaphoreType.DMA((2,))],
        compiler_params=pltpu.CompilerParams(collective_id=number, has_side_effects=True),
        cost_estimate=pl.CostEstimate(
            flops=0, bytes_accessed=4 * experts * own.size, transcendentals=0
        ),
        name="line_gather",
    )(own, *waits)


def hold(value, *others):
    for other in others:
        last = other[(slice(-1, None),) * other.ndim].reshape(())
        value = value + jnp.minimum(jnp.abs(last), 0).astype(value.dtype)
    return value


def exchange(rows):
    return lax.all_to_all(rows, "expert", split_axis=0, concat_axis=0, tiled=True)


def hop_sum(parts, place, count):
    total = lax.dynamic_index_in_dim(parts, place, 0, keepdims=False).astype(f32)
    got = []
    for hop in range(1, count):
        ring = [(i, (i + hop) % count) for i in range(count)]
        piece = lax.dynamic_index_in_dim(parts, (place + hop) % count, 0, keepdims=False)
        got.append(lax.ppermute(piece, "expert", ring))
    for piece in got:
        total = total + piece.astype(f32)
    return total


def after(value, *others):
    return lax.optimization_barrier((value,) + others)[0]


def plane_sum(terms):
    return lax.psum_scatter(terms, "dp", scatter_dimension=0, tiled=True)


def hops(rows, sign):
    count = rows.shape[0]
    pieces = [rows[0]]
    for hop in range(1, count):
        ring = [(i, (i + sign * hop) % count) for i in range(count)]
        pieces.append(lax.ppermute(rows[hop], "expert", ring))
    return jnp.stack(pieces)


def spread(rows, axes, count):
    copies = jnp.broadcast_to(rows[None], (count,) + rows.shape)
    return lax.all_to_all(copies, axes, split_axis=0, concat_axis=0, tiled=True)


def layer(
    layer_input,
    cotangent,
    cont_ids,
    attn_routes,
    attn_gates,
    mlp_routes,
    mlp_gates,
    gain_attn,
    gain_mlp,
    kv_weight,
    query_weight,
    output_weight,
    mlp_weight,
):
    experts = lax.axis_size("expert")
    owners = lax.axis_size("dp")
    expert_id = lax.axis_index("expert")
    tok_dev, width = layer_input.shape
    per_token = attn_routes.shape[1]
    capacity = tok_dev * per_token * 9 // (8 * experts)
    slots = -(-capacity // 8) * 8
    slot_total = experts * slots
    group = cont_ids.shape[0]
    features = query_weight.shape[2]
    expert_ids = jnp.arange(experts, dtype=jnp.int32)
    slot_ids = jnp.arange(slots, dtype=jnp.int32)

    kv_part = line_gather(kv_weight, experts, 6).reshape(-1, kv_weight.shape[1])
    kv_full = lax.all_gather(kv_part, "dp", axis=0, tiled=True)
    x_all = line_gather(layer_input, experts, 7, kv_part).reshape(group, width)
    query_full = lax.all_gather(query_weight[:, 0, :], "dp", axis=0, tiled=True)
    output_full = lax.all_gather(output_weight[:, 0, :], "dp", axis=0, tiled=True)
    gains = jnp.concatenate([gain_attn, gain_mlp])[None]
    gains = spread(gains, ("dp", "expert"), owners * experts)
    part_size = gain_attn.shape[0]
    gains = gains.reshape(owners * experts, 2, part_size)
    gain_one = gains[:, 0].reshape(-1).astype(f32)
    gain_two = gains[:, 1].reshape(-1).astype(f32)

    hop_ids = (expert_id + expert_ids) % experts
    mlp_hot = mlp_routes.T[:, None, :] == hop_ids[None, :, None]
    mlp_mine = jnp.any(mlp_hot, axis=0)
    mlp_rank = before_counts(mlp_mine)
    mlp_pick = mlp_mine[:, None, :] & (mlp_rank[:, None, :] == slot_ids[None, :, None])
    mlp_gate_tok = jnp.sum(jnp.where(mlp_hot, mlp_gates.T[:, None, :], 0.0), axis=0)
    mlp_slot_gate = jnp.sum(jnp.where(mlp_pick, mlp_gate_tok[:, None, :], 0.0), axis=2)
    mlp_pick_low = mlp_pick.astype(bf16).reshape(slot_total, tok_dev)
    mlp_choice = [
        (mlp_pick & mlp_hot[k][:, None, :]).astype(bf16).reshape(slot_total, tok_dev)
        for k in range(per_token)
    ]
    mlp_back = jnp.concatenate(mlp_choice, axis=1)

    attn_all = attn_routes.reshape(experts, tok_dev, per_token)
    own_mine = jnp.any(attn_all == expert_id, axis=2)
    own_rank = before_counts(own_mine)
    own_pick = own_mine[:, None, :] & (own_rank[:, None, :] == slot_ids[None, :, None])
    own_low = own_pick.astype(bf16)
    places_row, positions_row = token_positions(cont_ids)

    def slot_value(row):
        return jnp.sum(
            jnp.where(own_pick, row.reshape(experts, 1, tok_dev), 0), axis=2, dtype=jnp.int32
        )

    slot_place = slot_value(places_row) + jnp.where(
        jnp.any(own_pick, axis=2), 0, expert_ids[:, None] * tok_dev
    )
    slot_cont = slot_value(cont_ids)
    slot_pos = slot_value(positions_row)
    attn_mine_routes = lax.dynamic_slice_in_dim(attn_routes, expert_id * tok_dev, tok_dev)
    attn_hot = attn_mine_routes.T[:, None, :] == expert_ids[None, :, None]
    attn_mine = jnp.any(attn_hot, axis=0)
    attn_rank = before_counts(attn_mine)
    attn_pick = attn_mine[:, None, :] & (attn_rank[:, None, :] == slot_ids[None, :, None])
    attn_gate_tok = jnp.sum(jnp.where(attn_hot, attn_gates.T[:, None, :], 0.0), axis=0)
    attn_slot_gate = jnp.sum(jnp.where(attn_pick, attn_gate_tok[:, None, :], 0.0), axis=2)
    attn_pick_low = attn_pick.astype(bf16).reshape(slot_total, tok_dev)
    attn_back = jnp.concatenate(
        [
            (attn_pick & attn_hot[k][:, None, :]).astype(bf16).reshape(slot_total, tok_dev)
            for k in range(per_token)
        ],
        axis=1,
    )
    kcos, ksin = rope_tables(positions_row)
    qcos, qsin = rope_tables(slot_pos.reshape(-1))

    cot_rows = dot_nn(mlp_pick_low, cotangent).reshape(experts, slots, width)
    send_grad = (mlp_slot_gate[:, :, None] * cot_rows).astype(bf16)
    steps = slots // 8
    cuts = [0, 8 * max(int(steps * MLP_FIRST), 1), slots]
    pieces = list(zip(cuts[:-1], cuts[1:]))

    def to_plane(rows):
        return lax.all_gather(rows.reshape(-1, width), "dp", axis=0, tiled=True)

    got_grad = hops(hold(send_grad, x_all), 1)

    input_f32 = x_all.astype(f32)
    normed_all, _ = rms_parts(input_f32)
    hidden_all = (normed_all * gain_one).astype(bf16)
    query_rows = lax.dot_general(
        own_low,
        hidden_all.reshape(experts, tok_dev, width),
        (((2,), (1,)), ((0,), (0,))),
        preferred_element_type=f32,
    ).astype(bf16).reshape(slot_total, width)
    query_low = project(
        query_rows, query_full, qcos, qsin, features, slot_total
    ).reshape(experts, slots, features)
    kv_low = project(hidden_all, kv_full, kcos, ksin, features, tok_dev)
    got_grad = hold(got_grad, kv_low)
    plane_grad = [to_plane(got_grad[:, low:high, :]) for low, high in pieces]
    slot_place3 = slot_place[:, :, None]
    slot_cont3 = slot_cont[:, :, None]
    key_cont = cont_ids[None, :]
    attn_low, lse = attend(query_low, kv_low, slot_place3, slot_cont3, key_cont, tok_dev)
    attn_flat = attn_low.reshape(slot_total, features)
    result_low = dot_nn(attn_flat, output_full).astype(bf16)
    result_back = exchange(result_low.reshape(experts, slots, width)).reshape(slot_total, width)
    result_tok = dot_tn(attn_back, result_back)
    own_f32 = layer_input.astype(f32)
    residual = own_f32
    for k in range(per_token):
        residual = residual + attn_gates[:, k : k + 1] * result_tok[k * tok_dev : (k + 1) * tok_dev]
    normed_two, scale_two = rms_parts(residual)
    second_low = (normed_two * gain_two).astype(bf16)

    send_in = dot_nn(mlp_pick_low, second_low).astype(bf16).reshape(experts, slots, width)
    gate_rows, up_rows, down_rows = (mlp_weight[:, 0, j, :] for j in range(3))
    plane_in = [to_plane(hops(send_in[:, low:high, :], 1)) for low, high in pieces]
    kept, out_parts, in_parts = [], [], []
    for number, (rows_in, rows_grad) in enumerate(zip(plane_in, plane_grad)):
        in_part, out_part, *keep = unit_block(
            rows_in, rows_grad, gate_rows, up_rows, down_rows, owners, number
        )
        in_parts.append(in_part)
        out_parts.append(out_part)
        kept.append(keep)

    def join(parts):
        back = []
        for part, (low, high) in zip(parts, pieces):
            back.append(hops(part.reshape(experts, high - low, width), -1))
        return jnp.concatenate(back, axis=1).reshape(slot_total, width)

    in_back = join(in_parts)
    grad_mlp = [dot_tn(k, r) for k, r in zip(kept[0], (plane_in[0], plane_in[0], plane_grad[0]))]
    grad_second = dot_tn(mlp_pick_low, after(in_back, *grad_mlp))
    cot_f32 = cotangent.astype(f32)
    grad_resid = cot_f32 + rms_back(grad_second, normed_two, scale_two, gain_two)

    cot_slots = dot_nn(attn_pick_low, grad_resid.astype(bf16)).reshape(experts, slots, width)
    send_cot = (attn_slot_gate[:, :, None] * cot_slots).astype(bf16)
    grad_mlp = [
        g + dot_tn(k, r)
        for g, k, r in zip(grad_mlp, kept[1], (plane_in[1], plane_in[1], plane_grad[1]))
    ]
    grad_mlp_weight = jnp.stack(grad_mlp, axis=1)[:, None, :, :]
    grad_result = after(exchange(send_cot), *grad_mlp).reshape(slot_total, width)
    output_term = dot_tn(attn_flat, grad_result).astype(bf16)
    grad_output_w = plane_sum(output_term)
    grad_attn = dot_nt(after(grad_result, output_term), output_full).astype(bf16)
    out_back = join([plane_sum(after(part, *in_parts)) for part in out_parts])
    attend_again = attend_back
    grad_query, grad_keys, grad_values = attend_again(
        query_low,
        kv_low,
        grad_attn.reshape(experts, slots, features),
        lse,
        slot_place3,
        slot_cont3,
        key_cont,
        qcos.reshape(experts, slots, HEAD),
        qsin.reshape(experts, slots, HEAD),
        kcos,
        ksin,
        tok_dev,
    )
    grad_query = grad_query.reshape(slot_total, features)
    mixed_tok = dot_tn(mlp_back, out_back)
    final = residual
    for k in range(per_token):
        final = final + mlp_gates[:, k : k + 1] * mixed_tok[k * tok_dev : (k + 1) * tok_dev]
    output = final.astype(bf16)

    grad_keys_w = dot_tn(hidden_all, grad_keys).astype(bf16)
    grad_values_w = dot_tn(hidden_all, grad_values).astype(bf16)
    grad_kv_w = jnp.concatenate([grad_keys_w, grad_values_w], axis=1)
    grad_query = hold(grad_query, grad_keys_w, grad_values_w)
    grad_kv_w = plane_sum(grad_kv_w)
    grad_rows = dot_nt(grad_query, query_full).astype(bf16)
    half = width // 2
    grad_h, grad_first = [], []
    for low in (0, half):
        span = slice(low, low + half)
        routed = lax.dot_general(
            own_low,
            grad_rows[:, span].reshape(experts, slots, half),
            (((1,), (1,)), ((0,), (0,))),
            preferred_element_type=f32,
        ).reshape(group, half)
        part = (
            dot_nt(grad_keys, kv_full[span, :features])
            + dot_nt(grad_values, kv_full[span, features:])
            + routed
        )
        grad_h.append(part)
        grad_first.append(
            hop_sum(part.astype(bf16).reshape(experts, tok_dev, half), expert_id, experts)
        )
    query_term = dot_tn(query_rows, hold(grad_query, grad_h[1])).astype(bf16)
    grad_query_w = plane_sum(query_term)
    grad_output_w, grad_query_w = hold(grad_output_w, grad_kv_w), hold(grad_query_w, grad_kv_w)
    grad_kv_w = hop_sum(grad_kv_w.reshape(experts, -1, 2 * features), expert_id, experts)
    grad_h = lax.optimization_barrier(tuple(grad_h))
    grad_gain_one = [
        jnp.sum(part * normed_all[:, low : low + half], axis=0)
        for part, low in zip(grad_h, (0, half))
    ]
    grad_gain_two = jnp.sum(grad_second * normed_two, axis=0)
    grad_first = jnp.concatenate(grad_first, axis=1)
    normed_one, scale_one = rms_parts(own_f32)
    grad_input = grad_resid + rms_back(grad_first, normed_one, scale_one, gain_one)

    gain_rows = jnp.concatenate(
        [
            jnp.concatenate(grad_gain_one).reshape(owners * experts, part_size),
            grad_gain_two.reshape(owners * experts, part_size),
        ],
        axis=1,
    )
    gain_rows = lax.all_to_all(
        gain_rows[:, None, :], ("dp", "expert"), split_axis=0, concat_axis=0, tiled=True
    )
    gain_rows = jnp.sum(gain_rows, axis=(0, 1))
    grad_gain_attn, grad_gain_mlp = gain_rows[:part_size], gain_rows[part_size:]
    return (
        output,
        grad_input,
        grad_gain_attn,
        grad_gain_mlp,
        grad_kv_w,
        grad_query_w.astype(f32)[:, None, :],
        grad_output_w.astype(f32)[:, None, :],
        grad_mlp_weight,
    )


def solution(mesh):
    placed = (
        P(("dp", "expert"), None),
        P(("dp", "expert"), None),
        P("dp"),
        P("dp", None),
        P(("dp", "expert"), None),
        P(("dp", "expert"), None),
        P(("dp", "expert"), None),
        P(("dp", "expert")),
        P(("dp", "expert")),
        P(("dp", "expert"), None),
        P("dp", "expert", None),
        P("dp", "expert", None),
        P("dp", "expert", None, None),
    )
    return jax.shard_map(
        layer,
        mesh=mesh,
        in_specs=placed,
        out_specs=(
            P(("dp", "expert"), None),
            P(("dp", "expert"), None),
            P(("dp", "expert")),
            P(("dp", "expert")),
            P(("dp", "expert"), None),
            P("dp", "expert", None),
            P("dp", "expert", None),
            P("dp", "expert", None, None),
        ),
        check_vma=False,
    )
```

```python
import functools
import math

import jax
import jax.numpy as jnp
from jax import lax
from jax.experimental import pallas as pl
from jax.experimental.pallas import tpu as pltpu
from jax.sharding import PartitionSpec as P


HEAD = 128
PROMPT = 1024
CONTS = 2
GROUP_TOK = 1280
MLP_FIRST = 0.5

norm_eps = 1e-06
rope_base = 10000.0
neg_fill = -1e30
log2e = 1.4426950408889634
MESH = pl.DeviceIdType.MESH
contract_last = (((1,), (1,)), ((), ()))
contract_first = (((0,), (0,)), ((), ()))
f32 = jnp.float32
bf16 = jnp.bfloat16


def rope_tables(positions):
    half_size = HEAD // 2
    freq_steps = jnp.arange(half_size, dtype=f32)
    inverse_freq = jnp.exp(-math.log(rope_base) * 2.0 * freq_steps / HEAD)
    angles = positions.astype(f32)[:, None] * inverse_freq[None, :]
    cosine, sine = jnp.cos(angles), jnp.sin(angles)
    return (
        jnp.concatenate([cosine, cosine], axis=1),
        jnp.concatenate([-sine, sine], axis=1),
    )


def token_positions(cont_ids):
    row_count = cont_ids.shape[0]
    group_count = row_count // GROUP_TOK
    places = jnp.arange(row_count, dtype=jnp.int32) % GROUP_TOK
    labels = jnp.arange(CONTS + 1, dtype=jnp.int32)
    one_hot = (cont_ids[:, None] == labels[None, :]).astype(jnp.int32)
    counts = jnp.sum(one_hot.reshape(group_count, GROUP_TOK, CONTS + 1), axis=1)
    starts = jnp.cumsum(counts, axis=1) - counts
    starts_tok = jnp.broadcast_to(starts[:, None, :], (group_count, GROUP_TOK, CONTS + 1)).reshape(
        row_count, CONTS + 1
    )
    start_of = jnp.sum(starts_tok * one_hot, axis=1)
    return (places, places - start_of + PROMPT * (cont_ids > 0).astype(jnp.int32))


def rms_parts(values):
    row_scale = lax.rsqrt(jnp.mean(values * values, axis=-1, keepdims=True) + norm_eps)
    return (values * row_scale, row_scale)


def rms_back(grad_out, normed, row_scale, gain_vec):
    through = grad_out * gain_vec
    grad_in = row_scale * (through - normed * jnp.mean(through * normed, axis=-1, keepdims=True))
    return grad_in


def dot_nt(left, right):
    return lax.dot_general(left, right, contract_last, preferred_element_type=f32)


def dot_tn(left, right):
    return lax.dot_general(left, right, contract_first, preferred_element_type=f32)


def dot_nn(left, right):
    return jnp.dot(left, right, preferred_element_type=f32)


def before_counts(flags):
    count = flags.shape[-1]
    steps = jnp.arange(count, dtype=jnp.int32)
    earlier = (steps[:, None] < steps[None, :]).astype(bf16)
    return jnp.dot(flags.astype(bf16), earlier, preferred_element_type=f32).astype(jnp.int32)


def project_kernel(rope_blocks, tile, x_ref, w_ref, cos_ref, sin_ref, out_ref):
    rows = x_ref.shape[0]
    turn = pl.program_id(0) < rope_blocks
    for start in range(0, rows, tile):
        span = pl.ds(start, tile)
        product = jnp.dot(x_ref[span, :], w_ref[...], preferred_element_type=f32)

        @pl.when(turn)
        def _():
            cosine, sine = cos_ref[span, :], sin_ref[span, :]
            for col in range(0, product.shape[1], HEAD):
                piece = product[:, col : col + HEAD]
                turned = piece * cosine + pltpu.roll(piece, HEAD // 2, 1) * sine
                out_ref[span, col : col + HEAD] = turned.astype(bf16)

        @pl.when(jnp.logical_not(turn))
        def _():
            out_ref[span, :] = product.astype(bf16)


def project(rows, weight, cosine, sine, rope_cols, tile):
    count, width = rows.shape
    cols = weight.shape[1]
    block = 512
    return pl.pallas_call(
        functools.partial(project_kernel, rope_cols // block, tile),
        grid=(cols // block,),
        in_specs=[
            pl.BlockSpec((count, width), lambda i: (0, 0)),
            pl.BlockSpec((width, block), lambda i: (0, i)),
            pl.BlockSpec((count, HEAD), lambda i: (0, 0)),
            pl.BlockSpec((count, HEAD), lambda i: (0, 0)),
        ],
        out_specs=pl.BlockSpec((count, block), lambda i: (0, i)),
        out_shape=jax.ShapeDtypeStruct((count, cols), bf16),
        cost_estimate=pl.CostEstimate(
            flops=2 * count * width * cols,
            bytes_accessed=2 * (count * width + width * cols + count * cols),
            transcendentals=0,
        ),
    )(rows, weight, cosine, sine)


def key_spans(blocks, tokens, keys):
    return [min(-(-(tokens * (s + 1)) // 128) * 128, keys) for s in range(blocks)]


def fill_bias(bias, place_ref, cont_ref, kcont_ref):
    blocks, slots, keys = bias.shape
    kplace = lax.broadcasted_iota(jnp.int32, (slots, keys), 1)
    kcont = kcont_ref[...]
    for s in range(blocks):
        allowed = (kplace <= place_ref[s]) & ((kcont == 0) | (kcont == cont_ref[s]))
        bias[s] = jnp.where(allowed, 0.0, neg_fill)


def attend_kernel(
    spans, low, q_ref, k_ref, v_ref, place_ref, cont_ref, kcont_ref, out_ref, lse_ref, bias
):
    high = low + out_ref.shape[1]

    @pl.when(pl.program_id(0) == 0)
    def _():
        fill_bias(bias, place_ref, cont_ref, kcont_ref)

    scale2 = log2e / math.sqrt(HEAD)
    for s, span in enumerate(spans):
        scores = dot_nt(q_ref[s, low:high, :], k_ref[:span, :]) * scale2 + bias[s, :, :span]
        peak = jnp.max(scores, axis=1, keepdims=True)
        weights = jnp.exp2(scores - peak)
        total = jnp.sum(weights, axis=1, keepdims=True)
        mixed = dot_nn(weights.astype(bf16), v_ref[:span, :])
        out_ref[s] = (mixed / total).astype(bf16)
        lse_ref[s] = jnp.broadcast_to(peak + jnp.log2(total), lse_ref.shape[1:])


def attend(query, kv_low, place, cont, kcont, tokens, low, high):
    blocks, total, features = query.shape
    slots = high - low
    keys = kv_low.shape[0]
    heads = features // HEAD
    spans = key_spans(blocks, tokens, keys)
    work = 2 * 2 * slots * sum(spans) * HEAD * heads
    qspec = pl.BlockSpec((blocks, total, HEAD), lambda h: (0, 0, h))
    ospec = pl.BlockSpec((blocks, slots, HEAD), lambda h: (0, 0, h))
    whole = pl.BlockSpec((blocks, slots, 1), lambda h: (0, 0, 0))
    return pl.pallas_call(
        functools.partial(attend_kernel, spans, low),
        grid=(heads,),
        in_specs=[
            qspec,
            pl.BlockSpec((keys, HEAD), lambda h: (0, h)),
            pl.BlockSpec((keys, HEAD), lambda h: (0, heads + h)),
            whole,
            whole,
            pl.BlockSpec((1, keys), lambda h: (0, 0)),
        ],
        out_specs=[ospec, ospec],
        out_shape=[
            jax.ShapeDtypeStruct((blocks, slots, features), bf16),
            jax.ShapeDtypeStruct((blocks, slots, features), f32),
        ],
        scratch_shapes=[pltpu.VMEM((blocks, slots, keys), f32)],
        cost_estimate=pl.CostEstimate(
            flops=work,
            bytes_accessed=2 * query.size + 2 * kv_low.size + 6 * blocks * slots * features,
            transcendentals=slots * sum(spans) * heads,
        ),
        name="attend",
    )(query, kv_low, kv_low, place[:, low:high], cont[:, low:high], kcont)


def attend_back_kernel(spans, low, carried, *refs):
    q_ref, k_ref, v_ref, g_ref, lse_ref, place_ref, cont_ref, kcont_ref = refs[:8]
    qcos_ref, qsin_ref, kcos_ref, ksin_ref = refs[8:12]
    refs = refs[12:]
    if carried:
        old_dq_ref, old_dk_ref, old_dv_ref = refs[:3]
        refs = refs[3:]
    dq_ref, dk_ref, dv_ref, bias, dk_sum, dv_sum = refs
    slots = g_ref.shape[1]
    high = low + slots

    @pl.when(pl.program_id(0) == 0)
    def _():
        fill_bias(bias, place_ref, cont_ref, kcont_ref)

    scale = 1.0 / math.sqrt(HEAD)
    scale2 = log2e * scale
    last = len(spans) - 1
    for s in range(last, -1, -1):
        span = spans[s]
        query, grad = q_ref[s, low:high, :], g_ref[s]
        keys = k_ref[:span, :]
        scores = dot_nt(query, keys) * scale2 + bias[s, :, :span]
        prob = jnp.exp2(scores - lse_ref[s][:, :1])
        grad_prob = dot_nt(grad, v_ref[:span, :])
        inner = jnp.sum(prob * grad_prob, axis=1, keepdims=True)
        grad_scores = (prob * (grad_prob - inner)).astype(bf16)
        dq = dot_nn(grad_scores, keys) * scale
        dq = dq * qcos_ref[s] - pltpu.roll(dq, HEAD // 2, 1) * qsin_ref[s]
        if carried:
            dq_ref[s, :low, :] = old_dq_ref[s]
            dq_ref[s, low:high, :] = dq.astype(bf16)
        else:
            dq_ref[s] = dq.astype(bf16)
        dk = dot_tn(grad_scores, query)
        dv = dot_tn(prob.astype(bf16), grad)
        if s < last:
            dk_sum[:span, :] += dk
            dv_sum[:span, :] += dv
        elif carried:
            dk_sum[...] = old_dk_ref[...] + dk
            dv_sum[...] = old_dv_ref[...] + dv
        else:
            dk_sum[...] = dk
            dv_sum[...] = dv
    if carried:
        dk = dk_sum[...] * scale
        dk = dk * kcos_ref[...] - pltpu.roll(dk, HEAD // 2, 1) * ksin_ref[...]
        dk_ref[...] = dk.astype(bf16)
        dv_ref[...] = dv_sum[...].astype(bf16)
    else:
        dk_ref[...] = dk_sum[...]
        dv_ref[...] = dv_sum[...]


def attend_back(
    query, kv_low, grad, lse, place, cont, kcont, qcos, qsin, kcos, ksin, tokens, low, old=()
):
    blocks, total, features = query.shape
    slots = grad.shape[1]
    high = low + slots
    keys = kv_low.shape[0]
    heads = features // HEAD
    spans = key_spans(blocks, tokens, keys)
    work = 5 * 2 * slots * sum(spans) * HEAD * heads
    carried = bool(old)

    def by_head(rows):
        return pl.BlockSpec((blocks, rows, HEAD), lambda h: (0, 0, h))

    kspec = pl.BlockSpec((keys, HEAD), lambda h: (0, h))
    whole = pl.BlockSpec((blocks, slots, 1), lambda h: (0, 0, 0))
    qtab = pl.BlockSpec((blocks, slots, HEAD), lambda h: (0, 0, 0))
    ktab = pl.BlockSpec((keys, HEAD), lambda h: (0, 0))
    kept_type = bf16 if carried else f32
    return pl.pallas_call(
        functools.partial(attend_back_kernel, spans, low, carried),
        grid=(heads,),
        in_specs=[
            by_head(total),
            kspec,
            pl.BlockSpec((keys, HEAD), lambda h: (0, heads + h)),
            by_head(slots),
            by_head(slots),
            whole,
            whole,
            pl.BlockSpec((1, keys), lambda h: (0, 0)),
            qtab,
            qtab,
            ktab,
            ktab,
        ]
        + ([by_head(low), kspec, kspec] if carried else []),
        out_specs=[by_head(total if carried else slots), kspec, kspec],
        out_shape=[
            jax.ShapeDtypeStruct((blocks, total if carried else slots, features), bf16),
            jax.ShapeDtypeStruct((keys, features), kept_type),
            jax.ShapeDtypeStruct((keys, features), kept_type),
        ],
        scratch_shapes=[
            pltpu.VMEM((blocks, slots, keys), f32),
            pltpu.VMEM((keys, HEAD), f32),
            pltpu.VMEM((keys, HEAD), f32),
        ],
        cost_estimate=pl.CostEstimate(
            flops=work,
            bytes_accessed=10 * blocks * slots * features + 8 * kv_low.size,
            transcendentals=slots * sum(spans) * heads,
        ),
        name="attend_back",
    )(
        query,
        kv_low,
        kv_low,
        grad,
        lse,
        place[:, low:high],
        cont[:, low:high],
        kcont,
        qcos[:, low:high],
        qsin[:, low:high],
        kcos,
        ksin,
        *old,
    )


def unit_kernel(
    x_hbm,
    g_hbm,
    gate_ref,
    up_ref,
    down_ref,
    in_ref,
    out_hbm,
    gg_hbm,
    gu_hbm,
    hid_hbm,
    xbuf,
    gbuf,
    obuf,
    kbuf,
    psend,
    precv,
    ssend,
    frecv,
    load_sem,
    store_sem,
    psend_sem,
    precv_sem,
    ssend_sem,
    frecv_sem,
):
    rows = xbuf.shape[1]
    chips = ssend.shape[0]
    me = lax.axis_index("dp")
    chip = me // 2
    core = me % 2
    partner = me + 1 - 2 * core

    def peer(hop):
        return {"dp": (chip + hop) % chips * 2 + core}

    barrier = pltpu.get_barrier_semaphore()
    pl.semaphore_signal(barrier, inc=1, device_id={"dp": partner}, device_id_type=MESH)
    for hop in range(1, chips):
        pl.semaphore_signal(barrier, inc=1, device_id=peer(hop), device_id_type=MESH)
    pl.semaphore_wait(barrier, chips)

    def block_rows(j, own):
        dest = (chip + chips - 1 - j) % chips
        block = dest * 2 + (core if own else 1 - core)
        return pl.ds(pl.multiple_of(block * rows, 8), rows)

    def loads(j, own):
        span, slot = block_rows(j, own), int(own)
        return [
            pltpu.make_async_copy(x_hbm.at[span], xbuf.at[slot], load_sem.at[0, slot]),
            pltpu.make_async_copy(g_hbm.at[span], gbuf.at[slot], load_sem.at[1, slot]),
        ]

    def stores(j, own):
        span, slot = block_rows(j, own), int(own)
        return [pltpu.make_async_copy(obuf.at[slot], out_hbm.at[span], store_sem.at[0, slot])] + [
            pltpu.make_async_copy(kbuf.at[slot, i], dst.at[span], store_sem.at[1 + i, slot])
            for i, dst in enumerate((gg_hbm, gu_hbm, hid_hbm))
        ]

    def to_partner(j):
        return pltpu.make_async_remote_copy(
            src_ref=psend.at[j % 2],
            dst_ref=precv.at[j],
            send_sem=psend_sem.at[j % 2],
            recv_sem=precv_sem.at[j],
            device_id={"dp": partner},
            device_id_type=MESH,
        )

    def to_owner(j):
        return pltpu.make_async_remote_copy(
            src_ref=ssend.at[j],
            dst_ref=frecv.at[j],
            send_sem=ssend_sem.at[j],
            recv_sem=frecv_sem.at[j],
            device_id=peer(chips - 1 - j),
            device_id_type=MESH,
        )

    def compute(j, own):
        slot = int(own)
        for copy in loads(j, own):
            copy.wait()
        rows_in, rows_grad = xbuf[slot], gbuf[slot]
        gate_val = dot_nt(rows_in, gate_ref[...])
        up_val = dot_nt(rows_in, up_ref[...])
        grad_hidden = dot_nt(rows_grad, down_ref[...])
        sigma = jax.nn.sigmoid(gate_val)
        active = gate_val * sigma
        hidden = (active * up_val).astype(bf16)
        grad_gate = (grad_hidden * up_val * sigma * (1.0 + gate_val * (1.0 - sigma))).astype(bf16)
        grad_up = (grad_hidden * active).astype(bf16)

        @pl.when(j > 0)
        def _():
            for copy in stores(j - 1, own):
                copy.wait()

        kbuf[slot, 0] = grad_gate
        kbuf[slot, 1] = grad_up
        kbuf[slot, 2] = hidden
        obuf[slot] = dot_nn(hidden, down_ref[...]).astype(bf16)
        for copy in stores(j, own):
            copy.start()
        return dot_nn(grad_gate, gate_ref[...]) + dot_nn(grad_up, up_ref[...])

    for copy in loads(0, False):
        copy.start()

    def step(j, carry):
        for copy in loads(j, True):
            copy.start()
        term = compute(j, False)

        @pl.when(j > 1)
        def _():
            to_partner(j - 2).wait_send()

        psend[j % 2] = term.astype(bf16)
        to_partner(j).start()

        @pl.when(j < chips - 1)
        def _():
            for copy in loads(j + 1, False):
                copy.start()

        term = compute(j, True)
        to_partner(j).wait_recv()
        ssend[j] = (term + precv[j].astype(f32)).astype(bf16)

        @pl.when(j < chips - 1)
        def _():
            to_owner(j).start()

        return carry

    lax.fori_loop(0, chips, step, 0)
    total = ssend[chips - 1].astype(f32)
    for j in range(chips - 1):
        to_owner(j).wait_recv()
        total = total + frecv[j].astype(f32)
    in_ref[...] = total.astype(bf16)
    for j in range(chips - 1):
        to_owner(j).wait_send()
    for j in range(max(chips - 2, 0), chips):
        to_partner(j).wait_send()
    for own in (False, True):
        for copy in stores(chips - 1, own):
            copy.wait()


def unit_block(rows_in, rows_grad, gate_rows, up_rows, down_rows, owners, number):
    total, width = rows_in.shape
    units = gate_rows.shape[0]
    rows = total // owners
    chips = owners // 2
    hbm = pl.BlockSpec(memory_space=pl.ANY)
    vmem = pl.BlockSpec(memory_space=pltpu.VMEM)
    kept = jax.ShapeDtypeStruct((total, units), bf16)
    return pl.pallas_call(
        unit_kernel,
        in_specs=[hbm, hbm, vmem, vmem, vmem],
        out_specs=[vmem, hbm, hbm, hbm, hbm],
        out_shape=[
            jax.ShapeDtypeStruct((rows, width), bf16),
            jax.ShapeDtypeStruct((total, width), bf16),
            kept,
            kept,
            kept,
        ],
        scratch_shapes=[
            pltpu.VMEM((2, rows, width), bf16),
            pltpu.VMEM((2, rows, width), bf16),
            pltpu.VMEM((2, rows, width), bf16),
            pltpu.VMEM((2, 3, rows, units), bf16),
            pltpu.VMEM((2, rows, width), bf16),
            pltpu.VMEM((chips, rows, width), bf16),
            pltpu.VMEM((chips, rows, width), bf16),
            pltpu.VMEM((chips - 1, rows, width), bf16),
            pltpu.SemaphoreType.DMA((2, 2)),
            pltpu.SemaphoreType.DMA((4, 2)),
            pltpu.SemaphoreType.DMA((2,)),
            pltpu.SemaphoreType.DMA((chips,)),
            pltpu.SemaphoreType.DMA((chips,)),
            pltpu.SemaphoreType.DMA((chips,)),
        ],
        compiler_params=pltpu.CompilerParams(
            collective_id=number, has_side_effects=True, vmem_limit_bytes=67043328
        ),
        cost_estimate=pl.CostEstimate(
            flops=6 * 2 * total * units * width,
            bytes_accessed=2 * (3 * total * width + 3 * total * units + 3 * units * width),
            transcendentals=total * units,
        ),
        name="unit_block",
    )(rows_in, rows_grad, gate_rows, up_rows, down_rows)


def line_kernel(own_ref, *refs):
    all_ref, bounce, up_send, up_recv, down_send, down_recv, local_sem = refs[-7:]
    me = lax.axis_index("expert")
    count = all_ref.shape[0]
    below = jnp.maximum(me - 1, 0)
    above = jnp.minimum(me + 1, count - 1)
    barrier = pltpu.get_barrier_semaphore()

    @pl.when(me > 0)
    def _():
        pl.semaphore_signal(barrier, inc=1, device_id={"expert": below}, device_id_type=MESH)

    @pl.when(me < count - 1)
    def _():
        pl.semaphore_signal(barrier, inc=1, device_id={"expert": above}, device_id_type=MESH)

    inner = (me > 0) & (me < count - 1)

    @pl.when(inner)
    def _():
        pl.semaphore_wait(barrier, 2)

    @pl.when(jnp.logical_not(inner))
    def _():
        pl.semaphore_wait(barrier, 1)

    def upward(step, block):
        return pltpu.make_async_remote_copy(
            src_ref=own_ref if step == 0 else all_ref.at[block],
            dst_ref=all_ref.at[block],
            send_sem=up_send.at[step],
            recv_sem=up_recv.at[step],
            device_id={"expert": above},
            device_id_type=MESH,
        )

    def downward(step, block):
        return pltpu.make_async_remote_copy(
            src_ref=own_ref if step == 0 else all_ref.at[block],
            dst_ref=all_ref.at[block],
            send_sem=down_send.at[step],
            recv_sem=down_recv.at[step],
            device_id={"expert": below},
            device_id_type=MESH,
        )

    steps = range(count - 1)
    for step in steps:
        if step > 0:

            @pl.when(me - step >= 0)
            def _():
                upward(step - 1, jnp.maximum(me - step, 0)).wait_recv()

            @pl.when(me + step < count)
            def _():
                downward(step - 1, jnp.minimum(me + step, count - 1)).wait_recv()

        @pl.when((me - step >= 0) & (me < count - 1))
        def _():
            upward(step, jnp.maximum(me - step, 0)).start()

        @pl.when((me + step < count) & (me > 0))
        def _():
            downward(step, jnp.minimum(me + step, count - 1)).start()

        if step == 0:
            copy = pltpu.make_async_copy(own_ref, bounce, local_sem.at[0])
            copy.start()
            copy.wait()
            copy = pltpu.make_async_copy(bounce, all_ref.at[me], local_sem.at[1])
            copy.start()
            copy.wait()

    @pl.when(me == count - 1)
    def _():
        upward(count - 2, 0).wait_recv()

    @pl.when(me == 0)
    def _():
        downward(count - 2, count - 1).wait_recv()

    for step in steps:

        @pl.when((me - step >= 0) & (me < count - 1))
        def _():
            upward(step, jnp.maximum(me - step, 0)).wait_send()

        @pl.when((me + step < count) & (me > 0))
        def _():
            downward(step, jnp.minimum(me + step, count - 1)).wait_send()


def line_gather(own, experts, number, *waits):
    hbm = pl.BlockSpec(memory_space=pl.ANY)
    steps = (max(experts - 1, 1),)
    return pl.pallas_call(
        line_kernel,
        in_specs=[hbm] * (1 + len(waits)),
        out_specs=hbm,
        out_shape=jax.ShapeDtypeStruct((experts,) + own.shape, own.dtype),
        scratch_shapes=[pltpu.VMEM(own.shape, own.dtype)]
        + [pltpu.SemaphoreType.DMA(steps)] * 4
        + [pltpu.SemaphoreType.DMA((2,))],
        compiler_params=pltpu.CompilerParams(collective_id=number, has_side_effects=True),
        cost_estimate=pl.CostEstimate(
            flops=0, bytes_accessed=4 * experts * own.size, transcendentals=0
        ),
        name="line_gather",
    )(own, *waits)


def hold(value, *others):
    for other in others:
        last = other[(slice(-1, None),) * other.ndim].reshape(())
        value = value + jnp.minimum(jnp.abs(last), 0).astype(value.dtype)
    return value


def hop_sum(parts, place, count):
    total = lax.dynamic_index_in_dim(parts, place, 0, keepdims=False).astype(f32)
    got = []
    for hop in range(1, count):
        ring = [(i, (i + hop) % count) for i in range(count)]
        piece = lax.dynamic_index_in_dim(parts, (place + hop) % count, 0, keepdims=False)
        got.append(lax.ppermute(piece, "expert", ring))
    for piece in got:
        total = total + piece.astype(f32)
    return total


def after(value, *others):
    return lax.optimization_barrier((value,) + others)[0]


def plane_sum(terms):
    return lax.psum_scatter(terms, "dp", scatter_dimension=0, tiled=True)


def chip_sum(terms, owners):
    chips = owners // 2
    place = lax.axis_index("dp")
    chip, core = place // 2, place % 2
    blocks = terms.reshape(chips, 2, -1, terms.shape[1])
    mine = lax.dynamic_index_in_dim(blocks, core, 1, keepdims=False)
    other = lax.dynamic_index_in_dim(blocks, 1 - core, 1, keepdims=False)
    other = lax.ppermute(other, "dp", [(i, i + 1 - 2 * (i % 2)) for i in range(owners)])
    mine = (mine.astype(f32) + other.astype(f32)).astype(bf16)
    got = [lax.dynamic_index_in_dim(mine, chip, 0, keepdims=False)]
    for hop in range(1, chips):
        ring = [(i, (i // 2 + hop) % chips * 2 + i % 2) for i in range(owners)]
        piece = lax.dynamic_index_in_dim(mine, (chip + hop) % chips, 0, keepdims=False)
        got.append(lax.ppermute(piece, "dp", ring))
    return sum(piece.astype(f32) for piece in got)


def hops(rows, sign):
    count = rows.shape[0]
    pieces = [rows[0]]
    for hop in range(1, count):
        ring = [(i, (i + sign * hop) % count) for i in range(count)]
        pieces.append(lax.ppermute(rows[hop], "expert", ring))
    return jnp.stack(pieces)


def scatter_hops(rows, place):
    count = rows.shape[0]
    pieces = [lax.dynamic_index_in_dim(rows, place, 0, keepdims=False)]
    for hop in range(1, count):
        ring = [(i, (i + hop) % count) for i in range(count)]
        piece = lax.dynamic_index_in_dim(rows, (place + hop) % count, 0, keepdims=False)
        pieces.append(lax.ppermute(piece, "expert", ring))
    return jnp.stack(pieces)


def ordered_hops(rows, place):
    count = rows.shape[0]
    got = jnp.zeros_like(rows)
    for hop in range(count):
        piece = lax.dynamic_index_in_dim(rows, (place + hop) % count, 0, keepdims=False)
        if hop:
            ring = [(i, (i + hop) % count) for i in range(count)]
            piece = lax.ppermute(piece, "expert", ring)
        got = lax.dynamic_update_index_in_dim(got, piece, (place - hop) % count, 0)
    return got


def spread(rows, axes, count):
    copies = jnp.broadcast_to(rows[None], (count,) + rows.shape)
    return lax.all_to_all(copies, axes, split_axis=0, concat_axis=0, tiled=True)


def layer(
    layer_input,
    cotangent,
    cont_ids,
    attn_routes,
    attn_gates,
    mlp_routes,
    mlp_gates,
    gain_attn,
    gain_mlp,
    kv_weight,
    query_weight,
    output_weight,
    mlp_weight,
):
    experts = lax.axis_size("expert")
    owners = lax.axis_size("dp")
    expert_id = lax.axis_index("expert")
    tok_dev, width = layer_input.shape
    per_token = attn_routes.shape[1]
    capacity = tok_dev * per_token * 9 // (8 * experts)
    slots = -(-capacity // 8) * 8
    slot_total = experts * slots
    group = cont_ids.shape[0]
    features = query_weight.shape[2]
    expert_ids = jnp.arange(experts, dtype=jnp.int32)
    slot_ids = jnp.arange(slots, dtype=jnp.int32)

    kv_part = line_gather(kv_weight, experts, 6).reshape(-1, kv_weight.shape[1])
    kv_full = lax.all_gather(kv_part, "dp", axis=0, tiled=True)
    x_all = line_gather(layer_input, experts, 7, kv_part).reshape(group, width)
    query_full = lax.all_gather(query_weight[:, 0, :], "dp", axis=0, tiled=True)
    output_full = lax.all_gather(output_weight[:, 0, :], "dp", axis=0, tiled=True)
    gains = jnp.concatenate([gain_attn, gain_mlp])[None]
    gains = spread(gains, ("dp", "expert"), owners * experts)
    part_size = gain_attn.shape[0]
    gains = gains.reshape(owners * experts, 2, part_size)
    gain_one = gains[:, 0].reshape(-1).astype(f32)
    gain_two = gains[:, 1].reshape(-1).astype(f32)

    hop_ids = (expert_id + expert_ids) % experts
    mlp_hot = mlp_routes.T[:, None, :] == hop_ids[None, :, None]
    mlp_mine = jnp.any(mlp_hot, axis=0)
    mlp_rank = before_counts(mlp_mine)
    mlp_pick = mlp_mine[:, None, :] & (mlp_rank[:, None, :] == slot_ids[None, :, None])
    mlp_gate_tok = jnp.sum(jnp.where(mlp_hot, mlp_gates.T[:, None, :], 0.0), axis=0)
    mlp_slot_gate = jnp.sum(jnp.where(mlp_pick, mlp_gate_tok[:, None, :], 0.0), axis=2)
    mlp_pick_low = mlp_pick.astype(bf16).reshape(slot_total, tok_dev)
    mlp_choice = [
        (mlp_pick & mlp_hot[k][:, None, :]).astype(bf16).reshape(slot_total, tok_dev)
        for k in range(per_token)
    ]
    mlp_back = jnp.concatenate(mlp_choice, axis=1)

    attn_all = attn_routes.reshape(experts, tok_dev, per_token)
    own_mine = jnp.any(attn_all == expert_id, axis=2)
    own_rank = before_counts(own_mine)
    own_pick = own_mine[:, None, :] & (own_rank[:, None, :] == slot_ids[None, :, None])
    own_low = own_pick.astype(bf16)
    places_row, positions_row = token_positions(cont_ids)

    def slot_value(row):
        return jnp.sum(
            jnp.where(own_pick, row.reshape(experts, 1, tok_dev), 0), axis=2, dtype=jnp.int32
        )

    slot_place = slot_value(places_row) + jnp.where(
        jnp.any(own_pick, axis=2), 0, expert_ids[:, None] * tok_dev
    )
    slot_cont = slot_value(cont_ids)
    slot_pos = slot_value(positions_row)
    attn_mine_routes = lax.dynamic_slice_in_dim(attn_routes, expert_id * tok_dev, tok_dev)
    attn_hot = attn_mine_routes.T[:, None, :] == expert_ids[None, :, None]
    attn_mine = jnp.any(attn_hot, axis=0)
    attn_rank = before_counts(attn_mine)
    attn_pick = attn_mine[:, None, :] & (attn_rank[:, None, :] == slot_ids[None, :, None])
    attn_gate_tok = jnp.sum(jnp.where(attn_hot, attn_gates.T[:, None, :], 0.0), axis=0)
    attn_slot_gate = jnp.sum(jnp.where(attn_pick, attn_gate_tok[:, None, :], 0.0), axis=2)
    attn_pick_low = attn_pick.astype(bf16).reshape(slot_total, tok_dev)
    from_ids = (expert_id - expert_ids) % experts
    result_hot = attn_mine_routes.T[:, None, :] == from_ids[None, :, None]
    result_pick = jnp.any(result_hot, axis=0)
    result_rank = before_counts(result_pick)
    result_pick = result_pick[:, None, :] & (
        result_rank[:, None, :] == slot_ids[None, :, None]
    )
    result_hot = jnp.concatenate(
        [(result_pick & result_hot[k][:, None, :]).astype(bf16) for k in range(per_token)], axis=2
    )
    kcos, ksin = rope_tables(positions_row)
    qcos, qsin = rope_tables(slot_pos.reshape(-1))

    cot_rows = dot_nn(mlp_pick_low, cotangent).reshape(experts, slots, width)
    send_grad = (mlp_slot_gate[:, :, None] * cot_rows).astype(bf16)
    steps = slots // 8
    cuts = [0, 8 * max(int(steps * MLP_FIRST), 1), slots]
    pieces = list(zip(cuts[:-1], cuts[1:]))

    def to_plane(rows):
        return lax.all_gather(rows.reshape(-1, width), "dp", axis=0, tiled=True)

    got_grad = hops(hold(send_grad, x_all), 1)

    input_f32 = x_all.astype(f32)
    normed_all, _ = rms_parts(input_f32)
    hidden_all = (normed_all * gain_one).astype(bf16)
    query_rows = lax.dot_general(
        own_low,
        hidden_all.reshape(experts, tok_dev, width),
        (((2,), (1,)), ((0,), (0,))),
        preferred_element_type=f32,
    ).astype(bf16).reshape(slot_total, width)
    query_low = project(
        query_rows, query_full, qcos, qsin, features, slot_total
    ).reshape(experts, slots, features)
    kv_low = project(hidden_all, kv_full, kcos, ksin, features, tok_dev)
    got_grad = hold(got_grad, kv_low)
    plane_grad = [to_plane(got_grad[:, low:high, :]) for low, high in pieces]
    slot_place3 = slot_place[:, :, None]
    slot_cont3 = slot_cont[:, :, None]
    key_cont = cont_ids[None, :]
    mid = min(-(-slots // 32) * 16, slots - 8)
    halves = ((0, mid), (mid, slots))
    attn_low, lse, result_tok = [], [], 0.0
    for low, high in halves:
        attn_part, lse_part = attend(
            query_low, kv_low, slot_place3, slot_cont3, key_cont, tok_dev, low, high
        )
        attn_part = attn_part.reshape(-1, features)
        attn_low.append(attn_part)
        lse.append(lse_part)
        result_low = dot_nn(attn_part, output_full).astype(bf16)
        result_back = scatter_hops(result_low.reshape(experts, high - low, width), expert_id)
        result_tok = result_tok + dot_tn(
            result_hot[:, low:high].reshape(-1, per_token * tok_dev), result_back.reshape(-1, width)
        )
    own_f32 = layer_input.astype(f32)
    residual = own_f32
    for k in range(per_token):
        residual = residual + attn_gates[:, k : k + 1] * result_tok[k * tok_dev : (k + 1) * tok_dev]
    normed_two, scale_two = rms_parts(residual)
    second_low = (normed_two * gain_two).astype(bf16)

    send_in = dot_nn(mlp_pick_low, second_low).astype(bf16).reshape(experts, slots, width)
    gate_rows, up_rows, down_rows = (mlp_weight[:, 0, j, :] for j in range(3))
    plane_in = [to_plane(hops(send_in[:, low:high, :], 1)) for low, high in pieces]
    kept, out_parts, in_parts = [], [], []
    for number, (rows_in, rows_grad) in enumerate(zip(plane_in, plane_grad)):
        in_part, out_part, *keep = unit_block(
            rows_in, rows_grad, gate_rows, up_rows, down_rows, owners, number
        )
        in_parts.append(in_part)
        out_parts.append(out_part)
        kept.append(keep)

    def join(parts):
        back = []
        for part, (low, high) in zip(parts, pieces):
            back.append(hops(part.reshape(experts, high - low, width), -1))
        return jnp.concatenate(back, axis=1).reshape(slot_total, width)

    in_back = join(in_parts)
    grad_mlp = [dot_tn(k, r) for k, r in zip(kept[0], (plane_in[0], plane_in[0], plane_grad[0]))]
    grad_second = dot_tn(mlp_pick_low, after(in_back, *grad_mlp))
    cot_f32 = cotangent.astype(f32)
    grad_resid = cot_f32 + rms_back(grad_second, normed_two, scale_two, gain_two)

    cot_slots = dot_nn(attn_pick_low, grad_resid.astype(bf16)).reshape(experts, slots, width)
    send_cot = (attn_slot_gate[:, :, None] * cot_slots).astype(bf16)
    for j, rows in enumerate((plane_in[1], plane_in[1], plane_grad[1])):
        grad_mlp[j] = grad_mlp[j] + dot_tn(kept[1][j], rows)
    grad_mlp_weight = jnp.stack(grad_mlp, axis=1)[:, None, :, :]
    grad_result = [
        ordered_hops(send_cot[:, low:high], expert_id).reshape(-1, width)
        for low, high in halves
    ]
    grad_attn = []
    for rows in grad_result:
        grad_attn.append(
            dot_nt(rows, output_full).astype(bf16).reshape(experts, -1, features)
        )
    output_term = (
        dot_tn(attn_low[0], grad_result[0]) + dot_tn(attn_low[1], grad_result[1])
    ).astype(bf16)
    grad_output_w = chip_sum(output_term, owners)
    out_back = join([plane_sum(part) for part in out_parts])
    tables = (
        slot_place3,
        slot_cont3,
        key_cont,
        qcos.reshape(experts, slots, HEAD),
        qsin.reshape(experts, slots, HEAD),
        kcos,
        ksin,
        tok_dev,
    )
    carried = attend_back(query_low, kv_low, grad_attn[0], lse[0], *tables, 0)
    grad_query, grad_keys, grad_values = attend_back(
        query_low, kv_low, grad_attn[1], lse[1], *tables, mid, tuple(carried)
    )
    grad_query = grad_query.reshape(slot_total, features)
    mixed_tok = dot_tn(mlp_back, out_back)
    final = residual
    for k in range(per_token):
        final = final + mlp_gates[:, k : k + 1] * mixed_tok[k * tok_dev : (k + 1) * tok_dev]
    output = final.astype(bf16)

    grad_keys_w = dot_tn(hidden_all, grad_keys).astype(bf16)
    grad_values_w = dot_tn(hidden_all, grad_values).astype(bf16)
    grad_query = hold(grad_query, grad_keys_w, grad_values_w)
    grad_kv_w = [plane_sum(grad_keys_w), plane_sum(grad_values_w)]

    grad_rows = dot_nt(grad_query, query_full).astype(bf16)
    half = width // 2
    grad_h, grad_first = [], []
    for low in (0, half):
        span = slice(low, low + half)
        routed = lax.dot_general(
            own_low,
            grad_rows[:, span].reshape(experts, slots, half),
            (((1,), (1,)), ((0,), (0,))),
            preferred_element_type=f32,
        ).reshape(group, half)
        part = (
            dot_nt(grad_keys, kv_full[span, :features])
            + dot_nt(grad_values, kv_full[span, features:])
            + routed
        )
        grad_h.append(part)
        grad_first.append(
            hop_sum(part.astype(bf16).reshape(experts, tok_dev, half), expert_id, experts)
        )
    query_term = dot_tn(query_rows, hold(grad_query, grad_h[1])).astype(bf16)
    grad_query_w = chip_sum(query_term, owners)
    grad_kv_w = jnp.concatenate(
        [hop_sum(part.reshape(experts, -1, features), expert_id, experts) for part in grad_kv_w],
        axis=1,
    )
    grad_h = lax.optimization_barrier(tuple(grad_h))
    grad_gain_one = [
        jnp.sum(part * normed_all[:, low : low + half], axis=0)
        for part, low in zip(grad_h, (0, half))
    ]
    grad_gain_two = jnp.sum(grad_second * normed_two, axis=0)
    first_sum = grad_first[0]
    grad_first = jnp.concatenate(grad_first, axis=1)
    normed_one, scale_one = rms_parts(own_f32)
    grad_input = grad_resid + rms_back(grad_first, normed_one, scale_one, gain_one)

    gain_rows = jnp.concatenate(
        [
            jnp.concatenate(grad_gain_one).reshape(owners * experts, part_size),
            grad_gain_two.reshape(owners * experts, part_size),
        ],
        axis=1,
    )
    gain_rows = lax.all_to_all(
        hold(gain_rows, first_sum)[:, None, :], ("dp", "expert"), split_axis=0, concat_axis=0, tiled=True
    )
    gain_rows = jnp.sum(gain_rows, axis=(0, 1))
    grad_gain_attn, grad_gain_mlp = gain_rows[:part_size], gain_rows[part_size:]
    return (
        output,
        grad_input,
        grad_gain_attn,
        grad_gain_mlp,
        grad_kv_w,
        grad_query_w[:, None, :],
        grad_output_w[:, None, :],
        grad_mlp_weight,
    )


def solution(mesh):
    placed = (
        P(("dp", "expert"), None),
        P(("dp", "expert"), None),
        P("dp"),
        P("dp", None),
        P(("dp", "expert"), None),
        P(("dp", "expert"), None),
        P(("dp", "expert"), None),
        P(("dp", "expert")),
        P(("dp", "expert")),
        P(("dp", "expert"), None),
        P("dp", "expert", None),
        P("dp", "expert", None),
        P("dp", "expert", None, None),
    )
    return jax.shard_map(
        layer,
        mesh=mesh,
        in_specs=placed,
        out_specs=(
            P(("dp", "expert"), None),
            P(("dp", "expert"), None),
            P(("dp", "expert")),
            P(("dp", "expert")),
            P(("dp", "expert"), None),
            P("dp", "expert", None),
            P("dp", "expert", None),
            P("dp", "expert", None, None),
        ),
        check_vma=False,
    )
```

```python
import functools
import math

import jax
import jax.numpy as jnp
from jax import lax
from jax.experimental import pallas as pl
from jax.experimental.pallas import tpu as pltpu
from jax.sharding import PartitionSpec as P


HEAD = 128
PROMPT = 1024
CONTS = 2
GROUP_TOK = 1280
MLP_FIRST = 0.5

norm_eps = 1e-06
rope_base = 10000.0
neg_fill = -1e30
log2e = 1.4426950408889634
MESH = pl.DeviceIdType.MESH
contract_last = (((1,), (1,)), ((), ()))
contract_first = (((0,), (0,)), ((), ()))
f32 = jnp.float32
bf16 = jnp.bfloat16


def rope_tables(positions):
    half_size = HEAD // 2
    freq_steps = jnp.arange(half_size, dtype=f32)
    inverse_freq = jnp.exp(-math.log(rope_base) * 2.0 * freq_steps / HEAD)
    angles = positions.astype(f32)[:, None] * inverse_freq[None, :]
    cosine, sine = jnp.cos(angles), jnp.sin(angles)
    return (
        jnp.concatenate([cosine, cosine], axis=1),
        jnp.concatenate([-sine, sine], axis=1),
    )


def token_positions(cont_ids):
    row_count = cont_ids.shape[0]
    group_count = row_count // GROUP_TOK
    places = jnp.arange(row_count, dtype=jnp.int32) % GROUP_TOK
    labels = jnp.arange(CONTS + 1, dtype=jnp.int32)
    one_hot = (cont_ids[:, None] == labels[None, :]).astype(jnp.int32)
    counts = jnp.sum(one_hot.reshape(group_count, GROUP_TOK, CONTS + 1), axis=1)
    starts = jnp.cumsum(counts, axis=1) - counts
    starts_tok = jnp.broadcast_to(starts[:, None, :], (group_count, GROUP_TOK, CONTS + 1)).reshape(
        row_count, CONTS + 1
    )
    start_of = jnp.sum(starts_tok * one_hot, axis=1)
    return (places, places - start_of + PROMPT * (cont_ids > 0).astype(jnp.int32))


def rms_parts(values):
    row_scale = lax.rsqrt(jnp.mean(values * values, axis=-1, keepdims=True) + norm_eps)
    return (values * row_scale, row_scale)


def rms_back(grad_out, normed, row_scale, gain_vec):
    through = grad_out * gain_vec
    grad_in = row_scale * (through - normed * jnp.mean(through * normed, axis=-1, keepdims=True))
    return grad_in


def dot_nt(left, right):
    return lax.dot_general(left, right, contract_last, preferred_element_type=f32)


def dot_tn(left, right):
    return lax.dot_general(left, right, contract_first, preferred_element_type=f32)


def dot_nn(left, right):
    return jnp.dot(left, right, preferred_element_type=f32)


def before_counts(flags):
    count = flags.shape[-1]
    steps = jnp.arange(count, dtype=jnp.int32)
    earlier = (steps[:, None] < steps[None, :]).astype(bf16)
    return jnp.dot(flags.astype(bf16), earlier, preferred_element_type=f32).astype(jnp.int32)


def project_kernel(rope_blocks, tile, x_ref, w_ref, cos_ref, sin_ref, out_ref):
    rows = x_ref.shape[0]
    turn = pl.program_id(0) < rope_blocks
    for start in range(0, rows, tile):
        span = pl.ds(start, tile)
        product = jnp.dot(x_ref[span, :], w_ref[...], preferred_element_type=f32)

        @pl.when(turn)
        def _():
            cosine, sine = cos_ref[span, :], sin_ref[span, :]
            for col in range(0, product.shape[1], HEAD):
                piece = product[:, col : col + HEAD]
                turned = piece * cosine + pltpu.roll(piece, HEAD // 2, 1) * sine
                out_ref[span, col : col + HEAD] = turned.astype(bf16)

        @pl.when(jnp.logical_not(turn))
        def _():
            out_ref[span, :] = product.astype(bf16)


def project(rows, weight, cosine, sine, rope_cols, tile):
    count, width = rows.shape
    cols = weight.shape[1]
    block = 512
    return pl.pallas_call(
        functools.partial(project_kernel, rope_cols // block, tile),
        grid=(cols // block,),
        in_specs=[
            pl.BlockSpec((count, width), lambda i: (0, 0)),
            pl.BlockSpec((width, block), lambda i: (0, i)),
            pl.BlockSpec((count, HEAD), lambda i: (0, 0)),
            pl.BlockSpec((count, HEAD), lambda i: (0, 0)),
        ],
        out_specs=pl.BlockSpec((count, block), lambda i: (0, i)),
        out_shape=jax.ShapeDtypeStruct((count, cols), bf16),
        cost_estimate=pl.CostEstimate(
            flops=2 * count * width * cols,
            bytes_accessed=2 * (count * width + width * cols + count * cols),
            transcendentals=0,
        ),
    )(rows, weight, cosine, sine)


def key_spans(blocks, tokens, keys):
    return [min(-(-(tokens * (s + 1)) // 128) * 128, keys) for s in range(blocks)]


def fill_bias(bias, place_ref, cont_ref, kcont_ref):
    blocks, slots, keys = bias.shape
    kplace = lax.broadcasted_iota(jnp.int32, (slots, keys), 1)
    kcont = kcont_ref[...]
    for s in range(blocks):
        allowed = (kplace <= place_ref[s]) & ((kcont == 0) | (kcont == cont_ref[s]))
        bias[s] = jnp.where(allowed, 0.0, neg_fill)


def attend_kernel(spans, q_ref, k_ref, v_ref, place_ref, cont_ref, kcont_ref, out_ref, lse_ref, bias):
    @pl.when(pl.program_id(0) == 0)
    def _():
        fill_bias(bias, place_ref, cont_ref, kcont_ref)

    scale2 = log2e / math.sqrt(HEAD)
    for s, span in enumerate(spans):
        scores = dot_nt(q_ref[s], k_ref[:span, :]) * scale2 + bias[s, :, :span]
        peak = jnp.max(scores, axis=1, keepdims=True)
        weights = jnp.exp2(scores - peak)
        total = jnp.sum(weights, axis=1, keepdims=True)
        mixed = dot_nn(weights.astype(bf16), v_ref[:span, :])
        out_ref[s] = (mixed / total).astype(bf16)
        lse_ref[s] = jnp.broadcast_to(peak + jnp.log2(total), lse_ref.shape[1:])


def attend(query, kv_low, place, cont, kcont, tokens):
    blocks, slots, features = query.shape
    keys = kv_low.shape[0]
    heads = features // HEAD
    spans = key_spans(blocks, tokens, keys)
    work = 2 * 2 * slots * sum(spans) * HEAD * heads
    qspec = pl.BlockSpec((blocks, slots, HEAD), lambda h: (0, 0, h))
    whole = pl.BlockSpec((blocks, slots, 1), lambda h: (0, 0, 0))
    return pl.pallas_call(
        functools.partial(attend_kernel, spans),
        grid=(heads,),
        in_specs=[
            qspec,
            pl.BlockSpec((keys, HEAD), lambda h: (0, h)),
            pl.BlockSpec((keys, HEAD), lambda h: (0, heads + h)),
            whole,
            whole,
            pl.BlockSpec((1, keys), lambda h: (0, 0)),
        ],
        out_specs=[qspec, qspec],
        out_shape=[
            jax.ShapeDtypeStruct(query.shape, bf16),
            jax.ShapeDtypeStruct(query.shape, f32),
        ],
        scratch_shapes=[pltpu.VMEM((blocks, slots, keys), f32)],
        cost_estimate=pl.CostEstimate(
            flops=work,
            bytes_accessed=4 * query.size + 2 * kv_low.size + 4 * query.size,
            transcendentals=slots * sum(spans) * heads,
        ),
        name="attend",
    )(query, kv_low, kv_low, place, cont, kcont)


def attend_back_kernel(spans, *refs):
    q_ref, k_ref, v_ref, g_ref, lse_ref, place_ref, cont_ref, kcont_ref = refs[:8]
    qcos_ref, qsin_ref, kcos_ref, ksin_ref = refs[8:12]
    dq_ref, dk_ref, dv_ref, bias, dk_sum, dv_sum = refs[12:]

    @pl.when(pl.program_id(0) == 0)
    def _():
        fill_bias(bias, place_ref, cont_ref, kcont_ref)

    scale = 1.0 / math.sqrt(HEAD)
    scale2 = log2e * scale
    last = len(spans) - 1
    for s in range(last, -1, -1):
        span = spans[s]
        query, grad = q_ref[s], g_ref[s]
        keys = k_ref[:span, :]
        scores = dot_nt(query, keys) * scale2 + bias[s, :, :span]
        prob = jnp.exp2(scores - lse_ref[s][:, :1])
        grad_prob = dot_nt(grad, v_ref[:span, :])
        inner = jnp.sum(prob * grad_prob, axis=1, keepdims=True)
        grad_scores = (prob * (grad_prob - inner)).astype(bf16)
        dq = dot_nn(grad_scores, keys) * scale
        dq = dq * qcos_ref[s] - pltpu.roll(dq, HEAD // 2, 1) * qsin_ref[s]
        dq_ref[s] = dq.astype(bf16)
        dk = dot_tn(grad_scores, query)
        dv = dot_tn(prob.astype(bf16), grad)
        if s < last:
            dk_sum[:span, :] += dk
            dv_sum[:span, :] += dv
        else:
            dk_sum[...] = dk
            dv_sum[...] = dv
    dk = dk_sum[...] * scale
    dk_ref[...] = (dk * kcos_ref[...] - pltpu.roll(dk, HEAD // 2, 1) * ksin_ref[...]).astype(bf16)
    dv_ref[...] = dv_sum[...].astype(bf16)


def attend_back(query, kv_low, grad, lse, place, cont, kcont, qcos, qsin, kcos, ksin, tokens):
    blocks, slots, features = query.shape
    keys = kv_low.shape[0]
    heads = features // HEAD
    spans = key_spans(blocks, tokens, keys)
    work = 5 * 2 * slots * sum(spans) * HEAD * heads
    qspec = pl.BlockSpec((blocks, slots, HEAD), lambda h: (0, 0, h))
    kspec = pl.BlockSpec((keys, HEAD), lambda h: (0, h))
    whole = pl.BlockSpec((blocks, slots, 1), lambda h: (0, 0, 0))
    qtab = pl.BlockSpec((blocks, slots, HEAD), lambda h: (0, 0, 0))
    ktab = pl.BlockSpec((keys, HEAD), lambda h: (0, 0))
    return pl.pallas_call(
        functools.partial(attend_back_kernel, spans),
        grid=(heads,),
        in_specs=[
            qspec,
            kspec,
            pl.BlockSpec((keys, HEAD), lambda h: (0, heads + h)),
            qspec,
            qspec,
            whole,
            whole,
            pl.BlockSpec((1, keys), lambda h: (0, 0)),
            qtab,
            qtab,
            ktab,
            ktab,
        ],
        out_specs=[qspec, kspec, kspec],
        out_shape=[
            jax.ShapeDtypeStruct(query.shape, bf16),
            jax.ShapeDtypeStruct((keys, features), bf16),
            jax.ShapeDtypeStruct((keys, features), bf16),
        ],
        scratch_shapes=[
            pltpu.VMEM((blocks, slots, keys), f32),
            pltpu.VMEM((keys, HEAD), f32),
            pltpu.VMEM((keys, HEAD), f32),
        ],
        cost_estimate=pl.CostEstimate(
            flops=work,
            bytes_accessed=10 * query.size + 4 * kv_low.size,
            transcendentals=slots * sum(spans) * heads,
        ),
        name="attend_back",
    )(query, kv_low, kv_low, grad, lse, place, cont, kcont, qcos, qsin, kcos, ksin)


def unit_kernel(
    x_hbm,
    g_hbm,
    gate_ref,
    up_ref,
    down_ref,
    in_ref,
    out_hbm,
    gg_hbm,
    gu_hbm,
    hid_hbm,
    xbuf,
    gbuf,
    obuf,
    kbuf,
    psend,
    precv,
    ssend,
    frecv,
    load_sem,
    store_sem,
    psend_sem,
    precv_sem,
    ssend_sem,
    frecv_sem,
):
    rows = xbuf.shape[1]
    chips = ssend.shape[0]
    me = lax.axis_index("dp")
    chip = me // 2
    core = me % 2
    partner = me + 1 - 2 * core

    def peer(hop):
        return {"dp": (chip + hop) % chips * 2 + core}

    barrier = pltpu.get_barrier_semaphore()
    pl.semaphore_signal(barrier, inc=1, device_id={"dp": partner}, device_id_type=MESH)
    for hop in range(1, chips):
        pl.semaphore_signal(barrier, inc=1, device_id=peer(hop), device_id_type=MESH)
    pl.semaphore_wait(barrier, chips)

    def block_rows(j, own):
        dest = (chip + chips - 1 - j) % chips
        block = dest * 2 + (core if own else 1 - core)
        return pl.ds(pl.multiple_of(block * rows, 8), rows)

    def loads(j, own):
        span, slot = block_rows(j, own), int(own)
        return [
            pltpu.make_async_copy(x_hbm.at[span], xbuf.at[slot], load_sem.at[0, slot]),
            pltpu.make_async_copy(g_hbm.at[span], gbuf.at[slot], load_sem.at[1, slot]),
        ]

    def stores(j, own):
        span, slot = block_rows(j, own), int(own)
        return [pltpu.make_async_copy(obuf.at[slot], out_hbm.at[span], store_sem.at[0, slot])] + [
            pltpu.make_async_copy(kbuf.at[slot, i], dst.at[span], store_sem.at[1 + i, slot])
            for i, dst in enumerate((gg_hbm, gu_hbm, hid_hbm))
        ]

    def to_partner(j):
        return pltpu.make_async_remote_copy(
            src_ref=psend.at[j % 2],
            dst_ref=precv.at[j],
            send_sem=psend_sem.at[j % 2],
            recv_sem=precv_sem.at[j],
            device_id={"dp": partner},
            device_id_type=MESH,
        )

    def to_owner(j):
        return pltpu.make_async_remote_copy(
            src_ref=ssend.at[j],
            dst_ref=frecv.at[j],
            send_sem=ssend_sem.at[j],
            recv_sem=frecv_sem.at[j],
            device_id=peer(chips - 1 - j),
            device_id_type=MESH,
        )

    def compute(j, own):
        slot = int(own)
        for copy in loads(j, own):
            copy.wait()
        rows_in, rows_grad = xbuf[slot], gbuf[slot]
        gate_val = dot_nt(rows_in, gate_ref[...])
        up_val = dot_nt(rows_in, up_ref[...])
        grad_hidden = dot_nt(rows_grad, down_ref[...])
        sigma = jax.nn.sigmoid(gate_val)
        active = gate_val * sigma
        hidden = (active * up_val).astype(bf16)
        grad_gate = (grad_hidden * up_val * sigma * (1.0 + gate_val * (1.0 - sigma))).astype(bf16)
        grad_up = (grad_hidden * active).astype(bf16)

        @pl.when(j > 0)
        def _():
            for copy in stores(j - 1, own):
                copy.wait()

        kbuf[slot, 0] = grad_gate
        kbuf[slot, 1] = grad_up
        kbuf[slot, 2] = hidden
        obuf[slot] = dot_nn(hidden, down_ref[...]).astype(bf16)
        for copy in stores(j, own):
            copy.start()
        return dot_nn(grad_gate, gate_ref[...]) + dot_nn(grad_up, up_ref[...])

    for copy in loads(0, False):
        copy.start()

    def step(j, carry):
        for copy in loads(j, True):
            copy.start()
        term = compute(j, False)

        @pl.when(j > 1)
        def _():
            to_partner(j - 2).wait_send()

        psend[j % 2] = term.astype(bf16)
        to_partner(j).start()

        @pl.when(j < chips - 1)
        def _():
            for copy in loads(j + 1, False):
                copy.start()

        term = compute(j, True)
        to_partner(j).wait_recv()
        ssend[j] = (term + precv[j].astype(f32)).astype(bf16)

        @pl.when(j < chips - 1)
        def _():
            to_owner(j).start()

        return carry

    lax.fori_loop(0, chips, step, 0)
    total = ssend[chips - 1].astype(f32)
    for j in range(chips - 1):
        to_owner(j).wait_recv()
        total = total + frecv[j].astype(f32)
    in_ref[...] = total.astype(bf16)
    for j in range(chips - 1):
        to_owner(j).wait_send()
    for j in range(max(chips - 2, 0), chips):
        to_partner(j).wait_send()
    for own in (False, True):
        for copy in stores(chips - 1, own):
            copy.wait()


def unit_block(rows_in, rows_grad, gate_rows, up_rows, down_rows, owners, number):
    total, width = rows_in.shape
    units = gate_rows.shape[0]
    rows = total // owners
    chips = owners // 2
    hbm = pl.BlockSpec(memory_space=pl.ANY)
    vmem = pl.BlockSpec(memory_space=pltpu.VMEM)
    kept = jax.ShapeDtypeStruct((total, units), bf16)
    return pl.pallas_call(
        unit_kernel,
        in_specs=[hbm, hbm, vmem, vmem, vmem],
        out_specs=[vmem, hbm, hbm, hbm, hbm],
        out_shape=[
            jax.ShapeDtypeStruct((rows, width), bf16),
            jax.ShapeDtypeStruct((total, width), bf16),
            kept,
            kept,
            kept,
        ],
        scratch_shapes=[
            pltpu.VMEM((2, rows, width), bf16),
            pltpu.VMEM((2, rows, width), bf16),
            pltpu.VMEM((2, rows, width), bf16),
            pltpu.VMEM((2, 3, rows, units), bf16),
            pltpu.VMEM((2, rows, width), bf16),
            pltpu.VMEM((chips, rows, width), bf16),
            pltpu.VMEM((chips, rows, width), bf16),
            pltpu.VMEM((chips - 1, rows, width), bf16),
            pltpu.SemaphoreType.DMA((2, 2)),
            pltpu.SemaphoreType.DMA((4, 2)),
            pltpu.SemaphoreType.DMA((2,)),
            pltpu.SemaphoreType.DMA((chips,)),
            pltpu.SemaphoreType.DMA((chips,)),
            pltpu.SemaphoreType.DMA((chips,)),
        ],
        compiler_params=pltpu.CompilerParams(
            collective_id=number, has_side_effects=True, vmem_limit_bytes=67043328
        ),
        cost_estimate=pl.CostEstimate(
            flops=6 * 2 * total * units * width,
            bytes_accessed=2 * (3 * total * width + 3 * total * units + 3 * units * width),
            transcendentals=total * units,
        ),
        name="unit_block",
    )(rows_in, rows_grad, gate_rows, up_rows, down_rows)


def line_kernel(own_ref, *refs):
    all_ref, bounce, up_send, up_recv, down_send, down_recv, local_sem = refs[-7:]
    me = lax.axis_index("expert")
    count = all_ref.shape[0]
    below = jnp.maximum(me - 1, 0)
    above = jnp.minimum(me + 1, count - 1)
    barrier = pltpu.get_barrier_semaphore()

    @pl.when(me > 0)
    def _():
        pl.semaphore_signal(barrier, inc=1, device_id={"expert": below}, device_id_type=MESH)

    @pl.when(me < count - 1)
    def _():
        pl.semaphore_signal(barrier, inc=1, device_id={"expert": above}, device_id_type=MESH)

    inner = (me > 0) & (me < count - 1)

    @pl.when(inner)
    def _():
        pl.semaphore_wait(barrier, 2)

    @pl.when(jnp.logical_not(inner))
    def _():
        pl.semaphore_wait(barrier, 1)

    def upward(step, block):
        return pltpu.make_async_remote_copy(
            src_ref=own_ref if step == 0 else all_ref.at[block],
            dst_ref=all_ref.at[block],
            send_sem=up_send.at[step],
            recv_sem=up_recv.at[step],
            device_id={"expert": above},
            device_id_type=MESH,
        )

    def downward(step, block):
        return pltpu.make_async_remote_copy(
            src_ref=own_ref if step == 0 else all_ref.at[block],
            dst_ref=all_ref.at[block],
            send_sem=down_send.at[step],
            recv_sem=down_recv.at[step],
            device_id={"expert": below},
            device_id_type=MESH,
        )

    steps = range(count - 1)
    for step in steps:
        if step > 0:

            @pl.when(me - step >= 0)
            def _():
                upward(step - 1, jnp.maximum(me - step, 0)).wait_recv()

            @pl.when(me + step < count)
            def _():
                downward(step - 1, jnp.minimum(me + step, count - 1)).wait_recv()

        @pl.when((me - step >= 0) & (me < count - 1))
        def _():
            upward(step, jnp.maximum(me - step, 0)).start()

        @pl.when((me + step < count) & (me > 0))
        def _():
            downward(step, jnp.minimum(me + step, count - 1)).start()

        if step == 0:
            copy = pltpu.make_async_copy(own_ref, bounce, local_sem.at[0])
            copy.start()
            copy.wait()
            copy = pltpu.make_async_copy(bounce, all_ref.at[me], local_sem.at[1])
            copy.start()
            copy.wait()

    @pl.when(me == count - 1)
    def _():
        upward(count - 2, 0).wait_recv()

    @pl.when(me == 0)
    def _():
        downward(count - 2, count - 1).wait_recv()

    for step in steps:

        @pl.when((me - step >= 0) & (me < count - 1))
        def _():
            upward(step, jnp.maximum(me - step, 0)).wait_send()

        @pl.when((me + step < count) & (me > 0))
        def _():
            downward(step, jnp.minimum(me + step, count - 1)).wait_send()


def line_gather(own, experts, number, *waits):
    hbm = pl.BlockSpec(memory_space=pl.ANY)
    steps = (max(experts - 1, 1),)
    return pl.pallas_call(
        line_kernel,
        in_specs=[hbm] * (1 + len(waits)),
        out_specs=hbm,
        out_shape=jax.ShapeDtypeStruct((experts,) + own.shape, own.dtype),
        scratch_shapes=[pltpu.VMEM(own.shape, own.dtype)]
        + [pltpu.SemaphoreType.DMA(steps)] * 4
        + [pltpu.SemaphoreType.DMA((2,))],
        compiler_params=pltpu.CompilerParams(collective_id=number, has_side_effects=True),
        cost_estimate=pl.CostEstimate(
            flops=0, bytes_accessed=4 * experts * own.size, transcendentals=0
        ),
        name="line_gather",
    )(own, *waits)


def hold(value, *others):
    for other in others:
        last = other[(slice(-1, None),) * other.ndim].reshape(())
        value = value + jnp.minimum(jnp.abs(last), 0).astype(value.dtype)
    return value


def exchange(rows):
    return lax.all_to_all(rows, "expert", split_axis=0, concat_axis=0, tiled=True)


def hop_sum(parts, place, count):
    total = lax.dynamic_index_in_dim(parts, place, 0, keepdims=False).astype(f32)
    got = []
    for hop in range(1, count):
        ring = [(i, (i + hop) % count) for i in range(count)]
        piece = lax.dynamic_index_in_dim(parts, (place + hop) % count, 0, keepdims=False)
        got.append(lax.ppermute(piece, "expert", ring))
    for piece in got:
        total = total + piece.astype(f32)
    return total


def after(value, *others):
    return lax.optimization_barrier((value,) + others)[0]


def plane_sum(terms):
    return lax.psum_scatter(terms, "dp", scatter_dimension=0, tiled=True)


def chip_sum(terms, owners):
    chips = owners // 2
    place = lax.axis_index("dp")
    chip, core = place // 2, place % 2
    blocks = terms.reshape(chips, 2, -1, terms.shape[1])
    mine = lax.dynamic_index_in_dim(blocks, core, 1, keepdims=False)
    other = lax.dynamic_index_in_dim(blocks, 1 - core, 1, keepdims=False)
    other = lax.ppermute(other, "dp", [(i, i + 1 - 2 * (i % 2)) for i in range(owners)])
    mine = (mine.astype(f32) + other.astype(f32)).astype(bf16)
    got = [lax.dynamic_index_in_dim(mine, chip, 0, keepdims=False)]
    for hop in range(1, chips):
        ring = [(i, (i // 2 + hop) % chips * 2 + i % 2) for i in range(owners)]
        piece = lax.dynamic_index_in_dim(mine, (chip + hop) % chips, 0, keepdims=False)
        got.append(lax.ppermute(piece, "dp", ring))
    return sum(piece.astype(f32) for piece in got)


def hops(rows, sign):
    count = rows.shape[0]
    pieces = [rows[0]]
    for hop in range(1, count):
        ring = [(i, (i + sign * hop) % count) for i in range(count)]
        pieces.append(lax.ppermute(rows[hop], "expert", ring))
    return jnp.stack(pieces)


def spread(rows, axes, count):
    copies = jnp.broadcast_to(rows[None], (count,) + rows.shape)
    return lax.all_to_all(copies, axes, split_axis=0, concat_axis=0, tiled=True)


def layer(
    layer_input,
    cotangent,
    cont_ids,
    attn_routes,
    attn_gates,
    mlp_routes,
    mlp_gates,
    gain_attn,
    gain_mlp,
    kv_weight,
    query_weight,
    output_weight,
    mlp_weight,
):
    experts = lax.axis_size("expert")
    owners = lax.axis_size("dp")
    expert_id = lax.axis_index("expert")
    tok_dev, width = layer_input.shape
    per_token = attn_routes.shape[1]
    capacity = tok_dev * per_token * 9 // (8 * experts)
    slots = -(-capacity // 8) * 8
    slot_total = experts * slots
    group = cont_ids.shape[0]
    features = query_weight.shape[2]
    expert_ids = jnp.arange(experts, dtype=jnp.int32)
    slot_ids = jnp.arange(slots, dtype=jnp.int32)

    kv_part = line_gather(kv_weight, experts, 6).reshape(-1, kv_weight.shape[1])
    kv_full = lax.all_gather(kv_part, "dp", axis=0, tiled=True)
    x_all = line_gather(layer_input, experts, 7, kv_part).reshape(group, width)
    query_full = lax.all_gather(query_weight[:, 0, :], "dp", axis=0, tiled=True)
    output_full = lax.all_gather(output_weight[:, 0, :], "dp", axis=0, tiled=True)
    gains = jnp.concatenate([gain_attn, gain_mlp])[None]
    gains = spread(gains, ("dp", "expert"), owners * experts)
    part_size = gain_attn.shape[0]
    gains = gains.reshape(owners * experts, 2, part_size)
    gain_one = gains[:, 0].reshape(-1).astype(f32)
    gain_two = gains[:, 1].reshape(-1).astype(f32)

    hop_ids = (expert_id + expert_ids) % experts
    mlp_hot = mlp_routes.T[:, None, :] == hop_ids[None, :, None]
    mlp_mine = jnp.any(mlp_hot, axis=0)
    mlp_rank = before_counts(mlp_mine)
    mlp_pick = mlp_mine[:, None, :] & (mlp_rank[:, None, :] == slot_ids[None, :, None])
    mlp_gate_tok = jnp.sum(jnp.where(mlp_hot, mlp_gates.T[:, None, :], 0.0), axis=0)
    mlp_slot_gate = jnp.sum(jnp.where(mlp_pick, mlp_gate_tok[:, None, :], 0.0), axis=2)
    mlp_pick_low = mlp_pick.astype(bf16).reshape(slot_total, tok_dev)
    mlp_choice = [
        (mlp_pick & mlp_hot[k][:, None, :]).astype(bf16).reshape(slot_total, tok_dev)
        for k in range(per_token)
    ]
    mlp_back = jnp.concatenate(mlp_choice, axis=1)

    attn_all = attn_routes.reshape(experts, tok_dev, per_token)
    own_mine = jnp.any(attn_all == expert_id, axis=2)
    own_rank = before_counts(own_mine)
    own_pick = own_mine[:, None, :] & (own_rank[:, None, :] == slot_ids[None, :, None])
    own_low = own_pick.astype(bf16)
    places_row, positions_row = token_positions(cont_ids)

    def slot_value(row):
        return jnp.sum(
            jnp.where(own_pick, row.reshape(experts, 1, tok_dev), 0), axis=2, dtype=jnp.int32
        )

    slot_place = slot_value(places_row) + jnp.where(
        jnp.any(own_pick, axis=2), 0, expert_ids[:, None] * tok_dev
    )
    slot_cont = slot_value(cont_ids)
    slot_pos = slot_value(positions_row)
    attn_mine_routes = lax.dynamic_slice_in_dim(attn_routes, expert_id * tok_dev, tok_dev)
    attn_hot = attn_mine_routes.T[:, None, :] == expert_ids[None, :, None]
    attn_mine = jnp.any(attn_hot, axis=0)
    attn_rank = before_counts(attn_mine)
    attn_pick = attn_mine[:, None, :] & (attn_rank[:, None, :] == slot_ids[None, :, None])
    attn_gate_tok = jnp.sum(jnp.where(attn_hot, attn_gates.T[:, None, :], 0.0), axis=0)
    attn_slot_gate = jnp.sum(jnp.where(attn_pick, attn_gate_tok[:, None, :], 0.0), axis=2)
    attn_pick_low = attn_pick.astype(bf16).reshape(slot_total, tok_dev)
    attn_back = jnp.concatenate(
        [
            (attn_pick & attn_hot[k][:, None, :]).astype(bf16).reshape(slot_total, tok_dev)
            for k in range(per_token)
        ],
        axis=1,
    )
    kcos, ksin = rope_tables(positions_row)
    qcos, qsin = rope_tables(slot_pos.reshape(-1))

    cot_rows = dot_nn(mlp_pick_low, cotangent).reshape(experts, slots, width)
    send_grad = (mlp_slot_gate[:, :, None] * cot_rows).astype(bf16)
    steps = slots // 8
    cuts = [0, 8 * max(int(steps * MLP_FIRST), 1), slots]
    pieces = list(zip(cuts[:-1], cuts[1:]))

    def to_plane(rows):
        return lax.all_gather(rows.reshape(-1, width), "dp", axis=0, tiled=True)

    got_grad = hops(hold(send_grad, x_all), 1)

    input_f32 = x_all.astype(f32)
    normed_all, _ = rms_parts(input_f32)
    hidden_all = (normed_all * gain_one).astype(bf16)
    query_rows = lax.dot_general(
        own_low,
        hidden_all.reshape(experts, tok_dev, width),
        (((2,), (1,)), ((0,), (0,))),
        preferred_element_type=f32,
    ).astype(bf16).reshape(slot_total, width)
    query_low = project(
        query_rows, query_full, qcos, qsin, features, slot_total
    ).reshape(experts, slots, features)
    kv_low = project(hidden_all, kv_full, kcos, ksin, features, tok_dev)
    got_grad = hold(got_grad, kv_low)
    plane_grad = [to_plane(got_grad[:, low:high, :]) for low, high in pieces]
    slot_place3 = slot_place[:, :, None]
    slot_cont3 = slot_cont[:, :, None]
    key_cont = cont_ids[None, :]
    attn_low, lse = attend(query_low, kv_low, slot_place3, slot_cont3, key_cont, tok_dev)
    attn_flat = attn_low.reshape(slot_total, features)
    result_low = dot_nn(attn_flat, output_full).astype(bf16)
    result_back = exchange(result_low.reshape(experts, slots, width)).reshape(slot_total, width)
    result_tok = dot_tn(attn_back, result_back)
    own_f32 = layer_input.astype(f32)
    residual = own_f32
    for k in range(per_token):
        residual = residual + attn_gates[:, k : k + 1] * result_tok[k * tok_dev : (k + 1) * tok_dev]
    normed_two, scale_two = rms_parts(residual)
    second_low = (normed_two * gain_two).astype(bf16)

    send_in = dot_nn(mlp_pick_low, second_low).astype(bf16).reshape(experts, slots, width)
    gate_rows, up_rows, down_rows = (mlp_weight[:, 0, j, :] for j in range(3))
    plane_in = [to_plane(hops(send_in[:, low:high, :], 1)) for low, high in pieces]
    kept, out_parts, in_parts = [], [], []
    for number, (rows_in, rows_grad) in enumerate(zip(plane_in, plane_grad)):
        in_part, out_part, *keep = unit_block(
            rows_in, rows_grad, gate_rows, up_rows, down_rows, owners, number
        )
        in_parts.append(in_part)
        out_parts.append(out_part)
        kept.append(keep)

    def join(parts):
        back = []
        for part, (low, high) in zip(parts, pieces):
            back.append(hops(part.reshape(experts, high - low, width), -1))
        return jnp.concatenate(back, axis=1).reshape(slot_total, width)

    in_back = join(in_parts)
    grad_mlp = [dot_tn(k, r) for k, r in zip(kept[0], (plane_in[0], plane_in[0], plane_grad[0]))]
    grad_second = dot_tn(mlp_pick_low, after(in_back, *grad_mlp))
    cot_f32 = cotangent.astype(f32)
    grad_resid = cot_f32 + rms_back(grad_second, normed_two, scale_two, gain_two)

    cot_slots = dot_nn(attn_pick_low, grad_resid.astype(bf16)).reshape(experts, slots, width)
    send_cot = (attn_slot_gate[:, :, None] * cot_slots).astype(bf16)
    for j, rows in enumerate((plane_in[1], plane_in[1], plane_grad[1])):
        grad_mlp[j] = grad_mlp[j] + dot_tn(kept[1][j], rows)
    grad_mlp_weight = jnp.stack(grad_mlp, axis=1)[:, None, :, :]
    grad_result = after(exchange(send_cot), grad_mlp_weight).reshape(slot_total, width)
    grad_attn = dot_nt(grad_result, output_full).astype(bf16)
    output_term = dot_tn(attn_flat, grad_result).astype(bf16)
    grad_output_w = chip_sum(output_term, owners)
    out_back = join([plane_sum(after(part, *in_parts)) for part in out_parts])
    grad_query, grad_keys, grad_values = attend_back(
        query_low,
        kv_low,
        grad_attn.reshape(experts, slots, features),
        lse,
        slot_place3,
        slot_cont3,
        key_cont,
        qcos.reshape(experts, slots, HEAD),
        qsin.reshape(experts, slots, HEAD),
        kcos,
        ksin,
        tok_dev,
    )
    grad_query = grad_query.reshape(slot_total, features)
    mixed_tok = dot_tn(mlp_back, out_back)
    final = residual
    for k in range(per_token):
        final = final + mlp_gates[:, k : k + 1] * mixed_tok[k * tok_dev : (k + 1) * tok_dev]
    output = final.astype(bf16)

    grad_keys_w = dot_tn(hidden_all, grad_keys).astype(bf16)
    grad_values_w = dot_tn(hidden_all, grad_values).astype(bf16)
    grad_query = hold(grad_query, grad_keys_w, grad_values_w)
    grad_kv_w = [plane_sum(grad_keys_w), plane_sum(grad_values_w)]

    grad_rows = dot_nt(grad_query, query_full).astype(bf16)
    half = width // 2
    grad_h, grad_first = [], []
    for low in (0, half):
        span = slice(low, low + half)
        routed = lax.dot_general(
            own_low,
            grad_rows[:, span].reshape(experts, slots, half),
            (((1,), (1,)), ((0,), (0,))),
            preferred_element_type=f32,
        ).reshape(group, half)
        part = (
            dot_nt(grad_keys, kv_full[span, :features])
            + dot_nt(grad_values, kv_full[span, features:])
            + routed
        )
        grad_h.append(part)
        grad_first.append(
            hop_sum(part.astype(bf16).reshape(experts, tok_dev, half), expert_id, experts)
        )
    query_term = dot_tn(query_rows, hold(grad_query, grad_h[1])).astype(bf16)
    grad_query_w = chip_sum(query_term, owners)
    grad_kv_w = jnp.concatenate(
        [hop_sum(part.reshape(experts, -1, features), expert_id, experts) for part in grad_kv_w],
        axis=1,
    )
    grad_h = lax.optimization_barrier(tuple(grad_h))
    grad_gain_one = [
        jnp.sum(part * normed_all[:, low : low + half], axis=0)
        for part, low in zip(grad_h, (0, half))
    ]
    grad_gain_two = jnp.sum(grad_second * normed_two, axis=0)
    first_sum = grad_first[0]
    grad_first = jnp.concatenate(grad_first, axis=1)
    normed_one, scale_one = rms_parts(own_f32)
    grad_input = grad_resid + rms_back(grad_first, normed_one, scale_one, gain_one)

    gain_rows = jnp.concatenate(
        [
            jnp.concatenate(grad_gain_one).reshape(owners * experts, part_size),
            grad_gain_two.reshape(owners * experts, part_size),
        ],
        axis=1,
    )
    gain_rows = lax.all_to_all(
        hold(gain_rows, first_sum)[:, None, :], ("dp", "expert"), split_axis=0, concat_axis=0, tiled=True
    )
    gain_rows = jnp.sum(gain_rows, axis=(0, 1))
    grad_gain_attn, grad_gain_mlp = gain_rows[:part_size], gain_rows[part_size:]
    return (
        output,
        grad_input,
        grad_gain_attn,
        grad_gain_mlp,
        grad_kv_w,
        grad_query_w[:, None, :],
        grad_output_w[:, None, :],
        grad_mlp_weight,
    )


def solution(mesh):
    placed = (
        P(("dp", "expert"), None),
        P(("dp", "expert"), None),
        P("dp"),
        P("dp", None),
        P(("dp", "expert"), None),
        P(("dp", "expert"), None),
        P(("dp", "expert"), None),
        P(("dp", "expert")),
        P(("dp", "expert")),
        P(("dp", "expert"), None),
        P("dp", "expert", None),
        P("dp", "expert", None),
        P("dp", "expert", None, None),
    )
    return jax.shard_map(
        layer,
        mesh=mesh,
        in_specs=placed,
        out_specs=(
            P(("dp", "expert"), None),
            P(("dp", "expert"), None),
            P(("dp", "expert")),
            P(("dp", "expert")),
            P(("dp", "expert"), None),
            P("dp", "expert", None),
            P("dp", "expert", None),
            P("dp", "expert", None, None),
        ),
        check_vma=False,
    )
```

```python
import functools
import math

import jax
import jax.numpy as jnp
from jax import lax
from jax.experimental import pallas as pl
from jax.experimental.pallas import tpu as pltpu
from jax.sharding import PartitionSpec as P


HEAD = 128
PROMPT = 1024
CONTS = 2
GROUP_TOK = 1280
MLP_FIRST = 0.5

norm_eps = 1e-06
rope_base = 10000.0
neg_fill = -1e30
log2e = 1.4426950408889634
MESH = pl.DeviceIdType.MESH
contract_last = (((1,), (1,)), ((), ()))
contract_first = (((0,), (0,)), ((), ()))
f32 = jnp.float32
bf16 = jnp.bfloat16


def rope_tables(positions):
    half_size = HEAD // 2
    freq_steps = jnp.arange(half_size, dtype=f32)
    inverse_freq = jnp.exp(-math.log(rope_base) * 2.0 * freq_steps / HEAD)
    angles = positions.astype(f32)[:, None] * inverse_freq[None, :]
    cosine, sine = jnp.cos(angles), jnp.sin(angles)
    return (
        jnp.concatenate([cosine, cosine], axis=1),
        jnp.concatenate([-sine, sine], axis=1),
    )


def token_positions(cont_ids):
    row_count = cont_ids.shape[0]
    group_count = row_count // GROUP_TOK
    places = jnp.arange(row_count, dtype=jnp.int32) % GROUP_TOK
    labels = jnp.arange(CONTS + 1, dtype=jnp.int32)
    one_hot = (cont_ids[:, None] == labels[None, :]).astype(jnp.int32)
    counts = jnp.sum(one_hot.reshape(group_count, GROUP_TOK, CONTS + 1), axis=1)
    starts = jnp.cumsum(counts, axis=1) - counts
    starts_tok = jnp.broadcast_to(starts[:, None, :], (group_count, GROUP_TOK, CONTS + 1)).reshape(
        row_count, CONTS + 1
    )
    start_of = jnp.sum(starts_tok * one_hot, axis=1)
    return (places, places - start_of + PROMPT * (cont_ids > 0).astype(jnp.int32))


def rms_parts(values):
    row_scale = lax.rsqrt(jnp.mean(values * values, axis=-1, keepdims=True) + norm_eps)
    return (values * row_scale, row_scale)


def rms_back(grad_out, normed, row_scale, gain_vec):
    through = grad_out * gain_vec
    grad_in = row_scale * (through - normed * jnp.mean(through * normed, axis=-1, keepdims=True))
    return grad_in


def dot_nt(left, right):
    return lax.dot_general(left, right, contract_last, preferred_element_type=f32)


def dot_tn(left, right):
    return lax.dot_general(left, right, contract_first, preferred_element_type=f32)


def dot_nn(left, right):
    return jnp.dot(left, right, preferred_element_type=f32)


def before_counts(flags):
    count = flags.shape[-1]
    steps = jnp.arange(count, dtype=jnp.int32)
    earlier = (steps[:, None] < steps[None, :]).astype(bf16)
    return jnp.dot(flags.astype(bf16), earlier, preferred_element_type=f32).astype(jnp.int32)


def project_kernel(rope_blocks, tile, x_ref, w_ref, cos_ref, sin_ref, out_ref):
    rows = x_ref.shape[0]
    turn = pl.program_id(0) < rope_blocks
    for start in range(0, rows, tile):
        span = pl.ds(start, tile)
        product = jnp.dot(x_ref[span, :], w_ref[...], preferred_element_type=f32)

        @pl.when(turn)
        def _():
            cosine, sine = cos_ref[span, :], sin_ref[span, :]
            for col in range(0, product.shape[1], HEAD):
                piece = product[:, col : col + HEAD]
                turned = piece * cosine + pltpu.roll(piece, HEAD // 2, 1) * sine
                out_ref[span, col : col + HEAD] = turned.astype(bf16)

        @pl.when(jnp.logical_not(turn))
        def _():
            out_ref[span, :] = product.astype(bf16)


def project(rows, weight, cosine, sine, rope_cols, tile):
    count, width = rows.shape
    cols = weight.shape[1]
    block = 512
    return pl.pallas_call(
        functools.partial(project_kernel, rope_cols // block, tile),
        grid=(cols // block,),
        in_specs=[
            pl.BlockSpec((count, width), lambda i: (0, 0)),
            pl.BlockSpec((width, block), lambda i: (0, i)),
            pl.BlockSpec((count, HEAD), lambda i: (0, 0)),
            pl.BlockSpec((count, HEAD), lambda i: (0, 0)),
        ],
        out_specs=pl.BlockSpec((count, block), lambda i: (0, i)),
        out_shape=jax.ShapeDtypeStruct((count, cols), bf16),
        cost_estimate=pl.CostEstimate(
            flops=2 * count * width * cols,
            bytes_accessed=2 * (count * width + width * cols + count * cols),
            transcendentals=0,
        ),
    )(rows, weight, cosine, sine)


def key_spans(blocks, tokens, keys):
    return [min(-(-(tokens * (s + 1)) // 128) * 128, keys) for s in range(blocks)]


def fill_bias(bias, place_ref, cont_ref, kcont_ref):
    blocks, slots, keys = bias.shape
    kplace = lax.broadcasted_iota(jnp.int32, (slots, keys), 1)
    kcont = kcont_ref[...]
    for s in range(blocks):
        allowed = (kplace <= place_ref[s]) & ((kcont == 0) | (kcont == cont_ref[s]))
        bias[s] = jnp.where(allowed, 0.0, neg_fill)


def attend_kernel(spans, q_ref, k_ref, v_ref, place_ref, cont_ref, kcont_ref, out_ref, lse_ref, bias):
    @pl.when(pl.program_id(0) == 0)
    def _():
        fill_bias(bias, place_ref, cont_ref, kcont_ref)

    scale2 = log2e / math.sqrt(HEAD)
    for s, span in enumerate(spans):
        scores = dot_nt(q_ref[s], k_ref[:span, :]) * scale2 + bias[s, :, :span]
        peak = jnp.max(scores, axis=1, keepdims=True)
        weights = jnp.exp2(scores - peak)
        total = jnp.sum(weights, axis=1, keepdims=True)
        mixed = dot_nn(weights.astype(bf16), v_ref[:span, :])
        out_ref[s] = (mixed / total).astype(bf16)
        lse_ref[s] = jnp.broadcast_to(peak + jnp.log2(total), lse_ref.shape[1:])


def attend(query, kv_low, place, cont, kcont, tokens):
    blocks, slots, features = query.shape
    keys = kv_low.shape[0]
    heads = features // HEAD
    spans = key_spans(blocks, tokens, keys)
    work = 2 * 2 * slots * sum(spans) * HEAD * heads
    qspec = pl.BlockSpec((blocks, slots, HEAD), lambda h: (0, 0, h))
    whole = pl.BlockSpec((blocks, slots, 1), lambda h: (0, 0, 0))
    return pl.pallas_call(
        functools.partial(attend_kernel, spans),
        grid=(heads,),
        in_specs=[
            qspec,
            pl.BlockSpec((keys, HEAD), lambda h: (0, h)),
            pl.BlockSpec((keys, HEAD), lambda h: (0, heads + h)),
            whole,
            whole,
            pl.BlockSpec((1, keys), lambda h: (0, 0)),
        ],
        out_specs=[qspec, qspec],
        out_shape=[
            jax.ShapeDtypeStruct(query.shape, bf16),
            jax.ShapeDtypeStruct(query.shape, f32),
        ],
        scratch_shapes=[pltpu.VMEM((blocks, slots, keys), f32)],
        cost_estimate=pl.CostEstimate(
            flops=work,
            bytes_accessed=4 * query.size + 2 * kv_low.size + 4 * query.size,
            transcendentals=slots * sum(spans) * heads,
        ),
        name="attend",
    )(query, kv_low, kv_low, place, cont, kcont)


def attend_back_kernel(spans, *refs):
    q_ref, k_ref, v_ref, g_ref, lse_ref, place_ref, cont_ref, kcont_ref = refs[:8]
    qcos_ref, qsin_ref, kcos_ref, ksin_ref = refs[8:12]
    dq_ref, dk_ref, dv_ref, bias, dk_sum, dv_sum = refs[12:]

    @pl.when(pl.program_id(0) == 0)
    def _():
        fill_bias(bias, place_ref, cont_ref, kcont_ref)

    scale = 1.0 / math.sqrt(HEAD)
    scale2 = log2e * scale
    last = len(spans) - 1
    for s in range(last, -1, -1):
        span = spans[s]
        query, grad = q_ref[s], g_ref[s]
        keys = k_ref[:span, :]
        scores = dot_nt(query, keys) * scale2 + bias[s, :, :span]
        prob = jnp.exp2(scores - lse_ref[s][:, :1])
        grad_prob = dot_nt(grad, v_ref[:span, :])
        inner = jnp.sum(prob * grad_prob, axis=1, keepdims=True)
        grad_scores = (prob * (grad_prob - inner)).astype(bf16)
        dq = dot_nn(grad_scores, keys) * scale
        dq = dq * qcos_ref[s] - pltpu.roll(dq, HEAD // 2, 1) * qsin_ref[s]
        dq_ref[s] = dq.astype(bf16)
        dk = dot_tn(grad_scores, query)
        dv = dot_tn(prob.astype(bf16), grad)
        if s < last:
            dk_sum[:span, :] += dk
            dv_sum[:span, :] += dv
        else:
            dk_sum[...] = dk
            dv_sum[...] = dv
    dk = dk_sum[...] * scale
    dk_ref[...] = (dk * kcos_ref[...] - pltpu.roll(dk, HEAD // 2, 1) * ksin_ref[...]).astype(bf16)
    dv_ref[...] = dv_sum[...].astype(bf16)


def attend_back(query, kv_low, grad, lse, place, cont, kcont, qcos, qsin, kcos, ksin, tokens):
    blocks, slots, features = query.shape
    keys = kv_low.shape[0]
    heads = features // HEAD
    spans = key_spans(blocks, tokens, keys)
    work = 5 * 2 * slots * sum(spans) * HEAD * heads
    qspec = pl.BlockSpec((blocks, slots, HEAD), lambda h: (0, 0, h))
    kspec = pl.BlockSpec((keys, HEAD), lambda h: (0, h))
    whole = pl.BlockSpec((blocks, slots, 1), lambda h: (0, 0, 0))
    qtab = pl.BlockSpec((blocks, slots, HEAD), lambda h: (0, 0, 0))
    ktab = pl.BlockSpec((keys, HEAD), lambda h: (0, 0))
    return pl.pallas_call(
        functools.partial(attend_back_kernel, spans),
        grid=(heads,),
        in_specs=[
            qspec,
            kspec,
            pl.BlockSpec((keys, HEAD), lambda h: (0, heads + h)),
            qspec,
            qspec,
            whole,
            whole,
            pl.BlockSpec((1, keys), lambda h: (0, 0)),
            qtab,
            qtab,
            ktab,
            ktab,
        ],
        out_specs=[qspec, kspec, kspec],
        out_shape=[
            jax.ShapeDtypeStruct(query.shape, bf16),
            jax.ShapeDtypeStruct((keys, features), bf16),
            jax.ShapeDtypeStruct((keys, features), bf16),
        ],
        scratch_shapes=[
            pltpu.VMEM((blocks, slots, keys), f32),
            pltpu.VMEM((keys, HEAD), f32),
            pltpu.VMEM((keys, HEAD), f32),
        ],
        cost_estimate=pl.CostEstimate(
            flops=work,
            bytes_accessed=10 * query.size + 4 * kv_low.size,
            transcendentals=slots * sum(spans) * heads,
        ),
        name="attend_back",
    )(query, kv_low, kv_low, grad, lse, place, cont, kcont, qcos, qsin, kcos, ksin)


def unit_kernel(
    x_hbm,
    g_hbm,
    gate_ref,
    up_ref,
    down_ref,
    in_ref,
    out_hbm,
    gg_hbm,
    gu_hbm,
    hid_hbm,
    xbuf,
    gbuf,
    obuf,
    kbuf,
    psend,
    precv,
    ssend,
    frecv,
    relay,
    load_sem,
    store_sem,
    psend_sem,
    precv_sem,
    ssend_sem,
    frecv_sem,
    relay_sem,
):
    rows = xbuf.shape[1]
    chips = ssend.shape[0]
    me = lax.axis_index("dp")
    chip = me // 2
    core = me % 2
    partner = me + 1 - 2 * core

    square = chips == 4
    fold = rows // 32 * 16
    parts = (pl.ds(0, fold), pl.ds(fold, rows - fold))
    incoming = 2 if square else chips - 1

    def target(j):
        if not square:
            return (chip + chips - 1 - j) % chips
        return (chip // 2 + 1 - j % 2) % 2 * 2 + (chip % 2 + 1 - j // 2) % 2

    def peer(j):
        return {"dp": target(j) * 2 + core}

    meets = (1, 2) if square else range(chips - 1)
    barrier = pltpu.get_barrier_semaphore()
    pl.semaphore_signal(barrier, inc=1, device_id={"dp": partner}, device_id_type=MESH)
    for j in meets:
        pl.semaphore_signal(barrier, inc=1, device_id=peer(j), device_id_type=MESH)
    pl.semaphore_wait(barrier, 1 + incoming)

    def block_rows(j, own):
        block = target(j) * 2 + (core if own else 1 - core)
        return pl.ds(pl.multiple_of(block * rows, 8), rows)

    def loads(j, own):
        span, slot = block_rows(j, own), int(own)
        return [
            pltpu.make_async_copy(x_hbm.at[span], xbuf.at[slot], load_sem.at[0, slot]),
            pltpu.make_async_copy(g_hbm.at[span], gbuf.at[slot], load_sem.at[1, slot]),
        ]

    def stores(j, own):
        span, slot = block_rows(j, own), int(own)
        return [pltpu.make_async_copy(obuf.at[slot], out_hbm.at[span], store_sem.at[0, slot])] + [
            pltpu.make_async_copy(kbuf.at[slot, i], dst.at[span], store_sem.at[1 + i, slot])
            for i, dst in enumerate((gg_hbm, gu_hbm, hid_hbm))
        ]

    def to_partner(j):
        return pltpu.make_async_remote_copy(
            src_ref=psend.at[j % 2],
            dst_ref=precv.at[j],
            send_sem=psend_sem.at[j % 2],
            recv_sem=precv_sem.at[j],
            device_id={"dp": partner},
            device_id_type=MESH,
        )

    def to_owner(j):
        return pltpu.make_async_remote_copy(
            src_ref=ssend.at[j],
            dst_ref=frecv.at[j - 1 if square else j],
            send_sem=ssend_sem.at[j],
            recv_sem=frecv_sem.at[j],
            device_id=peer(j),
            device_id_type=MESH,
        )

    def to_relay(part):
        return pltpu.make_async_remote_copy(
            src_ref=ssend.at[0, parts[part]],
            dst_ref=relay.at[parts[part]],
            send_sem=relay_sem.at[0, part],
            recv_sem=relay_sem.at[1, part],
            device_id=peer(1 + part),
            device_id_type=MESH,
        )

    def compute(j, own):
        slot = int(own)
        for copy in loads(j, own):
            copy.wait()
        rows_in, rows_grad = xbuf[slot], gbuf[slot]
        gate_val = dot_nt(rows_in, gate_ref[...])
        up_val = dot_nt(rows_in, up_ref[...])
        grad_hidden = dot_nt(rows_grad, down_ref[...])
        sigma = jax.nn.sigmoid(gate_val)
        active = gate_val * sigma
        hidden = (active * up_val).astype(bf16)
        grad_gate = (grad_hidden * up_val * sigma * (1.0 + gate_val * (1.0 - sigma))).astype(bf16)
        grad_up = (grad_hidden * active).astype(bf16)

        @pl.when(j > 0)
        def _():
            for copy in stores(j - 1, own):
                copy.wait()

        kbuf[slot, 0] = grad_gate
        kbuf[slot, 1] = grad_up
        kbuf[slot, 2] = hidden
        obuf[slot] = dot_nn(hidden, down_ref[...]).astype(bf16)
        for copy in stores(j, own):
            copy.start()
        return dot_nn(grad_gate, gate_ref[...]) + dot_nn(grad_up, up_ref[...])

    for copy in loads(0, False):
        copy.start()

    def step(j, carry):
        for copy in loads(j, True):
            copy.start()
        term = compute(j, False)

        @pl.when(j > 1)
        def _():
            to_partner(j - 2).wait_send()

        psend[j % 2] = term.astype(bf16)
        to_partner(j).start()

        @pl.when(j < chips - 1)
        def _():
            for copy in loads(j + 1, False):
                copy.start()

        term = compute(j, True)
        to_partner(j).wait_recv()
        ssend[j] = (term + precv[j].astype(f32)).astype(bf16)
        if square:

            @pl.when(j == 0)
            def _():
                for part in (0, 1):
                    to_relay(part).start()

            for part in (0, 1):

                @pl.when(j == 2 - part)
                def _():
                    to_relay(part).wait_recv()
                    span = parts[part]
                    ssend[j, span] = (
                        ssend[j, span].astype(f32) + relay[span].astype(f32)
                    ).astype(bf16)

        @pl.when((j < chips - 1) & (j > 0) if square else j < chips - 1)
        def _():
            to_owner(j).start()

        return carry

    lax.fori_loop(0, chips, step, 0)
    total = ssend[chips - 1].astype(f32)
    for slot, j in enumerate(meets):
        to_owner(j).wait_recv()
        total = total + frecv[slot].astype(f32)
    in_ref[...] = total.astype(bf16)
    for j in meets:
        to_owner(j).wait_send()
    if square:
        for part in (0, 1):
            to_relay(part).wait_send()
    for j in range(max(chips - 2, 0), chips):
        to_partner(j).wait_send()
    for own in (False, True):
        for copy in stores(chips - 1, own):
            copy.wait()


def unit_block(rows_in, rows_grad, gate_rows, up_rows, down_rows, owners, number):
    total, width = rows_in.shape
    units = gate_rows.shape[0]
    rows = total // owners
    chips = owners // 2
    hbm = pl.BlockSpec(memory_space=pl.ANY)
    vmem = pl.BlockSpec(memory_space=pltpu.VMEM)
    kept = jax.ShapeDtypeStruct((total, units), bf16)
    return pl.pallas_call(
        unit_kernel,
        in_specs=[hbm, hbm, vmem, vmem, vmem],
        out_specs=[vmem, hbm, hbm, hbm, hbm],
        out_shape=[
            jax.ShapeDtypeStruct((rows, width), bf16),
            jax.ShapeDtypeStruct((total, width), bf16),
            kept,
            kept,
            kept,
        ],
        scratch_shapes=[
            pltpu.VMEM((2, rows, width), bf16),
            pltpu.VMEM((2, rows, width), bf16),
            pltpu.VMEM((2, rows, width), bf16),
            pltpu.VMEM((2, 3, rows, units), bf16),
            pltpu.VMEM((2, rows, width), bf16),
            pltpu.VMEM((chips, rows, width), bf16),
            pltpu.VMEM((chips, rows, width), bf16),
            pltpu.VMEM((2 if chips == 4 else chips - 1, rows, width), bf16),
            pltpu.VMEM((rows if chips == 4 else 16, width), bf16),
            pltpu.SemaphoreType.DMA((2, 2)),
            pltpu.SemaphoreType.DMA((4, 2)),
            pltpu.SemaphoreType.DMA((2,)),
            pltpu.SemaphoreType.DMA((chips,)),
            pltpu.SemaphoreType.DMA((chips,)),
            pltpu.SemaphoreType.DMA((chips,)),
            pltpu.SemaphoreType.DMA((2, 2)),
        ],
        compiler_params=pltpu.CompilerParams(
            collective_id=number, has_side_effects=True, vmem_limit_bytes=67043328
        ),
        cost_estimate=pl.CostEstimate(
            flops=6 * 2 * total * units * width,
            bytes_accessed=2 * (3 * total * width + 3 * total * units + 3 * units * width),
            transcendentals=total * units,
        ),
        name="unit_block",
    )(rows_in, rows_grad, gate_rows, up_rows, down_rows)


def line_kernel(own_ref, *refs):
    all_ref, bounce, up_send, up_recv, down_send, down_recv, local_sem = refs[-7:]
    me = lax.axis_index("expert")
    count = all_ref.shape[0]
    below = jnp.maximum(me - 1, 0)
    above = jnp.minimum(me + 1, count - 1)
    barrier = pltpu.get_barrier_semaphore()

    @pl.when(me > 0)
    def _():
        pl.semaphore_signal(barrier, inc=1, device_id={"expert": below}, device_id_type=MESH)

    @pl.when(me < count - 1)
    def _():
        pl.semaphore_signal(barrier, inc=1, device_id={"expert": above}, device_id_type=MESH)

    inner = (me > 0) & (me < count - 1)

    @pl.when(inner)
    def _():
        pl.semaphore_wait(barrier, 2)

    @pl.when(jnp.logical_not(inner))
    def _():
        pl.semaphore_wait(barrier, 1)

    def upward(step, block):
        return pltpu.make_async_remote_copy(
            src_ref=own_ref if step == 0 else all_ref.at[block],
            dst_ref=all_ref.at[block],
            send_sem=up_send.at[step],
            recv_sem=up_recv.at[step],
            device_id={"expert": above},
            device_id_type=MESH,
        )

    def downward(step, block):
        return pltpu.make_async_remote_copy(
            src_ref=own_ref if step == 0 else all_ref.at[block],
            dst_ref=all_ref.at[block],
            send_sem=down_send.at[step],
            recv_sem=down_recv.at[step],
            device_id={"expert": below},
            device_id_type=MESH,
        )

    steps = range(count - 1)
    for step in steps:
        if step > 0:

            @pl.when(me - step >= 0)
            def _():
                upward(step - 1, jnp.maximum(me - step, 0)).wait_recv()

            @pl.when(me + step < count)
            def _():
                downward(step - 1, jnp.minimum(me + step, count - 1)).wait_recv()

        @pl.when((me - step >= 0) & (me < count - 1))
        def _():
            upward(step, jnp.maximum(me - step, 0)).start()

        @pl.when((me + step < count) & (me > 0))
        def _():
            downward(step, jnp.minimum(me + step, count - 1)).start()

        if step == 0:
            copy = pltpu.make_async_copy(own_ref, bounce, local_sem.at[0])
            copy.start()
            copy.wait()
            copy = pltpu.make_async_copy(bounce, all_ref.at[me], local_sem.at[1])
            copy.start()
            copy.wait()

    @pl.when(me == count - 1)
    def _():
        upward(count - 2, 0).wait_recv()

    @pl.when(me == 0)
    def _():
        downward(count - 2, count - 1).wait_recv()

    for step in steps:

        @pl.when((me - step >= 0) & (me < count - 1))
        def _():
            upward(step, jnp.maximum(me - step, 0)).wait_send()

        @pl.when((me + step < count) & (me > 0))
        def _():
            downward(step, jnp.minimum(me + step, count - 1)).wait_send()


def line_gather(own, experts, number, *waits):
    hbm = pl.BlockSpec(memory_space=pl.ANY)
    steps = (max(experts - 1, 1),)
    return pl.pallas_call(
        line_kernel,
        in_specs=[hbm] * (1 + len(waits)),
        out_specs=hbm,
        out_shape=jax.ShapeDtypeStruct((experts,) + own.shape, own.dtype),
        scratch_shapes=[pltpu.VMEM(own.shape, own.dtype)]
        + [pltpu.SemaphoreType.DMA(steps)] * 4
        + [pltpu.SemaphoreType.DMA((2,))],
        compiler_params=pltpu.CompilerParams(collective_id=number, has_side_effects=True),
        cost_estimate=pl.CostEstimate(
            flops=0, bytes_accessed=4 * experts * own.size, transcendentals=0
        ),
        name="line_gather",
    )(own, *waits)


def hold(value, *others):
    for other in others:
        last = other[(slice(-1, None),) * other.ndim].reshape(())
        value = value + jnp.minimum(jnp.abs(last), 0).astype(value.dtype)
    return value


def exchange(rows):
    return lax.all_to_all(rows, "expert", split_axis=0, concat_axis=0, tiled=True)


def hop_sum(parts, place, count):
    total = lax.dynamic_index_in_dim(parts, place, 0, keepdims=False).astype(f32)
    got = []
    for hop in range(1, count):
        ring = [(i, (i + hop) % count) for i in range(count)]
        piece = lax.dynamic_index_in_dim(parts, (place + hop) % count, 0, keepdims=False)
        got.append(lax.ppermute(piece, "expert", ring))
    for piece in got:
        total = total + piece.astype(f32)
    return total


def after(value, *others):
    return lax.optimization_barrier((value,) + others)[0]


def plane_sum(terms):
    return lax.psum_scatter(terms, "dp", scatter_dimension=0, tiled=True)


def chip_sum(terms, owners):
    chips = owners // 2
    place = lax.axis_index("dp")
    chip, core = place // 2, place % 2
    blocks = terms.reshape(chips, 2, -1, terms.shape[1])
    mine = lax.dynamic_index_in_dim(blocks, core, 1, keepdims=False)
    other = lax.dynamic_index_in_dim(blocks, 1 - core, 1, keepdims=False)
    other = lax.ppermute(other, "dp", [(i, i + 1 - 2 * (i % 2)) for i in range(owners)])
    mine = (mine.astype(f32) + other.astype(f32)).astype(bf16)
    got = [lax.dynamic_index_in_dim(mine, chip, 0, keepdims=False)]
    for hop in range(1, chips):
        ring = [(i, (i // 2 + hop) % chips * 2 + i % 2) for i in range(owners)]
        piece = lax.dynamic_index_in_dim(mine, (chip + hop) % chips, 0, keepdims=False)
        got.append(lax.ppermute(piece, "dp", ring))
    return sum(piece.astype(f32) for piece in got)


def hops(rows, sign):
    count = rows.shape[0]
    pieces = [rows[0]]
    for hop in range(1, count):
        ring = [(i, (i + sign * hop) % count) for i in range(count)]
        pieces.append(lax.ppermute(rows[hop], "expert", ring))
    return jnp.stack(pieces)


def spread(rows, axes, count):
    copies = jnp.broadcast_to(rows[None], (count,) + rows.shape)
    return lax.all_to_all(copies, axes, split_axis=0, concat_axis=0, tiled=True)


def layer(
    layer_input,
    cotangent,
    cont_ids,
    attn_routes,
    attn_gates,
    mlp_routes,
    mlp_gates,
    gain_attn,
    gain_mlp,
    kv_weight,
    query_weight,
    output_weight,
    mlp_weight,
):
    experts = lax.axis_size("expert")
    owners = lax.axis_size("dp")
    expert_id = lax.axis_index("expert")
    tok_dev, width = layer_input.shape
    per_token = attn_routes.shape[1]
    capacity = tok_dev * per_token * 9 // (8 * experts)
    slots = -(-capacity // 8) * 8
    slot_total = experts * slots
    group = cont_ids.shape[0]
    features = query_weight.shape[2]
    expert_ids = jnp.arange(experts, dtype=jnp.int32)
    slot_ids = jnp.arange(slots, dtype=jnp.int32)

    kv_part = line_gather(kv_weight, experts, 6).reshape(-1, kv_weight.shape[1])
    kv_full = lax.all_gather(kv_part, "dp", axis=0, tiled=True)
    x_all = line_gather(layer_input, experts, 7, kv_part).reshape(group, width)
    query_full = lax.all_gather(query_weight[:, 0, :], "dp", axis=0, tiled=True)
    output_full = lax.all_gather(output_weight[:, 0, :], "dp", axis=0, tiled=True)
    gains = jnp.concatenate([gain_attn, gain_mlp])[None]
    gains = spread(gains, ("dp", "expert"), owners * experts)
    part_size = gain_attn.shape[0]
    gains = gains.reshape(owners * experts, 2, part_size)
    gain_one = gains[:, 0].reshape(-1).astype(f32)
    gain_two = gains[:, 1].reshape(-1).astype(f32)

    hop_ids = (expert_id + expert_ids) % experts
    mlp_hot = mlp_routes.T[:, None, :] == hop_ids[None, :, None]
    mlp_mine = jnp.any(mlp_hot, axis=0)
    mlp_rank = before_counts(mlp_mine)
    mlp_pick = mlp_mine[:, None, :] & (mlp_rank[:, None, :] == slot_ids[None, :, None])
    mlp_gate_tok = jnp.sum(jnp.where(mlp_hot, mlp_gates.T[:, None, :], 0.0), axis=0)
    mlp_slot_gate = jnp.sum(jnp.where(mlp_pick, mlp_gate_tok[:, None, :], 0.0), axis=2)
    mlp_pick_low = mlp_pick.astype(bf16).reshape(slot_total, tok_dev)
    mlp_choice = [
        (mlp_pick & mlp_hot[k][:, None, :]).astype(bf16).reshape(slot_total, tok_dev)
        for k in range(per_token)
    ]
    mlp_back = jnp.concatenate(mlp_choice, axis=1)

    attn_all = attn_routes.reshape(experts, tok_dev, per_token)
    own_mine = jnp.any(attn_all == expert_id, axis=2)
    own_rank = before_counts(own_mine)
    own_pick = own_mine[:, None, :] & (own_rank[:, None, :] == slot_ids[None, :, None])
    own_low = own_pick.astype(bf16)
    places_row, positions_row = token_positions(cont_ids)

    def slot_value(row):
        return jnp.sum(
            jnp.where(own_pick, row.reshape(experts, 1, tok_dev), 0), axis=2, dtype=jnp.int32
        )

    slot_place = slot_value(places_row) + jnp.where(
        jnp.any(own_pick, axis=2), 0, expert_ids[:, None] * tok_dev
    )
    slot_cont = slot_value(cont_ids)
    slot_pos = slot_value(positions_row)
    attn_mine_routes = lax.dynamic_slice_in_dim(attn_routes, expert_id * tok_dev, tok_dev)
    attn_hot = attn_mine_routes.T[:, None, :] == expert_ids[None, :, None]
    attn_mine = jnp.any(attn_hot, axis=0)
    attn_rank = before_counts(attn_mine)
    attn_pick = attn_mine[:, None, :] & (attn_rank[:, None, :] == slot_ids[None, :, None])
    attn_gate_tok = jnp.sum(jnp.where(attn_hot, attn_gates.T[:, None, :], 0.0), axis=0)
    attn_slot_gate = jnp.sum(jnp.where(attn_pick, attn_gate_tok[:, None, :], 0.0), axis=2)
    attn_pick_low = attn_pick.astype(bf16).reshape(slot_total, tok_dev)
    attn_back = jnp.concatenate(
        [
            (attn_pick & attn_hot[k][:, None, :]).astype(bf16).reshape(slot_total, tok_dev)
            for k in range(per_token)
        ],
        axis=1,
    )
    kcos, ksin = rope_tables(positions_row)
    qcos, qsin = rope_tables(slot_pos.reshape(-1))

    cot_rows = dot_nn(mlp_pick_low, cotangent).reshape(experts, slots, width)
    send_grad = (mlp_slot_gate[:, :, None] * cot_rows).astype(bf16)
    steps = slots // 8
    cuts = [0, 8 * max(int(steps * MLP_FIRST), 1), slots]
    pieces = list(zip(cuts[:-1], cuts[1:]))

    def to_plane(rows):
        return lax.all_gather(rows.reshape(-1, width), "dp", axis=0, tiled=True)

    got_grad = hops(hold(send_grad, x_all), 1)

    input_f32 = x_all.astype(f32)
    normed_all, _ = rms_parts(input_f32)
    hidden_all = (normed_all * gain_one).astype(bf16)
    query_rows = lax.dot_general(
        own_low,
        hidden_all.reshape(experts, tok_dev, width),
        (((2,), (1,)), ((0,), (0,))),
        preferred_element_type=f32,
    ).astype(bf16).reshape(slot_total, width)
    query_low = project(
        query_rows, query_full, qcos, qsin, features, slot_total
    ).reshape(experts, slots, features)
    kv_low = project(hidden_all, kv_full, kcos, ksin, features, tok_dev)
    got_grad = hold(got_grad, kv_low)
    plane_grad = [to_plane(got_grad[:, low:high, :]) for low, high in pieces]
    slot_place3 = slot_place[:, :, None]
    slot_cont3 = slot_cont[:, :, None]
    key_cont = cont_ids[None, :]
    attn_low, lse = attend(query_low, kv_low, slot_place3, slot_cont3, key_cont, tok_dev)
    attn_flat = attn_low.reshape(slot_total, features)
    result_low = dot_nn(attn_flat, output_full).astype(bf16)
    result_back = exchange(result_low.reshape(experts, slots, width)).reshape(slot_total, width)
    result_tok = dot_tn(attn_back, result_back)
    own_f32 = layer_input.astype(f32)
    residual = own_f32
    for k in range(per_token):
        residual = residual + attn_gates[:, k : k + 1] * result_tok[k * tok_dev : (k + 1) * tok_dev]
    normed_two, scale_two = rms_parts(residual)
    second_low = (normed_two * gain_two).astype(bf16)

    send_in = dot_nn(mlp_pick_low, second_low).astype(bf16).reshape(experts, slots, width)
    gate_rows, up_rows, down_rows = (mlp_weight[:, 0, j, :] for j in range(3))
    plane_in = [to_plane(hops(send_in[:, low:high, :], 1)) for low, high in pieces]
    kept, out_parts, in_parts = [], [], []
    for number, (rows_in, rows_grad) in enumerate(zip(plane_in, plane_grad)):
        in_part, out_part, *keep = unit_block(
            rows_in, rows_grad, gate_rows, up_rows, down_rows, owners, number
        )
        in_parts.append(in_part)
        out_parts.append(out_part)
        kept.append(keep)

    def join(parts):
        back = []
        for part, (low, high) in zip(parts, pieces):
            back.append(hops(part.reshape(experts, high - low, width), -1))
        return jnp.concatenate(back, axis=1).reshape(slot_total, width)

    in_back = join(in_parts)
    grad_mlp = [dot_tn(k, r) for k, r in zip(kept[0], (plane_in[0], plane_in[0], plane_grad[0]))]
    grad_second = dot_tn(mlp_pick_low, after(in_back, *grad_mlp))
    cot_f32 = cotangent.astype(f32)
    grad_resid = cot_f32 + rms_back(grad_second, normed_two, scale_two, gain_two)

    cot_slots = dot_nn(attn_pick_low, grad_resid.astype(bf16)).reshape(experts, slots, width)
    send_cot = (attn_slot_gate[:, :, None] * cot_slots).astype(bf16)
    for j, rows in enumerate((plane_in[1], plane_in[1], plane_grad[1])):
        grad_mlp[j] = grad_mlp[j] + dot_tn(kept[1][j], rows)
    grad_mlp_weight = jnp.stack(grad_mlp, axis=1)[:, None, :, :]
    grad_result = after(exchange(send_cot), grad_mlp_weight).reshape(slot_total, width)
    grad_attn = dot_nt(grad_result, output_full).astype(bf16)
    output_term = dot_tn(attn_flat, grad_result).astype(bf16)
    grad_output_w = chip_sum(output_term, owners)
    out_back = join([plane_sum(after(part, *in_parts)) for part in out_parts])
    grad_query, grad_keys, grad_values = attend_back(
        query_low,
        kv_low,
        grad_attn.reshape(experts, slots, features),
        lse,
        slot_place3,
        slot_cont3,
        key_cont,
        qcos.reshape(experts, slots, HEAD),
        qsin.reshape(experts, slots, HEAD),
        kcos,
        ksin,
        tok_dev,
    )
    grad_query = grad_query.reshape(slot_total, features)
    mixed_tok = dot_tn(mlp_back, out_back)
    final = residual
    for k in range(per_token):
        final = final + mlp_gates[:, k : k + 1] * mixed_tok[k * tok_dev : (k + 1) * tok_dev]
    output = final.astype(bf16)

    grad_keys_w = dot_tn(hidden_all, grad_keys).astype(bf16)
    grad_values_w = dot_tn(hidden_all, grad_values).astype(bf16)
    grad_query = hold(grad_query, grad_keys_w, grad_values_w)
    grad_kv_w = [plane_sum(grad_keys_w), plane_sum(grad_values_w)]

    grad_rows = dot_nt(grad_query, query_full).astype(bf16)
    half = width // 2
    grad_h, grad_first = [], []
    for low in (0, half):
        span = slice(low, low + half)
        routed = lax.dot_general(
            own_low,
            grad_rows[:, span].reshape(experts, slots, half),
            (((1,), (1,)), ((0,), (0,))),
            preferred_element_type=f32,
        ).reshape(group, half)
        part = (
            dot_nt(grad_keys, kv_full[span, :features])
            + dot_nt(grad_values, kv_full[span, features:])
            + routed
        )
        grad_h.append(part)
        grad_first.append(
            hop_sum(part.astype(bf16).reshape(experts, tok_dev, half), expert_id, experts)
        )
    query_term = dot_tn(query_rows, hold(grad_query, grad_h[1])).astype(bf16)
    grad_query_w = chip_sum(query_term, owners)
    grad_kv_w = jnp.concatenate(
        [hop_sum(part.reshape(experts, -1, features), expert_id, experts) for part in grad_kv_w],
        axis=1,
    )
    grad_h = lax.optimization_barrier(tuple(grad_h))
    grad_gain_one = [
        jnp.sum(part * normed_all[:, low : low + half], axis=0)
        for part, low in zip(grad_h, (0, half))
    ]
    grad_gain_two = jnp.sum(grad_second * normed_two, axis=0)
    first_sum = grad_first[0]
    grad_first = jnp.concatenate(grad_first, axis=1)
    normed_one, scale_one = rms_parts(own_f32)
    grad_input = grad_resid + rms_back(grad_first, normed_one, scale_one, gain_one)

    gain_rows = jnp.concatenate(
        [
            jnp.concatenate(grad_gain_one).reshape(owners * experts, part_size),
            grad_gain_two.reshape(owners * experts, part_size),
        ],
        axis=1,
    )
    gain_rows = lax.all_to_all(
        hold(gain_rows, first_sum)[:, None, :], ("dp", "expert"), split_axis=0, concat_axis=0, tiled=True
    )
    gain_rows = jnp.sum(gain_rows, axis=(0, 1))
    grad_gain_attn, grad_gain_mlp = gain_rows[:part_size], gain_rows[part_size:]
    return (
        output,
        grad_input,
        grad_gain_attn,
        grad_gain_mlp,
        grad_kv_w,
        grad_query_w[:, None, :],
        grad_output_w[:, None, :],
        grad_mlp_weight,
    )


def solution(mesh):
    placed = (
        P(("dp", "expert"), None),
        P(("dp", "expert"), None),
        P("dp"),
        P("dp", None),
        P(("dp", "expert"), None),
        P(("dp", "expert"), None),
        P(("dp", "expert"), None),
        P(("dp", "expert")),
        P(("dp", "expert")),
        P(("dp", "expert"), None),
        P("dp", "expert", None),
        P("dp", "expert", None),
        P("dp", "expert", None, None),
    )
    return jax.shard_map(
        layer,
        mesh=mesh,
        in_specs=placed,
        out_specs=(
            P(("dp", "expert"), None),
            P(("dp", "expert"), None),
            P(("dp", "expert")),
            P(("dp", "expert")),
            P(("dp", "expert"), None),
            P("dp", "expert", None),
            P("dp", "expert", None),
            P("dp", "expert", None, None),
        ),
        check_vma=False,
    )
```

```python
import functools
import math

import jax
import jax.numpy as jnp
from jax import lax
from jax.experimental import pallas as pl
from jax.experimental.pallas import tpu as pltpu
from jax.sharding import PartitionSpec as P


HEAD = 128
PROMPT = 1024
CONTS = 2
GROUP_TOK = 1280
MLP_CUTS = (0.27, 0.61)

norm_eps = 1e-06
rope_base = 10000.0
neg_fill = -1e30
log2e = 1.4426950408889634
MESH = pl.DeviceIdType.MESH
contract_last = (((1,), (1,)), ((), ()))
contract_first = (((0,), (0,)), ((), ()))
f32 = jnp.float32
bf16 = jnp.bfloat16


def rope_tables(positions):
    half_size = HEAD // 2
    freq_steps = jnp.arange(half_size, dtype=f32)
    inverse_freq = jnp.exp(-math.log(rope_base) * 2.0 * freq_steps / HEAD)
    angles = positions.astype(f32)[:, None] * inverse_freq[None, :]
    cosine, sine = jnp.cos(angles), jnp.sin(angles)
    return (
        jnp.concatenate([cosine, cosine], axis=1),
        jnp.concatenate([-sine, sine], axis=1),
    )


def token_positions(cont_ids):
    row_count = cont_ids.shape[0]
    group_count = row_count // GROUP_TOK
    places = jnp.arange(row_count, dtype=jnp.int32) % GROUP_TOK
    labels = jnp.arange(CONTS + 1, dtype=jnp.int32)
    one_hot = (cont_ids[:, None] == labels[None, :]).astype(jnp.int32)
    counts = jnp.sum(one_hot.reshape(group_count, GROUP_TOK, CONTS + 1), axis=1)
    starts = jnp.cumsum(counts, axis=1) - counts
    starts_tok = jnp.broadcast_to(starts[:, None, :], (group_count, GROUP_TOK, CONTS + 1)).reshape(
        row_count, CONTS + 1
    )
    start_of = jnp.sum(starts_tok * one_hot, axis=1)
    return (places, places - start_of + PROMPT * (cont_ids > 0).astype(jnp.int32))


def rms_parts(values):
    row_scale = lax.rsqrt(jnp.mean(values * values, axis=-1, keepdims=True) + norm_eps)
    return (values * row_scale, row_scale)


def rms_back(grad_out, normed, row_scale, gain_vec):
    through = grad_out * gain_vec
    grad_in = row_scale * (through - normed * jnp.mean(through * normed, axis=-1, keepdims=True))
    return grad_in


def dot_nt(left, right):
    return lax.dot_general(left, right, contract_last, preferred_element_type=f32)


def dot_tn(left, right):
    return lax.dot_general(left, right, contract_first, preferred_element_type=f32)


def dot_nn(left, right):
    return jnp.dot(left, right, preferred_element_type=f32)


def before_counts(flags):
    count = flags.shape[-1]
    steps = jnp.arange(count, dtype=jnp.int32)
    earlier = (steps[:, None] < steps[None, :]).astype(bf16)
    return jnp.dot(flags.astype(bf16), earlier, preferred_element_type=f32).astype(jnp.int32)


def project_kernel(rope_blocks, tile, x_ref, w_ref, cos_ref, sin_ref, out_ref):
    rows = x_ref.shape[0]
    turn = pl.program_id(0) < rope_blocks
    for start in range(0, rows, tile):
        span = pl.ds(start, tile)
        product = jnp.dot(x_ref[span, :], w_ref[...], preferred_element_type=f32)

        @pl.when(turn)
        def _():
            cosine, sine = cos_ref[span, :], sin_ref[span, :]
            for col in range(0, product.shape[1], HEAD):
                piece = product[:, col : col + HEAD]
                turned = piece * cosine + pltpu.roll(piece, HEAD // 2, 1) * sine
                out_ref[span, col : col + HEAD] = turned.astype(bf16)

        @pl.when(jnp.logical_not(turn))
        def _():
            out_ref[span, :] = product.astype(bf16)


def project(rows, weight, cosine, sine, rope_cols, tile):
    count, width = rows.shape
    cols = weight.shape[1]
    block = 512
    return pl.pallas_call(
        functools.partial(project_kernel, rope_cols // block, tile),
        grid=(cols // block,),
        in_specs=[
            pl.BlockSpec((count, width), lambda i: (0, 0)),
            pl.BlockSpec((width, block), lambda i: (0, i)),
            pl.BlockSpec((count, HEAD), lambda i: (0, 0)),
            pl.BlockSpec((count, HEAD), lambda i: (0, 0)),
        ],
        out_specs=pl.BlockSpec((count, block), lambda i: (0, i)),
        out_shape=jax.ShapeDtypeStruct((count, cols), bf16),
        cost_estimate=pl.CostEstimate(
            flops=2 * count * width * cols,
            bytes_accessed=2 * (count * width + width * cols + count * cols),
            transcendentals=0,
        ),
    )(rows, weight, cosine, sine)


def key_spans(blocks, tokens, keys):
    return [min(-(-(tokens * (s + 1)) // 128) * 128, keys) for s in range(blocks)]


def fill_bias(bias, place_ref, cont_ref, kcont_ref):
    blocks, slots, keys = bias.shape
    kplace = lax.broadcasted_iota(jnp.int32, (slots, keys), 1)
    kcont = kcont_ref[...]
    for s in range(blocks):
        allowed = (kplace <= place_ref[s]) & ((kcont == 0) | (kcont == cont_ref[s]))
        bias[s] = jnp.where(allowed, 0.0, neg_fill)


def attend_kernel(spans, q_ref, k_ref, v_ref, place_ref, cont_ref, kcont_ref, out_ref, lse_ref, bias):
    @pl.when(pl.program_id(0) == 0)
    def _():
        fill_bias(bias, place_ref, cont_ref, kcont_ref)

    scale2 = log2e / math.sqrt(HEAD)
    for s, span in enumerate(spans):
        scores = dot_nt(q_ref[s], k_ref[:span, :]) * scale2 + bias[s, :, :span]
        peak = jnp.max(scores, axis=1, keepdims=True)
        weights = jnp.exp2(scores - peak)
        total = jnp.sum(weights, axis=1, keepdims=True)
        mixed = dot_nn(weights.astype(bf16), v_ref[:span, :])
        out_ref[s] = (mixed / total).astype(bf16)
        lse_ref[s] = jnp.broadcast_to(peak + jnp.log2(total), lse_ref.shape[1:])


def attend(query, kv_low, place, cont, kcont, tokens):
    blocks, slots, features = query.shape
    keys = kv_low.shape[0]
    heads = features // HEAD
    spans = key_spans(blocks, tokens, keys)
    work = 2 * 2 * slots * sum(spans) * HEAD * heads
    qspec = pl.BlockSpec((blocks, slots, HEAD), lambda h: (0, 0, h))
    whole = pl.BlockSpec((blocks, slots, 1), lambda h: (0, 0, 0))
    return pl.pallas_call(
        functools.partial(attend_kernel, spans),
        grid=(heads,),
        in_specs=[
            qspec,
            pl.BlockSpec((keys, HEAD), lambda h: (0, h)),
            pl.BlockSpec((keys, HEAD), lambda h: (0, heads + h)),
            whole,
            whole,
            pl.BlockSpec((1, keys), lambda h: (0, 0)),
        ],
        out_specs=[qspec, qspec],
        out_shape=[
            jax.ShapeDtypeStruct(query.shape, bf16),
            jax.ShapeDtypeStruct(query.shape, f32),
        ],
        scratch_shapes=[pltpu.VMEM((blocks, slots, keys), f32)],
        cost_estimate=pl.CostEstimate(
            flops=work,
            bytes_accessed=4 * query.size + 2 * kv_low.size + 4 * query.size,
            transcendentals=slots * sum(spans) * heads,
        ),
        name="attend",
    )(query, kv_low, kv_low, place, cont, kcont)


def attend_back_kernel(spans, *refs):
    q_ref, k_ref, v_ref, g_ref, lse_ref, place_ref, cont_ref, kcont_ref = refs[:8]
    qcos_ref, qsin_ref, kcos_ref, ksin_ref = refs[8:12]
    dq_ref, dk_ref, dv_ref, bias, dk_sum, dv_sum = refs[12:]

    @pl.when(pl.program_id(0) == 0)
    def _():
        fill_bias(bias, place_ref, cont_ref, kcont_ref)

    scale = 1.0 / math.sqrt(HEAD)
    scale2 = log2e * scale
    last = len(spans) - 1
    for s in range(last, -1, -1):
        span = spans[s]
        query, grad = q_ref[s], g_ref[s]
        keys = k_ref[:span, :]
        scores = dot_nt(query, keys) * scale2 + bias[s, :, :span]
        prob = jnp.exp2(scores - lse_ref[s][:, :1])
        grad_prob = dot_nt(grad, v_ref[:span, :])
        inner = jnp.sum(prob * grad_prob, axis=1, keepdims=True)
        grad_scores = (prob * (grad_prob - inner)).astype(bf16)
        dq = dot_nn(grad_scores, keys) * scale
        dq = dq * qcos_ref[s] - pltpu.roll(dq, HEAD // 2, 1) * qsin_ref[s]
        dq_ref[s] = dq.astype(bf16)
        dk = dot_tn(grad_scores, query)
        dv = dot_tn(prob.astype(bf16), grad)
        if s < last:
            dk_sum[:span, :] += dk
            dv_sum[:span, :] += dv
        else:
            dk_sum[...] = dk
            dv_sum[...] = dv
    dk = dk_sum[...] * scale
    dk_ref[...] = (dk * kcos_ref[...] - pltpu.roll(dk, HEAD // 2, 1) * ksin_ref[...]).astype(bf16)
    dv_ref[...] = dv_sum[...].astype(bf16)


def attend_back(query, kv_low, grad, lse, place, cont, kcont, qcos, qsin, kcos, ksin, tokens):
    blocks, slots, features = query.shape
    keys = kv_low.shape[0]
    heads = features // HEAD
    spans = key_spans(blocks, tokens, keys)
    work = 5 * 2 * slots * sum(spans) * HEAD * heads
    qspec = pl.BlockSpec((blocks, slots, HEAD), lambda h: (0, 0, h))
    kspec = pl.BlockSpec((keys, HEAD), lambda h: (0, h))
    whole = pl.BlockSpec((blocks, slots, 1), lambda h: (0, 0, 0))
    qtab = pl.BlockSpec((blocks, slots, HEAD), lambda h: (0, 0, 0))
    ktab = pl.BlockSpec((keys, HEAD), lambda h: (0, 0))
    return pl.pallas_call(
        functools.partial(attend_back_kernel, spans),
        grid=(heads,),
        in_specs=[
            qspec,
            kspec,
            pl.BlockSpec((keys, HEAD), lambda h: (0, heads + h)),
            qspec,
            qspec,
            whole,
            whole,
            pl.BlockSpec((1, keys), lambda h: (0, 0)),
            qtab,
            qtab,
            ktab,
            ktab,
        ],
        out_specs=[qspec, kspec, kspec],
        out_shape=[
            jax.ShapeDtypeStruct(query.shape, bf16),
            jax.ShapeDtypeStruct((keys, features), bf16),
            jax.ShapeDtypeStruct((keys, features), bf16),
        ],
        scratch_shapes=[
            pltpu.VMEM((blocks, slots, keys), f32),
            pltpu.VMEM((keys, HEAD), f32),
            pltpu.VMEM((keys, HEAD), f32),
        ],
        cost_estimate=pl.CostEstimate(
            flops=work,
            bytes_accessed=10 * query.size + 4 * kv_low.size,
            transcendentals=slots * sum(spans) * heads,
        ),
        name="attend_back",
    )(query, kv_low, kv_low, grad, lse, place, cont, kcont, qcos, qsin, kcos, ksin)


def unit_kernel(
    x_hbm,
    g_hbm,
    gate_ref,
    up_ref,
    down_ref,
    in_ref,
    out_hbm,
    gg_hbm,
    gu_hbm,
    hid_hbm,
    xbuf,
    gbuf,
    obuf,
    kbuf,
    psend,
    precv,
    ssend,
    frecv,
    relay,
    load_sem,
    store_sem,
    psend_sem,
    precv_sem,
    ssend_sem,
    frecv_sem,
    relay_sem,
):
    rows = xbuf.shape[1]
    chips = ssend.shape[0]
    me = lax.axis_index("dp")
    chip = me // 2
    core = me % 2
    partner = me + 1 - 2 * core

    square = chips == 4
    fold = rows // 32 * 16
    parts = (pl.ds(0, fold), pl.ds(fold, rows - fold))
    incoming = 2 if square else chips - 1

    def target(j):
        if not square:
            return (chip + chips - 1 - j) % chips
        return (chip // 2 + 1 - j % 2) % 2 * 2 + (chip % 2 + 1 - j // 2) % 2

    def peer(j):
        return {"dp": target(j) * 2 + core}

    meets = (1, 2) if square else range(chips - 1)
    barrier = pltpu.get_barrier_semaphore()
    pl.semaphore_signal(barrier, inc=1, device_id={"dp": partner}, device_id_type=MESH)
    for j in meets:
        pl.semaphore_signal(barrier, inc=1, device_id=peer(j), device_id_type=MESH)
    pl.semaphore_wait(barrier, 1 + incoming)

    def block_rows(j, own):
        block = target(j) * 2 + (core if own else 1 - core)
        return pl.ds(pl.multiple_of(block * rows, 8), rows)

    def loads(j, own):
        span, slot = block_rows(j, own), int(own)
        return [
            pltpu.make_async_copy(x_hbm.at[span], xbuf.at[slot], load_sem.at[0, slot]),
            pltpu.make_async_copy(g_hbm.at[span], gbuf.at[slot], load_sem.at[1, slot]),
        ]

    def stores(j, own):
        span, slot = block_rows(j, own), int(own)
        return [pltpu.make_async_copy(obuf.at[slot], out_hbm.at[span], store_sem.at[0, slot])] + [
            pltpu.make_async_copy(kbuf.at[slot, i], dst.at[span], store_sem.at[1 + i, slot])
            for i, dst in enumerate((gg_hbm, gu_hbm, hid_hbm))
        ]

    def to_partner(j):
        return pltpu.make_async_remote_copy(
            src_ref=psend.at[j % 2],
            dst_ref=precv.at[j],
            send_sem=psend_sem.at[j % 2],
            recv_sem=precv_sem.at[j],
            device_id={"dp": partner},
            device_id_type=MESH,
        )

    def to_owner(j):
        return pltpu.make_async_remote_copy(
            src_ref=ssend.at[j],
            dst_ref=frecv.at[j - 1 if square else j],
            send_sem=ssend_sem.at[j],
            recv_sem=frecv_sem.at[j],
            device_id=peer(j),
            device_id_type=MESH,
        )

    def to_relay(part):
        return pltpu.make_async_remote_copy(
            src_ref=ssend.at[0, parts[part]],
            dst_ref=relay.at[parts[part]],
            send_sem=relay_sem.at[0, part],
            recv_sem=relay_sem.at[1, part],
            device_id=peer(1 + part),
            device_id_type=MESH,
        )

    def compute(j, own):
        slot = int(own)
        for copy in loads(j, own):
            copy.wait()
        rows_in, rows_grad = xbuf[slot], gbuf[slot]
        gate_val = dot_nt(rows_in, gate_ref[...])
        up_val = dot_nt(rows_in, up_ref[...])
        grad_hidden = dot_nt(rows_grad, down_ref[...])
        sigma = jax.nn.sigmoid(gate_val)
        active = gate_val * sigma
        hidden = (active * up_val).astype(bf16)
        grad_gate = (grad_hidden * up_val * sigma * (1.0 + gate_val * (1.0 - sigma))).astype(bf16)
        grad_up = (grad_hidden * active).astype(bf16)

        @pl.when(j > 0)
        def _():
            for copy in stores(j - 1, own):
                copy.wait()

        kbuf[slot, 0] = grad_gate
        kbuf[slot, 1] = grad_up
        kbuf[slot, 2] = hidden
        obuf[slot] = dot_nn(hidden, down_ref[...]).astype(bf16)
        for copy in stores(j, own):
            copy.start()
        return dot_nn(grad_gate, gate_ref[...]) + dot_nn(grad_up, up_ref[...])

    for copy in loads(0, False):
        copy.start()

    def step(j, carry):
        for copy in loads(j, True):
            copy.start()
        term = compute(j, False)

        @pl.when(j > 1)
        def _():
            to_partner(j - 2).wait_send()

        psend[j % 2] = term.astype(bf16)
        to_partner(j).start()

        @pl.when(j < chips - 1)
        def _():
            for copy in loads(j + 1, False):
                copy.start()

        term = compute(j, True)
        to_partner(j).wait_recv()
        ssend[j] = (term + precv[j].astype(f32)).astype(bf16)
        if square:

            @pl.when(j == 0)
            def _():
                for part in (0, 1):
                    to_relay(part).start()

            for part in (0, 1):

                @pl.when(j == 2 - part)
                def _():
                    to_relay(part).wait_recv()
                    span = parts[part]
                    ssend[j, span] = (
                        ssend[j, span].astype(f32) + relay[span].astype(f32)
                    ).astype(bf16)

        @pl.when((j < chips - 1) & (j > 0) if square else j < chips - 1)
        def _():
            to_owner(j).start()

        return carry

    lax.fori_loop(0, chips, step, 0)
    total = ssend[chips - 1].astype(f32)
    for slot, j in enumerate(meets):
        to_owner(j).wait_recv()
        total = total + frecv[slot].astype(f32)
    in_ref[...] = total.astype(bf16)
    for j in meets:
        to_owner(j).wait_send()
    if square:
        for part in (0, 1):
            to_relay(part).wait_send()
    for j in range(max(chips - 2, 0), chips):
        to_partner(j).wait_send()
    for own in (False, True):
        for copy in stores(chips - 1, own):
            copy.wait()


def unit_block(rows_in, rows_grad, gate_rows, up_rows, down_rows, owners, number):
    total, width = rows_in.shape
    units = gate_rows.shape[0]
    rows = total // owners
    chips = owners // 2
    hbm = pl.BlockSpec(memory_space=pl.ANY)
    vmem = pl.BlockSpec(memory_space=pltpu.VMEM)
    kept = jax.ShapeDtypeStruct((total, units), bf16)
    return pl.pallas_call(
        unit_kernel,
        in_specs=[hbm, hbm, vmem, vmem, vmem],
        out_specs=[vmem, hbm, hbm, hbm, hbm],
        out_shape=[
            jax.ShapeDtypeStruct((rows, width), bf16),
            jax.ShapeDtypeStruct((total, width), bf16),
            kept,
            kept,
            kept,
        ],
        scratch_shapes=[
            pltpu.VMEM((2, rows, width), bf16),
            pltpu.VMEM((2, rows, width), bf16),
            pltpu.VMEM((2, rows, width), bf16),
            pltpu.VMEM((2, 3, rows, units), bf16),
            pltpu.VMEM((2, rows, width), bf16),
            pltpu.VMEM((chips, rows, width), bf16),
            pltpu.VMEM((chips, rows, width), bf16),
            pltpu.VMEM((2 if chips == 4 else chips - 1, rows, width), bf16),
            pltpu.VMEM((rows if chips == 4 else 16, width), bf16),
            pltpu.SemaphoreType.DMA((2, 2)),
            pltpu.SemaphoreType.DMA((4, 2)),
            pltpu.SemaphoreType.DMA((2,)),
            pltpu.SemaphoreType.DMA((chips,)),
            pltpu.SemaphoreType.DMA((chips,)),
            pltpu.SemaphoreType.DMA((chips,)),
            pltpu.SemaphoreType.DMA((2, 2)),
        ],
        compiler_params=pltpu.CompilerParams(
            collective_id=number, has_side_effects=True, vmem_limit_bytes=67043328
        ),
        cost_estimate=pl.CostEstimate(
            flops=6 * 2 * total * units * width,
            bytes_accessed=2 * (3 * total * width + 3 * total * units + 3 * units * width),
            transcendentals=total * units,
        ),
        name="unit_block",
    )(rows_in, rows_grad, gate_rows, up_rows, down_rows)


def line_kernel(own_ref, *refs):
    all_ref, bounce, up_send, up_recv, down_send, down_recv, local_sem = refs[-7:]
    me = lax.axis_index("expert")
    count = all_ref.shape[0]
    below = jnp.maximum(me - 1, 0)
    above = jnp.minimum(me + 1, count - 1)
    barrier = pltpu.get_barrier_semaphore()

    @pl.when(me > 0)
    def _():
        pl.semaphore_signal(barrier, inc=1, device_id={"expert": below}, device_id_type=MESH)

    @pl.when(me < count - 1)
    def _():
        pl.semaphore_signal(barrier, inc=1, device_id={"expert": above}, device_id_type=MESH)

    inner = (me > 0) & (me < count - 1)

    @pl.when(inner)
    def _():
        pl.semaphore_wait(barrier, 2)

    @pl.when(jnp.logical_not(inner))
    def _():
        pl.semaphore_wait(barrier, 1)

    def upward(step, block):
        return pltpu.make_async_remote_copy(
            src_ref=own_ref if step == 0 else all_ref.at[block],
            dst_ref=all_ref.at[block],
            send_sem=up_send.at[step],
            recv_sem=up_recv.at[step],
            device_id={"expert": above},
            device_id_type=MESH,
        )

    def downward(step, block):
        return pltpu.make_async_remote_copy(
            src_ref=own_ref if step == 0 else all_ref.at[block],
            dst_ref=all_ref.at[block],
            send_sem=down_send.at[step],
            recv_sem=down_recv.at[step],
            device_id={"expert": below},
            device_id_type=MESH,
        )

    steps = range(count - 1)
    for step in steps:
        if step > 0:

            @pl.when(me - step >= 0)
            def _():
                upward(step - 1, jnp.maximum(me - step, 0)).wait_recv()

            @pl.when(me + step < count)
            def _():
                downward(step - 1, jnp.minimum(me + step, count - 1)).wait_recv()

        @pl.when((me - step >= 0) & (me < count - 1))
        def _():
            upward(step, jnp.maximum(me - step, 0)).start()

        @pl.when((me + step < count) & (me > 0))
        def _():
            downward(step, jnp.minimum(me + step, count - 1)).start()

        if step == 0:
            copy = pltpu.make_async_copy(own_ref, bounce, local_sem.at[0])
            copy.start()
            copy.wait()
            copy = pltpu.make_async_copy(bounce, all_ref.at[me], local_sem.at[1])
            copy.start()
            copy.wait()

    @pl.when(me == count - 1)
    def _():
        upward(count - 2, 0).wait_recv()

    @pl.when(me == 0)
    def _():
        downward(count - 2, count - 1).wait_recv()

    for step in steps:

        @pl.when((me - step >= 0) & (me < count - 1))
        def _():
            upward(step, jnp.maximum(me - step, 0)).wait_send()

        @pl.when((me + step < count) & (me > 0))
        def _():
            downward(step, jnp.minimum(me + step, count - 1)).wait_send()


def line_gather(own, experts, number, *waits):
    hbm = pl.BlockSpec(memory_space=pl.ANY)
    steps = (max(experts - 1, 1),)
    return pl.pallas_call(
        line_kernel,
        in_specs=[hbm] * (1 + len(waits)),
        out_specs=hbm,
        out_shape=jax.ShapeDtypeStruct((experts,) + own.shape, own.dtype),
        scratch_shapes=[pltpu.VMEM(own.shape, own.dtype)]
        + [pltpu.SemaphoreType.DMA(steps)] * 4
        + [pltpu.SemaphoreType.DMA((2,))],
        compiler_params=pltpu.CompilerParams(collective_id=number, has_side_effects=True),
        cost_estimate=pl.CostEstimate(
            flops=0, bytes_accessed=4 * experts * own.size, transcendentals=0
        ),
        name="line_gather",
    )(own, *waits)


def hold(value, *others):
    for other in others:
        last = other[(slice(-1, None),) * other.ndim].reshape(())
        value = value + jnp.minimum(jnp.abs(last), 0).astype(value.dtype)
    return value


def exchange(rows):
    return lax.all_to_all(rows, "expert", split_axis=0, concat_axis=0, tiled=True)


def hop_sum(parts, place, count):
    total = lax.dynamic_index_in_dim(parts, place, 0, keepdims=False).astype(f32)
    got = []
    for hop in range(1, count):
        ring = [(i, (i + hop) % count) for i in range(count)]
        piece = lax.dynamic_index_in_dim(parts, (place + hop) % count, 0, keepdims=False)
        got.append(lax.ppermute(piece, "expert", ring))
    for piece in got:
        total = total + piece.astype(f32)
    return total


def after(value, *others):
    return lax.optimization_barrier((value,) + others)[0]


def plane_sum(terms):
    return lax.psum_scatter(terms, "dp", scatter_dimension=0, tiled=True)


def chip_sum(terms, owners):
    chips = owners // 2
    place = lax.axis_index("dp")
    chip, core = place // 2, place % 2
    blocks = terms.reshape(chips, 2, -1, terms.shape[1])
    mine = lax.dynamic_index_in_dim(blocks, core, 1, keepdims=False)
    other = lax.dynamic_index_in_dim(blocks, 1 - core, 1, keepdims=False)
    other = lax.ppermute(other, "dp", [(i, i + 1 - 2 * (i % 2)) for i in range(owners)])
    mine = (mine.astype(f32) + other.astype(f32)).astype(bf16)
    got = [lax.dynamic_index_in_dim(mine, chip, 0, keepdims=False)]
    for hop in range(1, chips):
        ring = [(i, (i // 2 + hop) % chips * 2 + i % 2) for i in range(owners)]
        piece = lax.dynamic_index_in_dim(mine, (chip + hop) % chips, 0, keepdims=False)
        got.append(lax.ppermute(piece, "dp", ring))
    return sum(piece.astype(f32) for piece in got)


def hops(rows, sign):
    count = rows.shape[0]
    pieces = [rows[0]]
    for hop in range(1, count):
        ring = [(i, (i + sign * hop) % count) for i in range(count)]
        pieces.append(lax.ppermute(rows[hop], "expert", ring))
    return jnp.stack(pieces)


def spread(rows, axes, count):
    copies = jnp.broadcast_to(rows[None], (count,) + rows.shape)
    return lax.all_to_all(copies, axes, split_axis=0, concat_axis=0, tiled=True)


def layer(
    layer_input,
    cotangent,
    cont_ids,
    attn_routes,
    attn_gates,
    mlp_routes,
    mlp_gates,
    gain_attn,
    gain_mlp,
    kv_weight,
    query_weight,
    output_weight,
    mlp_weight,
):
    experts = lax.axis_size("expert")
    owners = lax.axis_size("dp")
    expert_id = lax.axis_index("expert")
    tok_dev, width = layer_input.shape
    per_token = attn_routes.shape[1]
    capacity = tok_dev * per_token * 9 // (8 * experts)
    slots = -(-capacity // 8) * 8
    slot_total = experts * slots
    group = cont_ids.shape[0]
    features = query_weight.shape[2]
    expert_ids = jnp.arange(experts, dtype=jnp.int32)
    slot_ids = jnp.arange(slots, dtype=jnp.int32)

    kv_part = line_gather(kv_weight, experts, 6).reshape(-1, kv_weight.shape[1])
    kv_full = lax.all_gather(kv_part, "dp", axis=0, tiled=True)
    x_all = line_gather(layer_input, experts, 7, kv_part).reshape(group, width)
    query_full = lax.all_gather(query_weight[:, 0, :], "dp", axis=0, tiled=True)
    output_full = lax.all_gather(output_weight[:, 0, :], "dp", axis=0, tiled=True)
    gains = jnp.concatenate([gain_attn, gain_mlp])[None]
    gains = spread(gains, ("dp", "expert"), owners * experts)
    part_size = gain_attn.shape[0]
    gains = gains.reshape(owners * experts, 2, part_size)
    gain_one = gains[:, 0].reshape(-1).astype(f32)
    gain_two = gains[:, 1].reshape(-1).astype(f32)

    hop_ids = (expert_id + expert_ids) % experts
    mlp_hot = mlp_routes.T[:, None, :] == hop_ids[None, :, None]
    mlp_mine = jnp.any(mlp_hot, axis=0)
    mlp_rank = before_counts(mlp_mine)
    mlp_pick = mlp_mine[:, None, :] & (mlp_rank[:, None, :] == slot_ids[None, :, None])
    mlp_gate_tok = jnp.sum(jnp.where(mlp_hot, mlp_gates.T[:, None, :], 0.0), axis=0)
    mlp_slot_gate = jnp.sum(jnp.where(mlp_pick, mlp_gate_tok[:, None, :], 0.0), axis=2)
    mlp_pick_low = mlp_pick.astype(bf16).reshape(slot_total, tok_dev)
    mlp_choice = [
        (mlp_pick & mlp_hot[k][:, None, :]).astype(bf16).reshape(slot_total, tok_dev)
        for k in range(per_token)
    ]
    mlp_back = jnp.concatenate(mlp_choice, axis=1)

    attn_all = attn_routes.reshape(experts, tok_dev, per_token)
    own_mine = jnp.any(attn_all == expert_id, axis=2)
    own_rank = before_counts(own_mine)
    own_pick = own_mine[:, None, :] & (own_rank[:, None, :] == slot_ids[None, :, None])
    own_low = own_pick.astype(bf16)
    places_row, positions_row = token_positions(cont_ids)

    def slot_value(row):
        return jnp.sum(
            jnp.where(own_pick, row.reshape(experts, 1, tok_dev), 0), axis=2, dtype=jnp.int32
        )

    slot_place = slot_value(places_row) + jnp.where(
        jnp.any(own_pick, axis=2), 0, expert_ids[:, None] * tok_dev
    )
    slot_cont = slot_value(cont_ids)
    slot_pos = slot_value(positions_row)
    attn_mine_routes = lax.dynamic_slice_in_dim(attn_routes, expert_id * tok_dev, tok_dev)
    attn_hot = attn_mine_routes.T[:, None, :] == expert_ids[None, :, None]
    attn_mine = jnp.any(attn_hot, axis=0)
    attn_rank = before_counts(attn_mine)
    attn_pick = attn_mine[:, None, :] & (attn_rank[:, None, :] == slot_ids[None, :, None])
    attn_gate_tok = jnp.sum(jnp.where(attn_hot, attn_gates.T[:, None, :], 0.0), axis=0)
    attn_slot_gate = jnp.sum(jnp.where(attn_pick, attn_gate_tok[:, None, :], 0.0), axis=2)
    attn_pick_low = attn_pick.astype(bf16).reshape(slot_total, tok_dev)
    attn_back = jnp.concatenate(
        [
            (attn_pick & attn_hot[k][:, None, :]).astype(bf16).reshape(slot_total, tok_dev)
            for k in range(per_token)
        ],
        axis=1,
    )
    kcos, ksin = rope_tables(positions_row)
    qcos, qsin = rope_tables(slot_pos.reshape(-1))

    cot_rows = dot_nn(mlp_pick_low, cotangent).reshape(experts, slots, width)
    send_grad = (mlp_slot_gate[:, :, None] * cot_rows).astype(bf16)
    steps = slots // 8
    cuts = [0] + [8 * int(steps * cut) for cut in MLP_CUTS] + [slots]
    pieces = list(zip(cuts[:-1], cuts[1:]))

    def to_plane(rows):
        return lax.all_gather(rows.reshape(-1, width), "dp", axis=0, tiled=True)

    got_grad = hops(hold(send_grad, x_all), 1)

    input_f32 = x_all.astype(f32)
    normed_all, _ = rms_parts(input_f32)
    hidden_all = (normed_all * gain_one).astype(bf16)
    query_rows = lax.dot_general(
        own_low,
        hidden_all.reshape(experts, tok_dev, width),
        (((2,), (1,)), ((0,), (0,))),
        preferred_element_type=f32,
    ).astype(bf16).reshape(slot_total, width)
    query_low = project(
        query_rows, query_full, qcos, qsin, features, slot_total
    ).reshape(experts, slots, features)
    kv_low = project(hidden_all, kv_full, kcos, ksin, features, tok_dev)
    got_grad = hold(got_grad, kv_low)
    plane_grad = [to_plane(got_grad[:, low:high, :]) for low, high in pieces]
    slot_place3 = slot_place[:, :, None]
    slot_cont3 = slot_cont[:, :, None]
    key_cont = cont_ids[None, :]
    attn_low, lse = attend(query_low, kv_low, slot_place3, slot_cont3, key_cont, tok_dev)
    attn_flat = attn_low.reshape(slot_total, features)
    result_low = dot_nn(attn_flat, output_full).astype(bf16)
    result_back = exchange(result_low.reshape(experts, slots, width)).reshape(slot_total, width)
    result_tok = dot_tn(attn_back, result_back)
    own_f32 = layer_input.astype(f32)
    residual = own_f32
    for k in range(per_token):
        residual = residual + attn_gates[:, k : k + 1] * result_tok[k * tok_dev : (k + 1) * tok_dev]
    normed_two, scale_two = rms_parts(residual)
    second_low = (normed_two * gain_two).astype(bf16)

    send_in = dot_nn(mlp_pick_low, second_low).astype(bf16).reshape(experts, slots, width)
    gate_rows, up_rows, down_rows = (mlp_weight[:, 0, j, :] for j in range(3))
    plane_in = []
    for low, high in pieces:
        got_in = hops(send_in[:, low:high, :], 1)
        plane_in.append(to_plane(got_in))
    kept, out_parts, in_parts = [], [], []
    for number, (rows_in, rows_grad) in enumerate(zip(plane_in, plane_grad)):
        in_part, out_part, *keep = unit_block(
            rows_in, rows_grad, gate_rows, up_rows, down_rows, owners, number
        )
        in_parts.append(in_part)
        out_parts.append(out_part)
        kept.append(keep)

    def join(parts):
        back = []
        for part, (low, high) in zip(parts, pieces):
            back.append(hops(part.reshape(experts, high - low, width), -1))
        return jnp.concatenate(back, axis=1).reshape(slot_total, width)

    in_back = join(in_parts)
    grad_mlp = []
    for j, rows in enumerate((plane_in[0], plane_in[0], plane_grad[0])):
        grad_mlp.append(dot_tn(kept[0][j], rows))
    grad_second = dot_tn(mlp_pick_low, in_back)
    cot_f32 = cotangent.astype(f32)
    grad_resid = cot_f32 + rms_back(grad_second, normed_two, scale_two, gain_two)

    cot_slots = dot_nn(attn_pick_low, grad_resid.astype(bf16)).reshape(experts, slots, width)
    send_cot = (attn_slot_gate[:, :, None] * cot_slots).astype(bf16)
    for number in range(1, len(pieces)):
        for j, rows in enumerate((plane_in, plane_in, plane_grad)):
            grad_mlp[j] = grad_mlp[j] + dot_tn(kept[number][j], rows[number])
    grad_mlp_weight = jnp.stack(grad_mlp, axis=1)[:, None, :, :]
    grad_result = after(exchange(send_cot), grad_mlp_weight).reshape(slot_total, width)
    grad_attn = dot_nt(grad_result, output_full).astype(bf16)
    output_term = dot_tn(attn_flat, grad_result).astype(bf16)
    grad_output_w = chip_sum(output_term, owners)
    out_back = join([plane_sum(after(part, *in_parts)) for part in out_parts])
    grad_query, grad_keys, grad_values = attend_back(
        query_low,
        kv_low,
        grad_attn.reshape(experts, slots, features),
        lse,
        slot_place3,
        slot_cont3,
        key_cont,
        qcos.reshape(experts, slots, HEAD),
        qsin.reshape(experts, slots, HEAD),
        kcos,
        ksin,
        tok_dev,
    )
    grad_query = grad_query.reshape(slot_total, features)
    mixed_tok = dot_tn(mlp_back, out_back)
    final = residual
    for k in range(per_token):
        final = final + mlp_gates[:, k : k + 1] * mixed_tok[k * tok_dev : (k + 1) * tok_dev]
    output = final.astype(bf16)

    grad_keys_w = dot_tn(hidden_all, grad_keys).astype(bf16)
    grad_values_w = dot_tn(hidden_all, grad_values).astype(bf16)
    grad_query = hold(grad_query, grad_keys_w, grad_values_w)
    kv_sums = [plane_sum(grad_keys_w), plane_sum(grad_values_w)]

    grad_rows = dot_nt(grad_query, query_full).astype(bf16)
    half = width // 2
    grad_h, grad_first = [], []
    for low in (0, half):
        span = slice(low, low + half)
        routed = lax.dot_general(
            own_low,
            grad_rows[:, span].reshape(experts, slots, half),
            (((1,), (1,)), ((0,), (0,))),
            preferred_element_type=f32,
        ).reshape(group, half)
        part = (
            dot_nt(grad_keys, kv_full[span, :features])
            + dot_nt(grad_values, kv_full[span, features:])
            + routed
        )
        grad_h.append(part)
        grad_first.append(
            hop_sum(part.astype(bf16).reshape(experts, tok_dev, half), expert_id, experts)
        )
    query_term = dot_tn(query_rows, hold(grad_query, grad_h[1])).astype(bf16)
    grad_query_w = chip_sum(query_term, owners)
    grad_kv_w = jnp.concatenate(
        [hop_sum(part.reshape(experts, -1, features), expert_id, experts) for part in kv_sums],
        axis=1,
    )
    grad_h = lax.optimization_barrier(tuple(grad_h))
    grad_gain_one = [
        jnp.sum(part * normed_all[:, low : low + half], axis=0)
        for part, low in zip(grad_h, (0, half))
    ]
    grad_gain_two = jnp.sum(grad_second * normed_two, axis=0)
    grad_first = jnp.concatenate(grad_first, axis=1)
    normed_one, scale_one = rms_parts(own_f32)
    grad_input = grad_resid + rms_back(grad_first, normed_one, scale_one, gain_one)

    gain_rows = jnp.concatenate(
        [
            jnp.concatenate(grad_gain_one).reshape(owners * experts, part_size),
            grad_gain_two.reshape(owners * experts, part_size),
        ],
        axis=1,
    )
    gain_rows = lax.all_to_all(
        hold(gain_rows, kv_sums[1])[:, None, :], ("dp", "expert"), split_axis=0, concat_axis=0, tiled=True
    )
    gain_rows = jnp.sum(gain_rows, axis=(0, 1))
    grad_gain_attn, grad_gain_mlp = gain_rows[:part_size], gain_rows[part_size:]
    return (
        output,
        grad_input,
        grad_gain_attn,
        grad_gain_mlp,
        grad_kv_w,
        grad_query_w[:, None, :],
        grad_output_w[:, None, :],
        grad_mlp_weight,
    )


def solution(mesh):
    placed = (
        P(("dp", "expert"), None),
        P(("dp", "expert"), None),
        P("dp"),
        P("dp", None),
        P(("dp", "expert"), None),
        P(("dp", "expert"), None),
        P(("dp", "expert"), None),
        P(("dp", "expert")),
        P(("dp", "expert")),
        P(("dp", "expert"), None),
        P("dp", "expert", None),
        P("dp", "expert", None),
        P("dp", "expert", None, None),
    )
    return jax.shard_map(
        layer,
        mesh=mesh,
        in_specs=placed,
        out_specs=(
            P(("dp", "expert"), None),
            P(("dp", "expert"), None),
            P(("dp", "expert")),
            P(("dp", "expert")),
            P(("dp", "expert"), None),
            P("dp", "expert", None),
            P("dp", "expert", None),
            P("dp", "expert", None, None),
        ),
        check_vma=False,
    )
```

```python
import functools
import math

import jax
import jax.numpy as jnp
from jax import lax
from jax.experimental import pallas as pl
from jax.experimental.pallas import tpu as pltpu
from jax.sharding import PartitionSpec as P


HEAD = 128
PROMPT = 1024
CONTS = 2
GROUP_TOK = 1280
MLP_FIRST = 0.5

norm_eps = 1e-06
rope_base = 10000.0
neg_fill = -1e30
log2e = 1.4426950408889634
MESH = pl.DeviceIdType.MESH
contract_last = (((1,), (1,)), ((), ()))
contract_first = (((0,), (0,)), ((), ()))
f32 = jnp.float32
bf16 = jnp.bfloat16


def rope_tables(positions):
    half_size = HEAD // 2
    freq_steps = jnp.arange(half_size, dtype=f32)
    inverse_freq = jnp.exp(-math.log(rope_base) * 2.0 * freq_steps / HEAD)
    angles = positions.astype(f32)[:, None] * inverse_freq[None, :]
    cosine, sine = jnp.cos(angles), jnp.sin(angles)
    return (
        jnp.concatenate([cosine, cosine], axis=1),
        jnp.concatenate([-sine, sine], axis=1),
    )


def token_positions(cont_ids):
    row_count = cont_ids.shape[0]
    group_count = row_count // GROUP_TOK
    places = jnp.arange(row_count, dtype=jnp.int32) % GROUP_TOK
    labels = jnp.arange(CONTS + 1, dtype=jnp.int32)
    one_hot = (cont_ids[:, None] == labels[None, :]).astype(jnp.int32)
    counts = jnp.sum(one_hot.reshape(group_count, GROUP_TOK, CONTS + 1), axis=1)
    starts = jnp.cumsum(counts, axis=1) - counts
    starts_tok = jnp.broadcast_to(starts[:, None, :], (group_count, GROUP_TOK, CONTS + 1)).reshape(
        row_count, CONTS + 1
    )
    start_of = jnp.sum(starts_tok * one_hot, axis=1)
    return (places, places - start_of + PROMPT * (cont_ids > 0).astype(jnp.int32))


def rms_parts(values):
    row_scale = lax.rsqrt(jnp.mean(values * values, axis=-1, keepdims=True) + norm_eps)
    return (values * row_scale, row_scale)


def rms_back(grad_out, normed, row_scale, gain_vec):
    through = grad_out * gain_vec
    grad_in = row_scale * (through - normed * jnp.mean(through * normed, axis=-1, keepdims=True))
    return grad_in


def dot_nt(left, right):
    return lax.dot_general(left, right, contract_last, preferred_element_type=f32)


def dot_tn(left, right):
    return lax.dot_general(left, right, contract_first, preferred_element_type=f32)


def dot_nn(left, right):
    return jnp.dot(left, right, preferred_element_type=f32)


def before_counts(flags):
    count = flags.shape[-1]
    steps = jnp.arange(count, dtype=jnp.int32)
    earlier = (steps[:, None] < steps[None, :]).astype(bf16)
    return jnp.dot(flags.astype(bf16), earlier, preferred_element_type=f32).astype(jnp.int32)


def project_kernel(rope_blocks, tile, x_ref, w_ref, cos_ref, sin_ref, out_ref):
    rows = x_ref.shape[0]
    turn = pl.program_id(0) < rope_blocks
    for start in range(0, rows, tile):
        span = pl.ds(start, tile)
        product = jnp.dot(x_ref[span, :], w_ref[...], preferred_element_type=f32)

        @pl.when(turn)
        def _():
            cosine, sine = cos_ref[span, :], sin_ref[span, :]
            for col in range(0, product.shape[1], HEAD):
                piece = product[:, col : col + HEAD]
                turned = piece * cosine + pltpu.roll(piece, HEAD // 2, 1) * sine
                out_ref[span, col : col + HEAD] = turned.astype(bf16)

        @pl.when(jnp.logical_not(turn))
        def _():
            out_ref[span, :] = product.astype(bf16)


def project(rows, weight, cosine, sine, rope_cols, tile):
    count, width = rows.shape
    cols = weight.shape[1]
    block = 512
    return pl.pallas_call(
        functools.partial(project_kernel, rope_cols // block, tile),
        grid=(cols // block,),
        in_specs=[
            pl.BlockSpec((count, width), lambda i: (0, 0)),
            pl.BlockSpec((width, block), lambda i: (0, i)),
            pl.BlockSpec((count, HEAD), lambda i: (0, 0)),
            pl.BlockSpec((count, HEAD), lambda i: (0, 0)),
        ],
        out_specs=pl.BlockSpec((count, block), lambda i: (0, i)),
        out_shape=jax.ShapeDtypeStruct((count, cols), bf16),
        cost_estimate=pl.CostEstimate(
            flops=2 * count * width * cols,
            bytes_accessed=2 * (count * width + width * cols + count * cols),
            transcendentals=0,
        ),
    )(rows, weight, cosine, sine)


def key_spans(blocks, tokens, keys):
    return [min(-(-(tokens * (s + 1)) // 128) * 128, keys) for s in range(blocks)]


def fill_bias(bias, place_ref, cont_ref, kcont_ref):
    blocks, slots, keys = bias.shape
    kplace = lax.broadcasted_iota(jnp.int32, (slots, keys), 1)
    kcont = kcont_ref[...]
    for s in range(blocks):
        allowed = (kplace <= place_ref[s]) & ((kcont == 0) | (kcont == cont_ref[s]))
        bias[s] = jnp.where(allowed, 0.0, neg_fill)


def attend_kernel(spans, q_ref, k_ref, v_ref, place_ref, cont_ref, kcont_ref, out_ref, lse_ref, bias):
    @pl.when(pl.program_id(0) == 0)
    def _():
        fill_bias(bias, place_ref, cont_ref, kcont_ref)

    scale2 = log2e / math.sqrt(HEAD)
    for s, span in enumerate(spans):
        scores = dot_nt(q_ref[s], k_ref[:span, :]) * scale2 + bias[s, :, :span]
        peak = jnp.max(scores, axis=1, keepdims=True)
        weights = jnp.exp2(scores - peak)
        total = jnp.sum(weights, axis=1, keepdims=True)
        mixed = dot_nn(weights.astype(bf16), v_ref[:span, :])
        out_ref[s] = (mixed / total).astype(bf16)
        lse_ref[s] = jnp.broadcast_to(peak + jnp.log2(total), lse_ref.shape[1:])


def attend(query, kv_low, place, cont, kcont, tokens):
    blocks, slots, features = query.shape
    keys = kv_low.shape[0]
    heads = features // HEAD
    spans = key_spans(blocks, tokens, keys)
    work = 2 * 2 * slots * sum(spans) * HEAD * heads
    qspec = pl.BlockSpec((blocks, slots, HEAD), lambda h: (0, 0, h))
    whole = pl.BlockSpec((blocks, slots, 1), lambda h: (0, 0, 0))
    return pl.pallas_call(
        functools.partial(attend_kernel, spans),
        grid=(heads,),
        in_specs=[
            qspec,
            pl.BlockSpec((keys, HEAD), lambda h: (0, h)),
            pl.BlockSpec((keys, HEAD), lambda h: (0, heads + h)),
            whole,
            whole,
            pl.BlockSpec((1, keys), lambda h: (0, 0)),
        ],
        out_specs=[qspec, qspec],
        out_shape=[
            jax.ShapeDtypeStruct(query.shape, bf16),
            jax.ShapeDtypeStruct(query.shape, f32),
        ],
        scratch_shapes=[pltpu.VMEM((blocks, slots, keys), f32)],
        cost_estimate=pl.CostEstimate(
            flops=work,
            bytes_accessed=4 * query.size + 2 * kv_low.size + 4 * query.size,
            transcendentals=slots * sum(spans) * heads,
        ),
        name="attend",
    )(query, kv_low, kv_low, place, cont, kcont)


def attend_back_kernel(spans, *refs):
    q_ref, k_ref, v_ref, g_ref, lse_ref, place_ref, cont_ref, kcont_ref = refs[:8]
    qcos_ref, qsin_ref, kcos_ref, ksin_ref = refs[8:12]
    dq_ref, dk_ref, dv_ref, bias, dk_sum, dv_sum = refs[12:]

    @pl.when(pl.program_id(0) == 0)
    def _():
        fill_bias(bias, place_ref, cont_ref, kcont_ref)

    scale = 1.0 / math.sqrt(HEAD)
    scale2 = log2e * scale
    last = len(spans) - 1
    for s in range(last, -1, -1):
        span = spans[s]
        query, grad = q_ref[s], g_ref[s]
        keys = k_ref[:span, :]
        scores = dot_nt(query, keys) * scale2 + bias[s, :, :span]
        prob = jnp.exp2(scores - lse_ref[s][:, :1])
        grad_prob = dot_nt(grad, v_ref[:span, :])
        inner = jnp.sum(prob * grad_prob, axis=1, keepdims=True)
        grad_scores = (prob * (grad_prob - inner)).astype(bf16)
        dq = dot_nn(grad_scores, keys) * scale
        dq = dq * qcos_ref[s] - pltpu.roll(dq, HEAD // 2, 1) * qsin_ref[s]
        dq_ref[s] = dq.astype(bf16)
        dk = dot_tn(grad_scores, query)
        dv = dot_tn(prob.astype(bf16), grad)
        if s < last:
            dk_sum[:span, :] += dk
            dv_sum[:span, :] += dv
        else:
            dk_sum[...] = dk
            dv_sum[...] = dv
    dk = dk_sum[...] * scale
    dk_ref[...] = (dk * kcos_ref[...] - pltpu.roll(dk, HEAD // 2, 1) * ksin_ref[...]).astype(bf16)
    dv_ref[...] = dv_sum[...].astype(bf16)


def attend_back(query, kv_low, grad, lse, place, cont, kcont, qcos, qsin, kcos, ksin, tokens):
    blocks, slots, features = query.shape
    keys = kv_low.shape[0]
    heads = features // HEAD
    spans = key_spans(blocks, tokens, keys)
    work = 5 * 2 * slots * sum(spans) * HEAD * heads
    qspec = pl.BlockSpec((blocks, slots, HEAD), lambda h: (0, 0, h))
    kspec = pl.BlockSpec((keys, HEAD), lambda h: (0, h))
    whole = pl.BlockSpec((blocks, slots, 1), lambda h: (0, 0, 0))
    qtab = pl.BlockSpec((blocks, slots, HEAD), lambda h: (0, 0, 0))
    ktab = pl.BlockSpec((keys, HEAD), lambda h: (0, 0))
    return pl.pallas_call(
        functools.partial(attend_back_kernel, spans),
        grid=(heads,),
        in_specs=[
            qspec,
            kspec,
            pl.BlockSpec((keys, HEAD), lambda h: (0, heads + h)),
            qspec,
            qspec,
            whole,
            whole,
            pl.BlockSpec((1, keys), lambda h: (0, 0)),
            qtab,
            qtab,
            ktab,
            ktab,
        ],
        out_specs=[qspec, kspec, kspec],
        out_shape=[
            jax.ShapeDtypeStruct(query.shape, bf16),
            jax.ShapeDtypeStruct((keys, features), bf16),
            jax.ShapeDtypeStruct((keys, features), bf16),
        ],
        scratch_shapes=[
            pltpu.VMEM((blocks, slots, keys), f32),
            pltpu.VMEM((keys, HEAD), f32),
            pltpu.VMEM((keys, HEAD), f32),
        ],
        cost_estimate=pl.CostEstimate(
            flops=work,
            bytes_accessed=10 * query.size + 4 * kv_low.size,
            transcendentals=slots * sum(spans) * heads,
        ),
        name="attend_back",
    )(query, kv_low, kv_low, grad, lse, place, cont, kcont, qcos, qsin, kcos, ksin)


def unit_kernel(
    x_hbm,
    g_hbm,
    gate_ref,
    up_ref,
    down_ref,
    in_ref,
    out_hbm,
    gg_hbm,
    gu_hbm,
    hid_hbm,
    xbuf,
    gbuf,
    obuf,
    kbuf,
    psend,
    precv,
    ssend,
    frecv,
    relay,
    load_sem,
    store_sem,
    psend_sem,
    precv_sem,
    ssend_sem,
    frecv_sem,
    relay_sem,
):
    rows = xbuf.shape[1]
    chips = ssend.shape[0]
    me = lax.axis_index("dp")
    chip = me // 2
    core = me % 2
    partner = me + 1 - 2 * core

    square = chips == 4
    fold = rows // 32 * 16
    parts = (pl.ds(0, fold), pl.ds(fold, rows - fold))
    incoming = 2 if square else chips - 1

    def target(j):
        if not square:
            return (chip + chips - 1 - j) % chips
        return (chip // 2 + 1 - j % 2) % 2 * 2 + (chip % 2 + 1 - j // 2) % 2

    def peer(j):
        return {"dp": target(j) * 2 + core}

    meets = (1, 2) if square else range(chips - 1)
    barrier = pltpu.get_barrier_semaphore()
    pl.semaphore_signal(barrier, inc=1, device_id={"dp": partner}, device_id_type=MESH)
    for j in meets:
        pl.semaphore_signal(barrier, inc=1, device_id=peer(j), device_id_type=MESH)
    pl.semaphore_wait(barrier, 1 + incoming)

    def block_rows(j, own):
        block = target(j) * 2 + (core if own else 1 - core)
        return pl.ds(pl.multiple_of(block * rows, 8), rows)

    def loads(j, own):
        span, slot = block_rows(j, own), int(own)
        return [
            pltpu.make_async_copy(x_hbm.at[span], xbuf.at[slot], load_sem.at[0, slot]),
            pltpu.make_async_copy(g_hbm.at[span], gbuf.at[slot], load_sem.at[1, slot]),
        ]

    def stores(j, own):
        span, slot = block_rows(j, own), int(own)
        return [pltpu.make_async_copy(obuf.at[slot], out_hbm.at[span], store_sem.at[0, slot])] + [
            pltpu.make_async_copy(kbuf.at[slot, i], dst.at[span], store_sem.at[1 + i, slot])
            for i, dst in enumerate((gg_hbm, gu_hbm, hid_hbm))
        ]

    def to_partner(j):
        return pltpu.make_async_remote_copy(
            src_ref=psend.at[j % 2],
            dst_ref=precv.at[j],
            send_sem=psend_sem.at[j % 2],
            recv_sem=precv_sem.at[j],
            device_id={"dp": partner},
            device_id_type=MESH,
        )

    def to_owner(j):
        return pltpu.make_async_remote_copy(
            src_ref=ssend.at[j],
            dst_ref=frecv.at[j - 1 if square else j],
            send_sem=ssend_sem.at[j],
            recv_sem=frecv_sem.at[j],
            device_id=peer(j),
            device_id_type=MESH,
        )

    def to_relay(part):
        return pltpu.make_async_remote_copy(
            src_ref=ssend.at[0, parts[part]],
            dst_ref=relay.at[parts[part]],
            send_sem=relay_sem.at[0, part],
            recv_sem=relay_sem.at[1, part],
            device_id=peer(1 + part),
            device_id_type=MESH,
        )

    def compute(j, own):
        slot = int(own)
        for copy in loads(j, own):
            copy.wait()
        rows_in, rows_grad = xbuf[slot], gbuf[slot]
        gate_val = dot_nt(rows_in, gate_ref[...])
        up_val = dot_nt(rows_in, up_ref[...])
        grad_hidden = dot_nt(rows_grad, down_ref[...])
        sigma = jax.nn.sigmoid(gate_val)
        active = gate_val * sigma
        hidden = (active * up_val).astype(bf16)
        grad_gate = (grad_hidden * up_val * sigma * (1.0 + gate_val * (1.0 - sigma))).astype(bf16)
        grad_up = (grad_hidden * active).astype(bf16)

        @pl.when(j > 0)
        def _():
            for copy in stores(j - 1, own):
                copy.wait()

        kbuf[slot, 0] = grad_gate
        kbuf[slot, 1] = grad_up
        kbuf[slot, 2] = hidden
        obuf[slot] = dot_nn(hidden, down_ref[...]).astype(bf16)
        for copy in stores(j, own):
            copy.start()
        return dot_nn(grad_gate, gate_ref[...]) + dot_nn(grad_up, up_ref[...])

    for copy in loads(0, False):
        copy.start()

    def step(j, carry):
        for copy in loads(j, True):
            copy.start()
        term = compute(j, False)

        @pl.when(j > 1)
        def _():
            to_partner(j - 2).wait_send()

        psend[j % 2] = term.astype(bf16)
        to_partner(j).start()

        @pl.when(j < chips - 1)
        def _():
            for copy in loads(j + 1, False):
                copy.start()

        term = compute(j, True)
        to_partner(j).wait_recv()
        ssend[j] = (term + precv[j].astype(f32)).astype(bf16)
        if square:

            @pl.when(j == 0)
            def _():
                for part in (0, 1):
                    to_relay(part).start()

            for part in (0, 1):

                @pl.when(j == 2 - part)
                def _():
                    to_relay(part).wait_recv()
                    span = parts[part]
                    ssend[j, span] = (
                        ssend[j, span].astype(f32) + relay[span].astype(f32)
                    ).astype(bf16)

        @pl.when((j < chips - 1) & (j > 0) if square else j < chips - 1)
        def _():
            to_owner(j).start()

        return carry

    lax.fori_loop(0, chips, step, 0)
    total = ssend[chips - 1].astype(f32)
    for slot, j in enumerate(meets):
        to_owner(j).wait_recv()
        total = total + frecv[slot].astype(f32)
    in_ref[...] = total.astype(bf16)
    for j in meets:
        to_owner(j).wait_send()
    if square:
        for part in (0, 1):
            to_relay(part).wait_send()
    for j in range(max(chips - 2, 0), chips):
        to_partner(j).wait_send()
    for own in (False, True):
        for copy in stores(chips - 1, own):
            copy.wait()


def unit_block(rows_in, rows_grad, gate_rows, up_rows, down_rows, owners, number):
    total, width = rows_in.shape
    units = gate_rows.shape[0]
    rows = total // owners
    chips = owners // 2
    hbm = pl.BlockSpec(memory_space=pl.ANY)
    vmem = pl.BlockSpec(memory_space=pltpu.VMEM)
    kept = jax.ShapeDtypeStruct((total, units), bf16)
    return pl.pallas_call(
        unit_kernel,
        in_specs=[hbm, hbm, vmem, vmem, vmem],
        out_specs=[vmem, hbm, hbm, hbm, hbm],
        out_shape=[
            jax.ShapeDtypeStruct((rows, width), bf16),
            jax.ShapeDtypeStruct((total, width), bf16),
            kept,
            kept,
            kept,
        ],
        scratch_shapes=[
            pltpu.VMEM((2, rows, width), bf16),
            pltpu.VMEM((2, rows, width), bf16),
            pltpu.VMEM((2, rows, width), bf16),
            pltpu.VMEM((2, 3, rows, units), bf16),
            pltpu.VMEM((2, rows, width), bf16),
            pltpu.VMEM((chips, rows, width), bf16),
            pltpu.VMEM((chips, rows, width), bf16),
            pltpu.VMEM((2 if chips == 4 else chips - 1, rows, width), bf16),
            pltpu.VMEM((rows if chips == 4 else 16, width), bf16),
            pltpu.SemaphoreType.DMA((2, 2)),
            pltpu.SemaphoreType.DMA((4, 2)),
            pltpu.SemaphoreType.DMA((2,)),
            pltpu.SemaphoreType.DMA((chips,)),
            pltpu.SemaphoreType.DMA((chips,)),
            pltpu.SemaphoreType.DMA((chips,)),
            pltpu.SemaphoreType.DMA((2, 2)),
        ],
        compiler_params=pltpu.CompilerParams(
            collective_id=number, has_side_effects=True, vmem_limit_bytes=67043328
        ),
        cost_estimate=pl.CostEstimate(
            flops=6 * 2 * total * units * width,
            bytes_accessed=2 * (3 * total * width + 3 * total * units + 3 * units * width),
            transcendentals=total * units,
        ),
        name="unit_block",
    )(rows_in, rows_grad, gate_rows, up_rows, down_rows)


def line_kernel(own_ref, *refs):
    all_ref, bounce, up_send, up_recv, down_send, down_recv, local_sem = refs[-7:]
    me = lax.axis_index("expert")
    count = all_ref.shape[0]
    below = jnp.maximum(me - 1, 0)
    above = jnp.minimum(me + 1, count - 1)
    barrier = pltpu.get_barrier_semaphore()

    @pl.when(me > 0)
    def _():
        pl.semaphore_signal(barrier, inc=1, device_id={"expert": below}, device_id_type=MESH)

    @pl.when(me < count - 1)
    def _():
        pl.semaphore_signal(barrier, inc=1, device_id={"expert": above}, device_id_type=MESH)

    inner = (me > 0) & (me < count - 1)

    @pl.when(inner)
    def _():
        pl.semaphore_wait(barrier, 2)

    @pl.when(jnp.logical_not(inner))
    def _():
        pl.semaphore_wait(barrier, 1)

    def upward(step, block):
        return pltpu.make_async_remote_copy(
            src_ref=own_ref if step == 0 else all_ref.at[block],
            dst_ref=all_ref.at[block],
            send_sem=up_send.at[step],
            recv_sem=up_recv.at[step],
            device_id={"expert": above},
            device_id_type=MESH,
        )

    def downward(step, block):
        return pltpu.make_async_remote_copy(
            src_ref=own_ref if step == 0 else all_ref.at[block],
            dst_ref=all_ref.at[block],
            send_sem=down_send.at[step],
            recv_sem=down_recv.at[step],
            device_id={"expert": below},
            device_id_type=MESH,
        )

    steps = range(count - 1)
    for step in steps:
        if step > 0:

            @pl.when(me - step >= 0)
            def _():
                upward(step - 1, jnp.maximum(me - step, 0)).wait_recv()

            @pl.when(me + step < count)
            def _():
                downward(step - 1, jnp.minimum(me + step, count - 1)).wait_recv()

        @pl.when((me - step >= 0) & (me < count - 1))
        def _():
            upward(step, jnp.maximum(me - step, 0)).start()

        @pl.when((me + step < count) & (me > 0))
        def _():
            downward(step, jnp.minimum(me + step, count - 1)).start()

        if step == 0:
            copy = pltpu.make_async_copy(own_ref, bounce, local_sem.at[0])
            copy.start()
            copy.wait()
            copy = pltpu.make_async_copy(bounce, all_ref.at[me], local_sem.at[1])
            copy.start()
            copy.wait()

    @pl.when(me == count - 1)
    def _():
        upward(count - 2, 0).wait_recv()

    @pl.when(me == 0)
    def _():
        downward(count - 2, count - 1).wait_recv()

    for step in steps:

        @pl.when((me - step >= 0) & (me < count - 1))
        def _():
            upward(step, jnp.maximum(me - step, 0)).wait_send()

        @pl.when((me + step < count) & (me > 0))
        def _():
            downward(step, jnp.minimum(me + step, count - 1)).wait_send()


def line_gather(own, experts, number, *waits):
    hbm = pl.BlockSpec(memory_space=pl.ANY)
    steps = (max(experts - 1, 1),)
    return pl.pallas_call(
        line_kernel,
        in_specs=[hbm] * (1 + len(waits)),
        out_specs=hbm,
        out_shape=jax.ShapeDtypeStruct((experts,) + own.shape, own.dtype),
        scratch_shapes=[pltpu.VMEM(own.shape, own.dtype)]
        + [pltpu.SemaphoreType.DMA(steps)] * 4
        + [pltpu.SemaphoreType.DMA((2,))],
        compiler_params=pltpu.CompilerParams(collective_id=number, has_side_effects=True),
        cost_estimate=pl.CostEstimate(
            flops=0, bytes_accessed=4 * experts * own.size, transcendentals=0
        ),
        name="line_gather",
    )(own, *waits)


def hold(value, *others):
    for other in others:
        last = other[(slice(-1, None),) * other.ndim].reshape(())
        value = value + jnp.minimum(jnp.abs(last), 0).astype(value.dtype)
    return value


def exchange(rows):
    return lax.all_to_all(rows, "expert", split_axis=0, concat_axis=0, tiled=True)


def hop_sum(parts, place, count):
    total = lax.dynamic_index_in_dim(parts, place, 0, keepdims=False).astype(f32)
    got = []
    for hop in range(1, count):
        ring = [(i, (i + hop) % count) for i in range(count)]
        piece = lax.dynamic_index_in_dim(parts, (place + hop) % count, 0, keepdims=False)
        got.append(lax.ppermute(piece, "expert", ring))
    for piece in got:
        total = total + piece.astype(f32)
    return total


def after(value, *others):
    return lax.optimization_barrier((value,) + others)[0]


def plane_sum(terms):
    return lax.psum_scatter(terms, "dp", scatter_dimension=0, tiled=True)


def chip_sum(terms, owners):
    chips = owners // 2
    place = lax.axis_index("dp")
    chip, core = place // 2, place % 2
    blocks = terms.reshape(chips, 2, -1, terms.shape[1])
    mine = lax.dynamic_index_in_dim(blocks, core, 1, keepdims=False)
    other = lax.dynamic_index_in_dim(blocks, 1 - core, 1, keepdims=False)
    other = lax.ppermute(other, "dp", [(i, i + 1 - 2 * (i % 2)) for i in range(owners)])
    mine = (mine.astype(f32) + other.astype(f32)).astype(bf16)
    got = [lax.dynamic_index_in_dim(mine, chip, 0, keepdims=False)]
    for hop in range(1, chips):
        ring = [(i, (i // 2 + hop) % chips * 2 + i % 2) for i in range(owners)]
        piece = lax.dynamic_index_in_dim(mine, (chip + hop) % chips, 0, keepdims=False)
        got.append(lax.ppermute(piece, "dp", ring))
    return sum(piece.astype(f32) for piece in got)


def hops(rows, sign):
    count = rows.shape[0]
    pieces = [rows[0]]
    for hop in range(1, count):
        ring = [(i, (i + sign * hop) % count) for i in range(count)]
        pieces.append(lax.ppermute(rows[hop], "expert", ring))
    return jnp.stack(pieces)


def spread(rows, axes, count):
    copies = jnp.broadcast_to(rows[None], (count,) + rows.shape)
    return lax.all_to_all(copies, axes, split_axis=0, concat_axis=0, tiled=True)


def layer(
    layer_input,
    cotangent,
    cont_ids,
    attn_routes,
    attn_gates,
    mlp_routes,
    mlp_gates,
    gain_attn,
    gain_mlp,
    kv_weight,
    query_weight,
    output_weight,
    mlp_weight,
):
    experts = lax.axis_size("expert")
    owners = lax.axis_size("dp")
    expert_id = lax.axis_index("expert")
    tok_dev, width = layer_input.shape
    per_token = attn_routes.shape[1]
    capacity = tok_dev * per_token * 9 // (8 * experts)
    slots = -(-capacity // 8) * 8
    slot_total = experts * slots
    group = cont_ids.shape[0]
    features = query_weight.shape[2]
    expert_ids = jnp.arange(experts, dtype=jnp.int32)
    slot_ids = jnp.arange(slots, dtype=jnp.int32)

    kv_part = line_gather(kv_weight, experts, 6).reshape(-1, kv_weight.shape[1])
    kv_full = lax.all_gather(kv_part, "dp", axis=0, tiled=True)
    x_all = line_gather(layer_input, experts, 7, kv_part).reshape(group, width)
    query_full = lax.all_gather(query_weight[:, 0, :], "dp", axis=0, tiled=True)
    output_full = lax.all_gather(output_weight[:, 0, :], "dp", axis=0, tiled=True)
    gains = jnp.concatenate([gain_attn, gain_mlp])[None]
    gains = spread(gains, ("dp", "expert"), owners * experts)
    part_size = gain_attn.shape[0]
    gains = gains.reshape(owners * experts, 2, part_size)
    gain_one = gains[:, 0].reshape(-1).astype(f32)
    gain_two = gains[:, 1].reshape(-1).astype(f32)

    hop_ids = (expert_id + expert_ids) % experts
    mlp_hot = mlp_routes.T[:, None, :] == hop_ids[None, :, None]
    mlp_mine = jnp.any(mlp_hot, axis=0)
    mlp_rank = before_counts(mlp_mine)
    mlp_pick = mlp_mine[:, None, :] & (mlp_rank[:, None, :] == slot_ids[None, :, None])
    mlp_gate_tok = jnp.sum(jnp.where(mlp_hot, mlp_gates.T[:, None, :], 0.0), axis=0)
    mlp_slot_gate = jnp.sum(jnp.where(mlp_pick, mlp_gate_tok[:, None, :], 0.0), axis=2)
    mlp_pick_low = mlp_pick.astype(bf16).reshape(slot_total, tok_dev)
    mlp_choice = [
        (mlp_pick & mlp_hot[k][:, None, :]).astype(bf16).reshape(slot_total, tok_dev)
        for k in range(per_token)
    ]
    mlp_back = jnp.concatenate(mlp_choice, axis=1)

    attn_all = attn_routes.reshape(experts, tok_dev, per_token)
    own_mine = jnp.any(attn_all == expert_id, axis=2)
    own_rank = before_counts(own_mine)
    own_pick = own_mine[:, None, :] & (own_rank[:, None, :] == slot_ids[None, :, None])
    own_low = own_pick.astype(bf16)
    places_row, positions_row = token_positions(cont_ids)

    def slot_value(row):
        return jnp.sum(
            jnp.where(own_pick, row.reshape(experts, 1, tok_dev), 0), axis=2, dtype=jnp.int32
        )

    slot_place = slot_value(places_row) + jnp.where(
        jnp.any(own_pick, axis=2), 0, expert_ids[:, None] * tok_dev
    )
    slot_cont = slot_value(cont_ids)
    slot_pos = slot_value(positions_row)
    attn_mine_routes = lax.dynamic_slice_in_dim(attn_routes, expert_id * tok_dev, tok_dev)
    attn_hot = attn_mine_routes.T[:, None, :] == expert_ids[None, :, None]
    attn_mine = jnp.any(attn_hot, axis=0)
    attn_rank = before_counts(attn_mine)
    attn_pick = attn_mine[:, None, :] & (attn_rank[:, None, :] == slot_ids[None, :, None])
    attn_gate_tok = jnp.sum(jnp.where(attn_hot, attn_gates.T[:, None, :], 0.0), axis=0)
    attn_slot_gate = jnp.sum(jnp.where(attn_pick, attn_gate_tok[:, None, :], 0.0), axis=2)
    attn_pick_low = attn_pick.astype(bf16).reshape(slot_total, tok_dev)
    attn_back = jnp.concatenate(
        [
            (attn_pick & attn_hot[k][:, None, :]).astype(bf16).reshape(slot_total, tok_dev)
            for k in range(per_token)
        ],
        axis=1,
    )
    kcos, ksin = rope_tables(positions_row)
    qcos, qsin = rope_tables(slot_pos.reshape(-1))

    cot_rows = dot_nn(mlp_pick_low, cotangent).reshape(experts, slots, width)
    send_grad = (mlp_slot_gate[:, :, None] * cot_rows).astype(bf16)
    steps = slots // 8
    cuts = [0, 8 * max(int(steps * MLP_FIRST), 1), slots]
    pieces = list(zip(cuts[:-1], cuts[1:]))

    def to_plane(rows):
        return lax.all_gather(rows.reshape(-1, width), "dp", axis=0, tiled=True)

    got_grad = hops(hold(send_grad, x_all), 1)

    input_f32 = x_all.astype(f32)
    normed_all, _ = rms_parts(input_f32)
    hidden_all = (normed_all * gain_one).astype(bf16)
    query_rows = lax.dot_general(
        own_low,
        hidden_all.reshape(experts, tok_dev, width),
        (((2,), (1,)), ((0,), (0,))),
        preferred_element_type=f32,
    ).astype(bf16).reshape(slot_total, width)
    query_low = project(
        query_rows, query_full, qcos, qsin, features, slot_total
    ).reshape(experts, slots, features)
    kv_low = project(hidden_all, kv_full, kcos, ksin, features, tok_dev)
    got_grad = hold(got_grad, kv_low)
    plane_grad = [to_plane(got_grad[:, low:high, :]) for low, high in pieces]
    slot_place3 = slot_place[:, :, None]
    slot_cont3 = slot_cont[:, :, None]
    key_cont = cont_ids[None, :]
    attn_low, lse = attend(query_low, kv_low, slot_place3, slot_cont3, key_cont, tok_dev)
    attn_flat = attn_low.reshape(slot_total, features)
    result_low = dot_nn(attn_flat, output_full).astype(bf16)
    result_back = exchange(result_low.reshape(experts, slots, width)).reshape(slot_total, width)
    result_tok = dot_tn(attn_back, result_back)
    own_f32 = layer_input.astype(f32)
    residual = own_f32
    for k in range(per_token):
        residual = residual + attn_gates[:, k : k + 1] * result_tok[k * tok_dev : (k + 1) * tok_dev]
    normed_two, scale_two = rms_parts(residual)
    second_low = (normed_two * gain_two).astype(bf16)

    send_in = dot_nn(mlp_pick_low, second_low).astype(bf16).reshape(experts, slots, width)
    gate_rows, up_rows, down_rows = (mlp_weight[:, 0, j, :] for j in range(3))
    plane_in = [to_plane(hops(send_in[:, low:high, :], 1)) for low, high in pieces]
    kept, out_parts, in_parts = [], [], []
    for number, (rows_in, rows_grad) in enumerate(zip(plane_in, plane_grad)):
        in_part, out_part, *keep = unit_block(
            rows_in, rows_grad, gate_rows, up_rows, down_rows, owners, number
        )
        in_parts.append(in_part)
        out_parts.append(out_part)
        kept.append(keep)

    def join(parts):
        back = []
        for part, (low, high) in zip(parts, pieces):
            back.append(hops(part.reshape(experts, high - low, width), -1))
        return jnp.concatenate(back, axis=1).reshape(slot_total, width)

    in_back = join(in_parts)
    grad_mlp = []
    for j, rows in enumerate((plane_in[0], plane_in[0], plane_grad[0])):
        grad_mlp.append(dot_tn(kept[0][j], rows))
    grad_second = dot_tn(mlp_pick_low, in_back)
    cot_f32 = cotangent.astype(f32)
    grad_resid = cot_f32 + rms_back(grad_second, normed_two, scale_two, gain_two)

    cot_slots = dot_nn(attn_pick_low, grad_resid.astype(bf16)).reshape(experts, slots, width)
    send_cot = (attn_slot_gate[:, :, None] * cot_slots).astype(bf16)
    for j, rows in enumerate((plane_in[1], plane_in[1], plane_grad[1])):
        grad_mlp[j] = grad_mlp[j] + dot_tn(kept[1][j], rows)
    grad_mlp_weight = jnp.stack(grad_mlp, axis=1)[:, None, :, :]
    grad_result = after(exchange(send_cot), grad_mlp_weight).reshape(slot_total, width)
    grad_attn = dot_nt(grad_result, output_full).astype(bf16)
    output_term = dot_tn(attn_flat, grad_result).astype(bf16)
    grad_output_w = chip_sum(output_term, owners)
    out_back = join([plane_sum(after(part, *in_parts)) for part in out_parts])
    grad_query, grad_keys, grad_values = attend_back(
        query_low,
        kv_low,
        grad_attn.reshape(experts, slots, features),
        lse,
        slot_place3,
        slot_cont3,
        key_cont,
        qcos.reshape(experts, slots, HEAD),
        qsin.reshape(experts, slots, HEAD),
        kcos,
        ksin,
        tok_dev,
    )
    grad_query = grad_query.reshape(slot_total, features)
    mixed_tok = dot_tn(mlp_back, out_back)
    final = residual
    for k in range(per_token):
        final = final + mlp_gates[:, k : k + 1] * mixed_tok[k * tok_dev : (k + 1) * tok_dev]
    output = final.astype(bf16)

    grad_keys_w = dot_tn(hidden_all, grad_keys).astype(bf16)
    grad_values_w = dot_tn(hidden_all, grad_values).astype(bf16)
    grad_query = hold(grad_query, grad_keys_w, grad_values_w)
    kv_sums = [plane_sum(grad_keys_w), plane_sum(grad_values_w)]

    grad_rows = dot_nt(grad_query, query_full).astype(bf16)
    half = width // 2
    grad_h, grad_first = [], []
    for low in (0, half):
        span = slice(low, low + half)
        routed = lax.dot_general(
            own_low,
            grad_rows[:, span].reshape(experts, slots, half),
            (((1,), (1,)), ((0,), (0,))),
            preferred_element_type=f32,
        ).reshape(group, half)
        part = (
            dot_nt(grad_keys, kv_full[span, :features])
            + dot_nt(grad_values, kv_full[span, features:])
            + routed
        )
        grad_h.append(part)
        grad_first.append(
            hop_sum(part.astype(bf16).reshape(experts, tok_dev, half), expert_id, experts)
        )
    query_term = dot_tn(query_rows, hold(grad_query, grad_h[1])).astype(bf16)
    grad_query_w = chip_sum(query_term, owners)
    grad_kv_w = jnp.concatenate(
        [hop_sum(part.reshape(experts, -1, features), expert_id, experts) for part in kv_sums],
        axis=1,
    )
    grad_h = lax.optimization_barrier(tuple(grad_h))
    grad_gain_one = [
        jnp.sum(part * normed_all[:, low : low + half], axis=0)
        for part, low in zip(grad_h, (0, half))
    ]
    grad_gain_two = jnp.sum(grad_second * normed_two, axis=0)
    grad_first = jnp.concatenate(grad_first, axis=1)
    normed_one, scale_one = rms_parts(own_f32)
    grad_input = grad_resid + rms_back(grad_first, normed_one, scale_one, gain_one)

    gain_rows = jnp.concatenate(
        [
            jnp.concatenate(grad_gain_one).reshape(owners * experts, part_size),
            grad_gain_two.reshape(owners * experts, part_size),
        ],
        axis=1,
    )
    gain_rows = lax.all_to_all(
        hold(gain_rows, kv_sums[1])[:, None, :], ("dp", "expert"), split_axis=0, concat_axis=0, tiled=True
    )
    gain_rows = jnp.sum(gain_rows, axis=(0, 1))
    grad_gain_attn, grad_gain_mlp = gain_rows[:part_size], gain_rows[part_size:]
    return (
        output,
        grad_input,
        grad_gain_attn,
        grad_gain_mlp,
        grad_kv_w,
        grad_query_w[:, None, :],
        grad_output_w[:, None, :],
        grad_mlp_weight,
    )


def solution(mesh):
    placed = (
        P(("dp", "expert"), None),
        P(("dp", "expert"), None),
        P("dp"),
        P("dp", None),
        P(("dp", "expert"), None),
        P(("dp", "expert"), None),
        P(("dp", "expert"), None),
        P(("dp", "expert")),
        P(("dp", "expert")),
        P(("dp", "expert"), None),
        P("dp", "expert", None),
        P("dp", "expert", None),
        P("dp", "expert", None, None),
    )
    return jax.shard_map(
        layer,
        mesh=mesh,
        in_specs=placed,
        out_specs=(
            P(("dp", "expert"), None),
            P(("dp", "expert"), None),
            P(("dp", "expert")),
            P(("dp", "expert")),
            P(("dp", "expert"), None),
            P("dp", "expert", None),
            P("dp", "expert", None),
            P("dp", "expert", None, None),
        ),
        check_vma=False,
    )
```
